32 devices in a mesh: shard: 4 (over x, core), rep: 8 (over z, y).
Axes of the slice: x: 2, y: 2, z: 4, core: 2. Of those that a mesh axis runs over, the one named last changes fastest.
Arguments:
- block_input: bfloat16 [1536, 49, 512], P(('shard', 'rep')), may hold values from -6 to 6
- out_grad: bfloat16 [1536, 49, 512], P(('shard', 'rep')), may hold values from -6 to 6
- qkv_weight: bfloat16 [512, 1536], P('shard'), may hold values from -0.25 to 0.25
- query_bias: float32 [512], replicated, may hold values from -3 to 3
- value_bias: float32 [512], replicated, may hold values from -3 to 3
- proj_weight: bfloat16 [512, 512], P('shard'), may hold values from -0.75 to 0.75
- proj_bias: float32 [512], replicated, may hold values from -3 to 3
- hidden_weight: bfloat16 [512, 2048], P('shard'), may hold values from -0.25 to 0.25
- hidden_bias: float32 [2048], replicated, may hold values from -3 to 3
- output_weight: bfloat16 [2048, 512], P('shard'), may hold values from -0.125 to 0.125
- output_bias: float32 [512], replicated, may hold values from -3 to 3
- first_gain: float32 [512], replicated, may hold values from 0.25 to 1.75
- first_shift: float32 [512], replicated, may hold values from -3 to 3
- second_gain: float32 [512], replicated, may hold values from 0.25 to 1.75
- second_shift: float32 [512], replicated, may hold values from -3 to 3
- bias_table: float32 [169, 16], replicated, may hold values from -2.5 to 303
- table_index: int32 [49, 49], replicated, may hold values from 0 to 168, as said below
Outputs:
- block_output: bfloat16 [1536, 49, 512], P(('shard', 'rep'))
- input_grad: float32 [1536, 49, 512], P(('shard', 'rep'))
- qkv_weight_grad: float32 [512, 1536], P('shard')
- query_bias_grad: float32 [512], replicated
- value_bias_grad: float32 [512], replicated
- proj_weight_grad: float32 [512, 512], P('shard')
- proj_bias_grad: float32 [512], replicated
- hidden_weight_grad: float32 [512, 2048], P('shard')
- hidden_bias_grad: float32 [2048], replicated
- output_weight_grad: float32 [2048, 512], P('shard')
- output_bias_grad: float32 [512], replicated
- first_gain_grad: float32 [512], replicated
- first_shift_grad: float32 [512], replicated
- second_gain_grad: float32 [512], replicated
- second_shift_grad: float32 [512], replicated
- bias_table_grad: float32 [169, 16], replicated
The draws below stay inside these ranges and needn't reach their ends.
Inputs may be any that keep to these rules, and one draw needn't show every extreme that they name: `table_index`: every one of the 169 table rows is named by some pair.
All inputs are finite; a program needn't handle non-finite values.
Results may differ from the reference program's by a relative error of at most 0.017.
Values may be sent and summed in bfloat16 or wider, within the bound.
A program may use at most 320 MiB of HBM per device.

```python
import jax
import jax.numpy as jnp
from jax import lax

C = 512
H = 16
MLP = 2048
TOK_WIN = 49
TABLE = 169
WIN_DEV = 48
WINDOWS = 1536


def draw_bias_table(key, part):
    result = jax.random.truncated_normal(key, -2.5, 2.5, (TABLE, H), jnp.float32)
    return result


def draw_table_index(key, part):
    first = jax.random.permutation(jax.random.fold_in(key, 1), TABLE).astype(jnp.int32)
    others = jax.random.randint(jax.random.fold_in(key, 2), (TOK_WIN * TOK_WIN - TABLE,), 0, TABLE).astype(jnp.int32)
    joined = jnp.concatenate([first, others])
    mixed = jax.random.permutation(jax.random.fold_in(key, 3), joined)
    return mixed.reshape(TOK_WIN, TOK_WIN).astype(jnp.int32)


def block_levels(rng, extent, split, low, largest):
    level = 1.0
    for axis_at, blocks in split:
        steps = jax.random.uniform(jax.random.fold_in(jax.random.fold_in(rng, 6), axis_at), (blocks,), jnp.float32, low / len(split), largest / len(split))
        level = level * jnp.repeat(jnp.exp(steps), extent[axis_at] // blocks).reshape((-1,) + (1,) * (len(extent) - 1 - axis_at))
    return level


def noise(stream_key, dims, deviation, bound, split=(), kind=jnp.bfloat16):
    values = jax.random.normal(stream_key, dims, jnp.float32) * deviation
    if len(split) > 0:
        values = block_levels(stream_key, dims, split, -0.22, 0.18) * values
    return jnp.clip(values, min=-bound, max=bound).astype(kind)


def setup_inputs(seed: int = 0) -> dict:
    arg_keys = jax.random.split(jax.random.key(seed), 18)
    return {
        "block_input": noise(arg_keys[0], (WINDOWS, TOK_WIN, C), 1.0, 6.0, ((0, 32),)),
        "out_grad": noise(arg_keys[1], (WINDOWS, TOK_WIN, C), 1.0, 6.0, ((0, 32),)),
        "qkv_weight": noise(arg_keys[2], (C, 3 * C), C ** -0.5, 0.25, ((0, 4),)),
        "query_bias": noise(arg_keys[3], (C,), 0.5, 3.0, (), jnp.float32),
        "value_bias": noise(arg_keys[4], (C,), 0.5, 3.0, (), jnp.float32),
        "proj_weight": noise(arg_keys[5], (C, C), (C // 8) ** -0.5, 0.75, ((0, 4),)),
        "proj_bias": noise(arg_keys[6], (C,), 0.5, 3.0, (), jnp.float32),
        "hidden_weight": noise(arg_keys[7], (C, MLP), C ** -0.5, 0.25, ((0, 4),)),
        "hidden_bias": noise(arg_keys[8], (MLP,), 0.5, 3.0, (), jnp.float32),
        "output_weight": noise(arg_keys[9], (MLP, C), MLP ** -0.5, 0.125, ((0, 4),)),
        "output_bias": noise(arg_keys[10], (C,), 0.5, 3.0, (), jnp.float32),
        "first_gain": jnp.clip(1.0 + 0.15 * jax.random.normal(arg_keys[11], (C,), jnp.float32), 0.25, 1.75),
        "first_shift": noise(arg_keys[12], (C,), 0.5, 3.0, (), jnp.float32),
        "second_gain": jnp.clip(1.0 + 0.15 * jax.random.normal(arg_keys[13], (C,), jnp.float32), 0.25, 1.75),
        "second_shift": noise(arg_keys[14], (C,), 0.5, 3.0, (), jnp.float32),
        "bias_table": draw_bias_table(jax.random.fold_in(arg_keys[17], 71), 0),
        "table_index": draw_table_index(jax.random.fold_in(arg_keys[17], 71), 0),
    }


epsilon = 1e-05

def widen(values):
    return lax.optimization_barrier(values).astype(jnp.float32)

def layer_norm(values, gain, shift):
    center = values - lax.optimization_barrier(jnp.mean(values, axis=-1, keepdims=True))
    inverse = lax.rsqrt(lax.optimization_barrier(jnp.mean(center * center, axis=-1, keepdims=True)) + epsilon)
    normal = center * inverse
    return (normal * gain + shift, normal, inverse)

def norm_back(grad, normal, inverse, gain):
    scaled = grad * gain
    back = inverse * (scaled - lax.optimization_barrier(jnp.mean(scaled, axis=-1, keepdims=True)) - normal * lax.optimization_barrier(jnp.mean(scaled * normal, axis=-1, keepdims=True)))
    return (back, lax.optimization_barrier(jnp.sum(grad * normal, axis=0)), lax.optimization_barrier(jnp.sum(grad, axis=0)))

def gelu_value(upper):
    return 0.5 * upper * (1.0 + lax.erf(upper * 0.7071067811865476))

def gelu_slope(upper):
    return 0.5 * (1.0 + lax.erf(upper * 0.7071067811865476)) + upper * jnp.exp(-0.5 * upper * upper) * 0.3989422804014327

def layer_pass(block, cotangent, weights, table_bias):
    qkv_weight, query_bias, value_bias, proj_weight, proj_bias, hidden_weight, hidden_bias, output_weight, output_bias, first_gain, first_shift, second_gain, second_shift = weights
    windows, tokens, width = block.shape
    heads = table_bias.shape[0]
    head_size = width // heads
    scale = head_size ** (-0.5)
    flat_input = block.reshape(-1, width).astype(jnp.float32)
    normed1, normal1, inverse1 = layer_norm(flat_input, first_gain, first_shift)
    first_act = normed1.astype(jnp.bfloat16)
    projected = jnp.dot(first_act, qkv_weight, preferred_element_type=jnp.float32)
    split_shape = (windows, tokens, heads, head_size)
    query = ((projected[:, :width] + query_bias) * scale).astype(jnp.bfloat16).reshape(split_shape)
    keys = projected[:, width:2 * width].astype(jnp.bfloat16).reshape(split_shape)
    values = (projected[:, 2 * width:] + value_bias).astype(jnp.bfloat16).reshape(split_shape)
    scores = jnp.einsum('wqhd,wkhd->whqk', widen(query), widen(keys)) + table_bias[None]
    top = lax.optimization_barrier(jnp.max(scores, axis=-1, keepdims=True))
    logsum = top + jnp.log(lax.optimization_barrier(jnp.sum(jnp.exp(scores - top), axis=-1, keepdims=True)))
    probs = jnp.exp(scores - logsum)
    prob_half = probs.astype(jnp.bfloat16)
    mixed = jnp.einsum('whqk,wkhd->wqhd', widen(prob_half), widen(values)).astype(jnp.bfloat16).reshape(-1, width)
    residual = flat_input + jnp.dot(mixed, proj_weight, preferred_element_type=jnp.float32) + proj_bias
    normed2, normal2, inverse2 = layer_norm(residual, second_gain, second_shift)
    second_act = normed2.astype(jnp.bfloat16)
    upper = jnp.dot(second_act, hidden_weight, preferred_element_type=jnp.float32) + hidden_bias
    activated = gelu_value(upper).astype(jnp.bfloat16)
    block_output = (residual + jnp.dot(activated, output_weight, preferred_element_type=jnp.float32) + output_bias).astype(jnp.bfloat16)
    flat_cot = cotangent.reshape(-1, width)
    cot_wide = flat_cot.astype(jnp.float32)
    output_weight_grad = jnp.dot(activated.T, flat_cot, preferred_element_type=jnp.float32)
    output_bias_grad = lax.optimization_barrier(jnp.sum(cot_wide, axis=0))
    upper_grad = (jnp.dot(flat_cot, output_weight.T, preferred_element_type=jnp.float32) * gelu_slope(upper)).astype(jnp.bfloat16)
    hidden_weight_grad = jnp.dot(second_act.T, upper_grad, preferred_element_type=jnp.float32)
    hidden_bias_grad = lax.optimization_barrier(jnp.sum(upper_grad.astype(jnp.float32), axis=0))
    second_grad = jnp.dot(upper_grad, hidden_weight.T, preferred_element_type=jnp.float32)
    second_back, second_gain_grad, second_shift_grad = norm_back(second_grad, normal2, inverse2, second_gain)
    residual_grad = cot_wide + second_back
    residual_half = residual_grad.astype(jnp.bfloat16)
    proj_weight_grad = jnp.dot(mixed.T, residual_half, preferred_element_type=jnp.float32)
    proj_bias_grad = lax.optimization_barrier(jnp.sum(residual_grad, axis=0))
    mixed_grad = jnp.dot(residual_half, proj_weight.T, preferred_element_type=jnp.float32).astype(jnp.bfloat16).reshape(split_shape)
    prob_grad = jnp.einsum('wqhd,wkhd->whqk', widen(mixed_grad), widen(values))
    value_grad = jnp.einsum('whqk,wqhd->wkhd', widen(prob_half), widen(mixed_grad))
    score_grad = probs * (prob_grad - lax.optimization_barrier(jnp.sum(probs * prob_grad, axis=-1, keepdims=True)))
    bias_sum = lax.optimization_barrier(jnp.sum(score_grad, axis=0))
    score_half = score_grad.astype(jnp.bfloat16)
    query_grad = jnp.einsum('whqk,wkhd->wqhd', widen(score_half), widen(keys)) * scale
    key_grad = jnp.einsum('whqk,wqhd->wkhd', widen(score_half), widen(query))
    query_flat = query_grad.reshape(-1, width)
    value_flat = value_grad.reshape(-1, width)
    merged_grad = jnp.concatenate([query_flat, key_grad.reshape(-1, width), value_flat], axis=1).astype(jnp.bfloat16)
    query_bias_grad = lax.optimization_barrier(jnp.sum(query_flat, axis=0))
    value_bias_grad = lax.optimization_barrier(jnp.sum(value_flat, axis=0))
    qkv_weight_grad = jnp.dot(first_act.T, merged_grad, preferred_element_type=jnp.float32)
    first_grad = jnp.dot(merged_grad, qkv_weight.T, preferred_element_type=jnp.float32)
    first_back, first_gain_grad, first_shift_grad = norm_back(first_grad, normal1, inverse1, first_gain)
    input_grad = (residual_grad + first_back).reshape(windows, tokens, width)
    grads = (qkv_weight_grad, query_bias_grad, value_bias_grad, proj_weight_grad, proj_bias_grad, hidden_weight_grad, hidden_bias_grad, output_weight_grad, output_bias_grad, first_gain_grad, first_shift_grad, second_gain_grad, second_shift_grad, bias_sum)
    return (block_output.reshape(windows, tokens, width), input_grad, grads)

def reference(block_input, out_grad, qkv_weight, query_bias, value_bias, proj_weight, proj_bias, hidden_weight, hidden_bias, output_weight, output_bias, first_gain, first_shift, second_gain, second_shift, bias_table, table_index):
    table_bias = jnp.transpose(bias_table[table_index], (2, 0, 1))
    blocks = block_input.shape[0] // WIN_DEV
    width = block_input.shape[2]
    inputs = block_input.reshape(blocks, WIN_DEV, TOK_WIN, width)
    cotangents = out_grad.reshape(blocks, WIN_DEV, TOK_WIN, width)
    weights = (qkv_weight, query_bias, value_bias, proj_weight, proj_bias, hidden_weight, hidden_bias, output_weight, output_bias, first_gain, first_shift, second_gain, second_shift)
    zeros = tuple((jnp.zeros(weight.shape, jnp.float32) for weight in weights)) + (jnp.zeros(table_bias.shape, jnp.float32),)

    def step(carry, pair):
        outputs, grad_in, grads = layer_pass(pair[0], pair[1], weights, table_bias)
        return (tuple((left + right for left, right in zip(carry, grads))), (outputs, grad_in))
    totals, stacked = lax.scan(step, zeros, (inputs, cotangents))
    heads = bias_table.shape[1]
    bias_table_grad = jnp.zeros(bias_table.shape, jnp.float32).at[table_index.reshape(-1)].add(totals[13].reshape(heads, -1).T)
    block_output = stacked[0].reshape(block_input.shape)
    input_grad = stacked[1].reshape(block_input.shape)
    return (block_output, input_grad, totals[0], totals[1], totals[2], totals[3], totals[4], totals[5], totals[6], totals[7], totals[8], totals[9], totals[10], totals[11], totals[12], bias_table_grad)
```

```python
import functools

import jax
import jax.numpy as jnp
from jax import lax
from jax.experimental import pallas as pl
from jax.experimental.pallas import tpu as pltpu
from jax.sharding import PartitionSpec as P

epsilon = 1e-05
f32 = jnp.float32
bf16 = jnp.bfloat16


def dot_nn(a, b):
    return lax.dot_general(a, b, (((1,), (0,)), ((), ())), preferred_element_type=f32)


def dot_nt(a, b):
    return lax.dot_general(a, b, (((1,), (1,)), ((), ())), preferred_element_type=f32)


def dot_tn(a, b):
    return lax.dot_general(a, b, (((0,), (0,)), ((), ())), preferred_element_type=f32)


def norm_parts(values):
    center = values - jnp.mean(values, axis=-1, keepdims=True)
    inverse = lax.rsqrt(jnp.mean(center * center, axis=-1, keepdims=True) + epsilon)
    return center * inverse, inverse


def fold_rows(values):
    rows, cols = values.shape
    return jnp.sum(values.reshape(rows // 8, 8, cols), axis=0)


def gelu_pair(upper):
    bell = jnp.exp(upper * upper * -0.5)
    t = 1.0 / (1.0 + 0.23164189 * jnp.abs(upper))
    poly = t * (
        0.127414796
        + t * (-0.142248368 + t * (0.7107068705 + t * (-0.7265760135 + t * 0.5307027145)))
    )
    tail = poly * bell
    phi = jnp.where(upper >= 0.0, 1.0 - tail, tail)
    return upper * phi, phi + upper * bell * 0.3989422804014327


def compute_kernel(
    dims,
    x_ref,
    dy_ref,
    wqkv_ref,
    wproj_ref,
    w1_ref,
    w2_ref,
    qkv_bias_ref,
    qkv_scale_ref,
    proj_bias_ref,
    hidden_bias_ref,
    output_bias_ref,
    gain1_ref,
    shift1_ref,
    gain2_ref,
    shift2_ref,
    bias_ref,
    y_ref,
    dx_ref,
    dwqkv_ref,
    dwproj_ref,
    dw1_ref,
    dw2t_ref,
    small_ref,
    dbias_ref,
    perm_ref,
    back_ref,
    act_w_ref,
    qkv_ref,
    mixed_w_ref,
    mixed_ref,
    lse_ref,
    wide_ref,
    sa_ref,
    sat_ref,
    dyt_ref,
    u_ref,
    da_ref,
    act_ref,
    dup_ref,
    acc_ref,
):
    tokens, windows, width, heads, hidden = dims
    head_size = width // heads
    scale = head_size ** (-0.5)
    pad = 64
    key_rows = 56
    sub = 8
    group = 2 * sub
    groups = windows // group
    quad = 128 // head_size
    quads = heads // quad
    rows8 = tokens * sub
    rows = tokens * group
    rows_w = sub * pad
    chunk = 256
    step = 7
    lane_head = lax.broadcasted_iota(jnp.int32, (pad, 128), 1) // head_size
    head_masks = [(lane_head == h).astype(f32) for h in range(quad)]
    head_masks_half = [m.astype(bf16) for m in head_masks]

    base = {}
    at = 0
    for name, size in (
        ("qb", width),
        ("vb", width),
        ("pb", width),
        ("hb", hidden),
        ("ob", width),
        ("g1", width),
        ("s1", width),
        ("g2", width),
        ("s2", width),
    ):
        base[name] = (at, size)
        at += size

    def add_small(name, value, offset=0):
        start = base[name][0] + offset
        cols = pl.ds(start, value.shape[1])
        small_ref[:, cols] = small_ref[:, cols] + value

    small_ref[...] = jnp.zeros(small_ref.shape, f32)
    dbias_ref[...] = jnp.zeros(dbias_ref.shape, f32)

    @pl.loop(0, rows_w // 64)
    def _(n):
        start = pl.multiple_of(n * 64, 64)
        to = lax.broadcasted_iota(jnp.int32, (64, rows8), 0) + start
        source = lax.broadcasted_iota(jnp.int32, (64, rows8), 1)
        hit = (to // pad == source % sub) & (to % pad == source // sub)
        perm_ref[pl.ds(start, 64), :] = hit.astype(f32).astype(bf16)

    @pl.loop(0, rows8 // 56)
    def _(n):
        start = pl.multiple_of(n * 56, 8)
        to = lax.broadcasted_iota(jnp.int32, (56, rows_w), 0) + start
        source = lax.broadcasted_iota(jnp.int32, (56, rows_w), 1)
        hit = (source // pad == to % sub) & (source % pad == to // sub)
        back_ref[pl.ds(start, 56), :] = hit.astype(f32).astype(bf16)

    def stacked(tile):
        return jnp.concatenate([tile * m for m in head_masks_half], axis=0)

    def diagonal(tall):
        total = tall[0:pad] * head_masks[0]
        for h in range(1, quad):
            total = total + tall[h * pad : (h + 1) * pad] * head_masks[h]
        return total

    def grow(values):
        return jnp.concatenate([values, jnp.zeros((pad - key_rows, values.shape[1]), f32)], axis=0)

    @pl.loop(0, groups)
    def _(g):
        win0 = pl.multiple_of(g * group, group)

        @pl.loop(0, tokens // step)
        def _(n):
            part = x_ref[pl.ds(n * step, step), pl.ds(win0, group), :].astype(f32)
            flat = part.reshape(step * group, width)
            normal, _ = norm_parts(flat)
            wide_ref[pl.ds(n * step, step)] = (normal * gain1_ref[...] + shift1_ref[...]).reshape(
                step, group, width
            )

        for s in range(2):
            g2 = g * 2 + s
            act8 = wide_ref[:, sub * s : sub * (s + 1), :].reshape(rows8, width).astype(bf16)
            act_w_ref[g2] = dot_nn(perm_ref[...], act8).astype(bf16)

            @pl.loop(0, 3 * width // chunk)
            def _(n):
                cols = pl.ds(pl.multiple_of(n * chunk, chunk), chunk)
                out = dot_nn(act_w_ref[g2], wqkv_ref[:, cols])
                qkv_ref[g2, :, cols] = (
                    (out + qkv_bias_ref[:, cols]) * qkv_scale_ref[:, cols]
                ).astype(bf16)

            @pl.loop(0, sub)
            def _(w):
                line = pl.ds(pl.multiple_of(w * pad, pad), pad)
                for t in range(quads):
                    q4 = qkv_ref[g2, line, 128 * t : 128 * (t + 1)]
                    k4 = qkv_ref[g2, line, width + 128 * t : width + 128 * (t + 1)]
                    v4 = qkv_ref[g2, line, 2 * width + 128 * t : 2 * width + 128 * (t + 1)]
                    scores = dot_nt(k4, stacked(q4))[0:key_rows] + bias_ref[t]
                    top = jnp.max(scores, axis=0, keepdims=True)
                    weight = jnp.exp(scores - top)
                    total = jnp.sum(weight, axis=0, keepdims=True)
                    lse_ref[g2, w, t : t + 1, :] = top + jnp.log(total)
                    probs = grow(weight * (1.0 / total)).astype(bf16)
                    mixed_w_ref[line, 128 * t : 128 * (t + 1)] = diagonal(dot_tn(probs, v4)).astype(
                        bf16
                    )

            wide_ref[:, sub * s : sub * (s + 1), :] = dot_nn(back_ref[...], mixed_w_ref[...]).reshape(
                tokens, sub, width
            )

        mixed_ref[:, pl.ds(win0, group), :] = wide_ref[...].astype(bf16)
        mixed = mixed_ref[:, pl.ds(win0, group), :].reshape(rows, width)
        for n in range(width // chunk):
            cols = slice(n * chunk, (n + 1) * chunk)
            out = dot_nn(mixed, wproj_ref[:, cols]) + proj_bias_ref[:, cols]
            dx_ref[:, pl.ds(win0, group), cols] = (
                x_ref[:, pl.ds(win0, group), cols].astype(f32) + out.reshape(tokens, group, chunk)
            )

    @pl.loop(0, groups)
    def _(g):
        win0 = pl.multiple_of(g * group, group)

        @pl.loop(0, tokens // step)
        def _(n):
            part = dx_ref[pl.ds(n * step, step), pl.ds(win0, group), :].reshape(step * group, width)
            normal, _ = norm_parts(part)
            lines = pl.ds(pl.multiple_of(n * step * group, step * group), step * group)
            sa_ref[lines, :] = (normal * gain2_ref[...] + shift2_ref[...]).astype(bf16)

        dy = dy_ref[:, pl.ds(win0, group), :].reshape(rows, width)
        sat_ref[...] = sa_ref[...].T
        dyt_ref[...] = dy.T

        @pl.loop(0, hidden // chunk)
        def _(n):
            start = pl.multiple_of(n * chunk, chunk)
            cols = pl.ds(start, chunk)
            u_ref[...] = dot_nn(sa_ref[...], w1_ref[:, cols])
            da_ref[...] = dot_nt(
                dy_ref[:, pl.ds(win0, group), :].reshape(rows, width), w2_ref[cols, :]
            )

            @pl.loop(0, tokens // step)
            def _(m):
                lines = pl.ds(pl.multiple_of(m * step * group, step * group), step * group)
                value, slope = gelu_pair(u_ref[lines, :] + hidden_bias_ref[:, cols])
                act_ref[lines, cols] = value.astype(bf16)
                dup = (da_ref[lines, :] * slope).astype(bf16)
                dup_ref[lines, cols] = dup
                add_small("hb", fold_rows(dup.astype(f32)), start)

            part1 = dot_nn(sat_ref[...], dup_ref[:, cols])
            part2 = dot_nn(dyt_ref[...], act_ref[:, cols])

            @pl.when(g == 0)
            def _():
                dw1_ref[:, cols] = part1
                dw2t_ref[:, cols] = part2

            @pl.when(g != 0)
            def _():
                dw1_ref[:, cols] += part1
                dw2t_ref[:, cols] += part2

        for n in range(width // chunk):
            cols = slice(n * chunk, (n + 1) * chunk)
            out = dot_nn(act_ref[...], w2_ref[:, cols]) + output_bias_ref[:, cols]
            y_ref[:, pl.ds(win0, group), cols] = (
                dx_ref[:, pl.ds(win0, group), cols] + out.reshape(tokens, group, chunk)
            ).astype(bf16)
            acc_ref[:, cols] = dot_nt(dup_ref[...], w1_ref[cols, :])

        @pl.loop(0, tokens // step)
        def _(n):
            lines = pl.ds(pl.multiple_of(n * step * group, step * group), step * group)
            normal, inverse = norm_parts(
                dx_ref[pl.ds(n * step, step), pl.ds(win0, group), :].reshape(step * group, width)
            )
            grad = acc_ref[lines, :]
            scaled = grad * gain2_ref[...]
            back = inverse * (
                scaled
                - jnp.mean(scaled, axis=-1, keepdims=True)
                - normal * jnp.mean(scaled * normal, axis=-1, keepdims=True)
            )
            cot = dy_ref[pl.ds(n * step, step), pl.ds(win0, group), :].astype(f32)
            cot = cot.reshape(step * group, width)
            total = cot + back
            dx_ref[pl.ds(n * step, step), pl.ds(win0, group), :] = total.reshape(step, group, width)
            sa_ref[lines, :] = total.astype(bf16)
            add_small("ob", fold_rows(cot))
            add_small("pb", fold_rows(total))
            add_small("g2", fold_rows(grad * normal))
            add_small("s2", fold_rows(grad))

        mixed = mixed_ref[:, pl.ds(win0, group), :].reshape(rows, width)
        part3 = dot_tn(mixed, sa_ref[...])

        @pl.when(g == 0)
        def _():
            dwproj_ref[...] = part3

        @pl.when(g != 0)
        def _():
            dwproj_ref[...] += part3

    @pl.loop(0, groups)
    def _(g):
        win0 = pl.multiple_of(g * group, group)
        wide_ref[...] = dx_ref[:, pl.ds(win0, group), :]
        for s in range(2):
            g2 = g * 2 + s
            half8 = wide_ref[:, sub * s : sub * (s + 1), :].reshape(rows8, width).astype(bf16)
            half_w = dot_nn(perm_ref[...], half8).astype(bf16)
            mixed_w_ref[...] = dot_nt(half_w, wproj_ref[...]).astype(bf16)

            @pl.loop(0, sub)
            def _(w):
                line = pl.ds(pl.multiple_of(w * pad, pad), pad)
                for t in range(quads):
                    cols_q = slice(128 * t, 128 * (t + 1))
                    cols_k = slice(width + 128 * t, width + 128 * (t + 1))
                    cols_v = slice(2 * width + 128 * t, 2 * width + 128 * (t + 1))
                    q4 = qkv_ref[g2, line, cols_q]
                    k4 = qkv_ref[g2, line, cols_k]
                    v4 = qkv_ref[g2, line, cols_v]
                    go4 = mixed_w_ref[line, cols_q]
                    queries = stacked(q4)
                    grads = stacked(go4)
                    scores = dot_nt(k4, queries)[0:key_rows] + bias_ref[t]
                    probs = jnp.exp(scores - lse_ref[g2, w, t : t + 1, :])
                    prob_grad = dot_nt(v4, grads)[0:key_rows]
                    delta = jnp.sum(probs * prob_grad, axis=0, keepdims=True)
                    score_grad = probs * (prob_grad - delta)
                    dbias_ref[t] += score_grad
                    prob_half = grow(probs).astype(bf16)
                    score_half = grow(score_grad).astype(bf16)
                    value_grad = dot_nn(prob_half, grads)
                    key_grad = dot_nn(score_half, queries)
                    query_grad = diagonal(dot_tn(score_half, k4)) * scale
                    add_small("qb", fold_rows(query_grad), 128 * t)
                    add_small("vb", fold_rows(value_grad), 128 * t)
                    qkv_ref[g2, line, cols_q] = query_grad.astype(bf16)
                    qkv_ref[g2, line, cols_k] = key_grad.astype(bf16)
                    qkv_ref[g2, line, cols_v] = value_grad.astype(bf16)

            @pl.loop(0, 3 * width // chunk)
            def _(n):
                cols = pl.ds(pl.multiple_of(n * chunk, chunk), chunk)
                part = dot_tn(act_w_ref[g2], qkv_ref[g2, :, cols])

                @pl.when(g2 == 0)
                def _():
                    dwqkv_ref[:, cols] = part

                @pl.when(g2 != 0)
                def _():
                    dwqkv_ref[:, cols] += part

            for n in range(width // chunk):
                cols = slice(n * chunk, (n + 1) * chunk)
                mixed_w_ref[:, cols] = dot_nt(qkv_ref[g2], wqkv_ref[cols, :]).astype(bf16)
            wide_ref[:, sub * s : sub * (s + 1), :] = dot_nn(back_ref[...], mixed_w_ref[...]).reshape(
                tokens, sub, width
            )

        @pl.loop(0, tokens // step)
        def _(n):
            part = x_ref[pl.ds(n * step, step), pl.ds(win0, group), :].astype(f32)
            normal, inverse = norm_parts(part.reshape(step * group, width))
            grad = wide_ref[pl.ds(n * step, step)].reshape(step * group, width)
            scaled = grad * gain1_ref[...]
            back = inverse * (
                scaled
                - jnp.mean(scaled, axis=-1, keepdims=True)
                - normal * jnp.mean(scaled * normal, axis=-1, keepdims=True)
            )
            dx_ref[pl.ds(n * step, step), pl.ds(win0, group), :] += back.reshape(step, group, width)
            add_small("g1", fold_rows(grad * normal))
            add_small("s1", fold_rows(grad))


def local_pass(x, dy, wqkv, wproj, w1, w2, vectors, bias, heads):
    tokens, windows, width = x.shape
    hidden = w1.shape[1]
    dims = (tokens, windows, width, heads, hidden)
    sub = 8
    pad = 64
    rows = tokens * 2 * sub
    small_size = 8 * width + hidden
    subs = windows // sub
    shapes = (
        jax.ShapeDtypeStruct(x.shape, bf16),
        jax.ShapeDtypeStruct(x.shape, f32),
        jax.ShapeDtypeStruct(wqkv.shape, f32),
        jax.ShapeDtypeStruct(wproj.shape, f32),
        jax.ShapeDtypeStruct(w1.shape, f32),
        jax.ShapeDtypeStruct((width, hidden), f32),
        jax.ShapeDtypeStruct((8, small_size), f32),
        jax.ShapeDtypeStruct(bias.shape, f32),
    )
    vmem = pl.BlockSpec(memory_space=pltpu.VMEM)
    return pl.pallas_call(
        functools.partial(compute_kernel, dims),
        out_shape=shapes,
        in_specs=[vmem] * 16,
        out_specs=[vmem] * len(shapes),
        scratch_shapes=[
            pltpu.VMEM((sub * pad, tokens * sub), bf16),
            pltpu.VMEM((tokens * sub, sub * pad), bf16),
            pltpu.VMEM((subs, sub * pad, width), bf16),
            pltpu.VMEM((subs, sub * pad, 3 * width), bf16),
            pltpu.VMEM((sub * pad, width), bf16),
            pltpu.VMEM(x.shape, bf16),
            pltpu.VMEM((subs, sub, heads // 4, 256), f32),
            pltpu.VMEM((tokens, 2 * sub, width), f32),
            pltpu.VMEM((rows, width), bf16),
            pltpu.VMEM((width, rows), bf16),
            pltpu.VMEM((width, rows), bf16),
            pltpu.VMEM((rows, 256), f32),
            pltpu.VMEM((rows, 256), f32),
            pltpu.VMEM((rows, hidden), bf16),
            pltpu.VMEM((rows, hidden), bf16),
            pltpu.VMEM((rows, width), f32),
        ],
        compiler_params=pltpu.CompilerParams(vmem_limit_bytes=67043328),
    )(x, dy, wqkv, wproj, w1, w2, *vectors, bias)


def on_device(
    block_input,
    out_grad,
    qkv_weight,
    query_bias,
    value_bias,
    proj_weight,
    proj_bias,
    hidden_weight,
    hidden_bias,
    output_weight,
    output_bias,
    first_gain,
    first_shift,
    second_gain,
    second_shift,
    bias_table,
    table_index,
):
    windows, tokens, width = block_input.shape
    table_rows, heads = bias_table.shape
    hidden = hidden_bias.shape[0]
    scale = (width // heads) ** (-0.5)
    pairs = tokens * tokens
    one_hot = (
        table_index.T.reshape(pairs, 1) == lax.broadcasted_iota(jnp.int32, (pairs, table_rows), 1)
    ).astype(f32)
    by_pair = jnp.dot(one_hot, bias_table, precision=lax.Precision.HIGHEST)
    by_key = by_pair.reshape(tokens, tokens, heads).transpose(0, 2, 1)
    by_key = jnp.pad(by_key, ((0, 0), (0, 0), (0, 64 - tokens)))
    by_key = jnp.pad(by_key, ((0, 56 - tokens), (0, 0), (0, 0)), constant_values=-1e30)
    quads = heads // 4
    bias = by_key.reshape(56, quads, 256).transpose(1, 0, 2)
    wqkv, wproj, w1, w2 = (
        lax.all_gather(w, "shard", axis=0, tiled=True)
        for w in (qkv_weight, proj_weight, hidden_weight, output_weight)
    )
    zeros = jnp.zeros((width,), f32)
    ones = jnp.ones((2 * width,), f32)
    vectors = [
        v.reshape(1, -1)
        for v in (
            jnp.concatenate([query_bias, zeros, value_bias]),
            jnp.concatenate([jnp.full((width,), scale, f32), ones]),
            proj_bias,
            hidden_bias,
            output_bias,
            first_gain,
            first_shift,
            second_gain,
            second_shift,
        )
    ]
    y, dx, dwqkv, dwproj, dw1, dw2t, small, dbias = local_pass(
        jnp.transpose(block_input, (1, 0, 2)),
        jnp.transpose(out_grad, (1, 0, 2)),
        wqkv,
        wproj,
        w1,
        w2,
        vectors,
        bias,
        heads,
    )
    dbias = dbias.transpose(1, 0, 2).reshape(56, heads, 64)[:tokens, :, :tokens]
    dbias = dbias.transpose(1, 0, 2).reshape(heads, pairs)
    bias_table_grad = jnp.dot(dbias, one_hot, precision=lax.Precision.HIGHEST).T
    shares = [
        lax.psum_scatter(g.astype(bf16), "shard", scatter_dimension=0, tiled=True)
        for g in (dwqkv, dwproj, dw1, dw2t.T)
    ]
    shares = [lax.psum(s, "rep").astype(f32) for s in shares]
    small, bias_table_grad = lax.psum(
        (jnp.sum(small, axis=0), bias_table_grad), ("shard", "rep")
    )
    cuts = [width, width, width, hidden, width, width, width, width, width]
    parts = []
    at = 0
    for size in cuts:
        parts.append(small[at : at + size])
        at += size
    qb, vb, pb, hb, ob, g1, s1, g2, s2 = parts
    return (
        jnp.transpose(y, (1, 0, 2)),
        jnp.transpose(dx, (1, 0, 2)),
        shares[0],
        qb,
        vb,
        shares[1],
        pb,
        shares[2],
        hb,
        shares[3],
        ob,
        g1,
        s1,
        g2,
        s2,
        bias_table_grad,
    )


def solution(mesh):
    rows = P(("shard", "rep"), None, None)
    cut = P("shard", None)
    full = P()
    return jax.shard_map(
        on_device,
        mesh=mesh,
        in_specs=(
            rows,
            rows,
            cut,
            full,
            full,
            cut,
            full,
            cut,
            full,
            cut,
            full,
            full,
            full,
            full,
            full,
            full,
            full,
        ),
        out_specs=(
            rows,
            rows,
            cut,
            full,
            full,
            cut,
            full,
            cut,
            full,
            cut,
            full,
            full,
            full,
            full,
            full,
            full,
        ),
        check_vma=False,
    )
```

```python
import functools

import jax
import jax.numpy as jnp
from jax import lax
from jax.experimental import pallas as pl
from jax.experimental.pallas import tpu as pltpu
from jax.sharding import PartitionSpec as P

epsilon = 1e-05
f32 = jnp.float32
bf16 = jnp.bfloat16


def dot_nn(a, b):
    return lax.dot_general(a, b, (((1,), (0,)), ((), ())), preferred_element_type=f32)


def dot_nt(a, b):
    return lax.dot_general(a, b, (((1,), (1,)), ((), ())), preferred_element_type=f32)


def dot_tn(a, b):
    return lax.dot_general(a, b, (((0,), (0,)), ((), ())), preferred_element_type=f32)


def norm_parts(values):
    center = values - jnp.mean(values, axis=-1, keepdims=True)
    inverse = lax.rsqrt(jnp.mean(center * center, axis=-1, keepdims=True) + epsilon)
    return center * inverse, inverse


def fold_rows(values):
    rows, cols = values.shape
    return jnp.sum(values.reshape(rows // 8, 8, cols), axis=0)


def gelu_pair(upper):
    bell = jnp.exp(upper * upper * -0.5)
    t = 1.0 / (1.0 + 0.23164189 * jnp.abs(upper))
    poly = t * (
        0.127414796
        + t * (-0.142248368 + t * (0.7107068705 + t * (-0.7265760135 + t * 0.5307027145)))
    )
    tail = poly * bell
    phi = jnp.where(upper >= 0.0, 1.0 - tail, tail)
    return upper * phi, phi + upper * bell * 0.3989422804014327


def compute_kernel(
    dims,
    x_ref,
    dy_ref,
    wqkv_shard,
    wproj_shard,
    w1_shard,
    w2_shard,
    qkv_bias_ref,
    qkv_scale_ref,
    proj_bias_ref,
    hidden_bias_ref,
    output_bias_ref,
    gain1_ref,
    shift1_ref,
    gain2_ref,
    shift2_ref,
    bias_ref,
    y_ref,
    dx_ref,
    dwqkv_ref,
    dwproj_ref,
    dw1_ref,
    dw2t_ref,
    small_ref,
    dbias_ref,
    perm_ref,
    back_ref,
    act_w_ref,
    qkv_ref,
    mixed_w_ref,
    mixed_ref,
    lse_ref,
    wide_ref,
    sa_ref,
    sat_ref,
    dyt_ref,
    u_ref,
    da_ref,
    act_ref,
    dup_ref,
    acc_ref,
    wqkv_ref,
    wproj_ref,
    w1_ref,
    w2_ref,
    own_sem,
    pair_send,
    pair_recv,
    chip_send,
    chip_recv,
):
    tokens, windows, width, heads, hidden, shards = dims
    me = lax.axis_index("shard")
    chips = shards // 2
    core = lax.rem(me, 2)
    chip = me // 2
    pair = chip * 2 + 1 - core

    def block(ref, index):
        size = ref.shape[0] // shards
        return ref.at[pl.ds(pl.multiple_of(index * size, size), size), :]

    def peer(k):
        return lax.rem(chip + k, chips) * 2 + core

    def owner(k, side):
        return lax.rem(chip + chips - k, chips) * 2 + side

    gathers = (
        (wqkv_shard, wqkv_ref),
        (wproj_shard, wproj_ref),
        (w1_shard, w1_ref),
        (w2_shard, w2_ref),
    )

    def own_copy(i):
        shard, full = gathers[i]
        return pltpu.make_async_copy(shard, block(full, me), own_sem.at[i])

    def chip_copy(i, k):
        shard, full = gathers[i]
        return pltpu.make_async_remote_copy(
            src_ref=shard,
            dst_ref=block(full, me),
            send_sem=chip_send.at[i, k - 1],
            recv_sem=chip_recv.at[i, k - 1],
            device_id={"shard": peer(k)},
            device_id_type=pl.DeviceIdType.MESH,
        )

    def pair_copy(i, k):
        shard, full = gathers[i]
        return pltpu.make_async_remote_copy(
            src_ref=shard if k == 0 else block(full, owner(k, core)),
            dst_ref=block(full, owner(k, core)),
            send_sem=pair_send.at[i, k],
            recv_sem=pair_recv.at[i, k],
            device_id={"shard": pair},
            device_id_type=pl.DeviceIdType.MESH,
        )

    def gather_start(i):
        own_copy(i).start()
        for k in range(1, chips):
            chip_copy(i, k).start()
        pair_copy(i, 0).start()

    def gather_finish(i):
        for k in range(1, chips):
            chip_copy(i, k).wait_recv()
            pair_copy(i, k).start()
        own_copy(i).wait()
        for k in range(chips):
            pair_copy(i, k).wait_recv()

    def gather_drain(i):
        for k in range(1, chips):
            chip_copy(i, k).wait_send()
        for k in range(chips):
            pair_copy(i, k).wait_send()

    barrier = pltpu.get_barrier_semaphore()
    for target in [pair] + [peer(k) for k in range(1, chips)]:
        pl.semaphore_signal(
            barrier, inc=1, device_id={"shard": target}, device_id_type=pl.DeviceIdType.MESH
        )
    pl.semaphore_wait(barrier, chips)
    gather_start(0)
    gather_start(1)

    head_size = width // heads
    scale = head_size ** (-0.5)
    pad = 64
    key_rows = 56
    sub = 8
    group = 2 * sub
    groups = windows // group
    quad = 128 // head_size
    quads = heads // quad
    rows8 = tokens * sub
    rows = tokens * group
    rows_w = sub * pad
    chunk = 256
    step = 7
    lane_head = lax.broadcasted_iota(jnp.int32, (pad, 128), 1) // head_size
    head_masks = [(lane_head == h).astype(f32) for h in range(quad)]
    head_masks_half = [m.astype(bf16) for m in head_masks]

    base = {}
    at = 0
    for name, size in (
        ("qb", width),
        ("vb", width),
        ("pb", width),
        ("hb", hidden),
        ("ob", width),
        ("g1", width),
        ("s1", width),
        ("g2", width),
        ("s2", width),
    ):
        base[name] = (at, size)
        at += size

    def add_small(name, value, offset=0):
        start = base[name][0] + offset
        cols = pl.ds(start, value.shape[1])
        small_ref[:, cols] = small_ref[:, cols] + value

    small_ref[...] = jnp.zeros(small_ref.shape, f32)
    dbias_ref[...] = jnp.zeros(dbias_ref.shape, f32)

    @pl.loop(0, rows_w // 64)
    def _(n):
        start = pl.multiple_of(n * 64, 64)
        to = lax.broadcasted_iota(jnp.int32, (64, rows8), 0) + start
        source = lax.broadcasted_iota(jnp.int32, (64, rows8), 1)
        hit = (to // pad == source % sub) & (to % pad == source // sub)
        perm_ref[pl.ds(start, 64), :] = hit.astype(f32).astype(bf16)

    @pl.loop(0, rows8 // 56)
    def _(n):
        start = pl.multiple_of(n * 56, 8)
        to = lax.broadcasted_iota(jnp.int32, (56, rows_w), 0) + start
        source = lax.broadcasted_iota(jnp.int32, (56, rows_w), 1)
        hit = (source // pad == to % sub) & (source % pad == to // sub)
        back_ref[pl.ds(start, 56), :] = hit.astype(f32).astype(bf16)

    def stacked(tile):
        return jnp.concatenate([tile * m for m in head_masks_half], axis=0)

    def diagonal(tall):
        total = tall[0:pad] * head_masks[0]
        for h in range(1, quad):
            total = total + tall[h * pad : (h + 1) * pad] * head_masks[h]
        return total

    def grow(values):
        return jnp.concatenate([values, jnp.zeros((pad - key_rows, values.shape[1]), f32)], axis=0)

    @pl.loop(0, groups)
    def _(g):
        win0 = pl.multiple_of(g * group, group)

        @pl.loop(0, tokens // step)
        def _(n):
            part = x_ref[pl.ds(n * step, step), pl.ds(win0, group), :].astype(f32)
            flat = part.reshape(step * group, width)
            normal, _ = norm_parts(flat)
            wide_ref[pl.ds(n * step, step)] = (normal * gain1_ref[...] + shift1_ref[...]).reshape(
                step, group, width
            )

        for s in range(2):
            g2 = g * 2 + s
            act8 = wide_ref[:, sub * s : sub * (s + 1), :].reshape(rows8, width).astype(bf16)
            act_w_ref[g2] = dot_nn(perm_ref[...], act8).astype(bf16)
            if s == 0:

                @pl.when(g == 0)
                def _():
                    gather_finish(0)
                    gather_finish(1)
                    gather_start(2)
                    gather_start(3)

            @pl.loop(0, 3 * width // chunk)
            def _(n):
                cols = pl.ds(pl.multiple_of(n * chunk, chunk), chunk)
                out = dot_nn(act_w_ref[g2], wqkv_ref[:, cols])
                qkv_ref[g2, :, cols] = (
                    (out + qkv_bias_ref[:, cols]) * qkv_scale_ref[:, cols]
                ).astype(bf16)

            @pl.loop(0, sub)
            def _(w):
                line = pl.ds(pl.multiple_of(w * pad, pad), pad)
                for t in range(quads):
                    q4 = qkv_ref[g2, line, 128 * t : 128 * (t + 1)]
                    k4 = qkv_ref[g2, line, width + 128 * t : width + 128 * (t + 1)]
                    v4 = qkv_ref[g2, line, 2 * width + 128 * t : 2 * width + 128 * (t + 1)]
                    scores = dot_nt(k4, stacked(q4))[0:key_rows] + bias_ref[t]
                    top = jnp.max(scores, axis=0, keepdims=True)
                    weight = jnp.exp(scores - top)
                    total = jnp.sum(weight, axis=0, keepdims=True)
                    lse_ref[g2, w, t : t + 1, :] = top + jnp.log(total)
                    probs = grow(weight * (1.0 / total)).astype(bf16)
                    mixed_w_ref[line, 128 * t : 128 * (t + 1)] = diagonal(dot_tn(probs, v4)).astype(
                        bf16
                    )

            wide_ref[:, sub * s : sub * (s + 1), :] = dot_nn(back_ref[...], mixed_w_ref[...]).reshape(
                tokens, sub, width
            )

        mixed_ref[:, pl.ds(win0, group), :] = wide_ref[...].astype(bf16)
        mixed = mixed_ref[:, pl.ds(win0, group), :].reshape(rows, width)
        for n in range(width // chunk):
            cols = slice(n * chunk, (n + 1) * chunk)
            out = dot_nn(mixed, wproj_ref[:, cols]) + proj_bias_ref[:, cols]
            dx_ref[:, pl.ds(win0, group), cols] = (
                x_ref[:, pl.ds(win0, group), cols].astype(f32) + out.reshape(tokens, group, chunk)
            )

    gather_finish(2)
    gather_finish(3)
    for i in range(4):
        gather_drain(i)

    @pl.loop(0, groups)
    def _(g):
        win0 = pl.multiple_of(g * group, group)

        @pl.loop(0, tokens // step)
        def _(n):
            part = dx_ref[pl.ds(n * step, step), pl.ds(win0, group), :].reshape(step * group, width)
            normal, _ = norm_parts(part)
            lines = pl.ds(pl.multiple_of(n * step * group, step * group), step * group)
            sa_ref[lines, :] = (normal * gain2_ref[...] + shift2_ref[...]).astype(bf16)

        dy = dy_ref[:, pl.ds(win0, group), :].reshape(rows, width)
        sat_ref[...] = sa_ref[...].T
        dyt_ref[...] = dy.T

        @pl.loop(0, hidden // chunk)
        def _(n):
            start = pl.multiple_of(n * chunk, chunk)
            cols = pl.ds(start, chunk)
            u_ref[...] = dot_nn(sa_ref[...], w1_ref[:, cols])
            da_ref[...] = dot_nt(
                dy_ref[:, pl.ds(win0, group), :].reshape(rows, width), w2_ref[cols, :]
            )

            @pl.loop(0, tokens // step)
            def _(m):
                lines = pl.ds(pl.multiple_of(m * step * group, step * group), step * group)
                value, slope = gelu_pair(u_ref[lines, :] + hidden_bias_ref[:, cols])
                act_ref[lines, cols] = value.astype(bf16)
                dup = (da_ref[lines, :] * slope).astype(bf16)
                dup_ref[lines, cols] = dup
                add_small("hb", fold_rows(dup.astype(f32)), start)

            part1 = dot_nn(sat_ref[...], dup_ref[:, cols])
            part2 = dot_nn(dyt_ref[...], act_ref[:, cols])

            @pl.when(g == 0)
            def _():
                dw1_ref[:, cols] = part1
                dw2t_ref[:, cols] = part2

            @pl.when(g != 0)
            def _():
                dw1_ref[:, cols] += part1
                dw2t_ref[:, cols] += part2

        for n in range(width // chunk):
            cols = slice(n * chunk, (n + 1) * chunk)
            out = dot_nn(act_ref[...], w2_ref[:, cols]) + output_bias_ref[:, cols]
            y_ref[:, pl.ds(win0, group), cols] = (
                dx_ref[:, pl.ds(win0, group), cols] + out.reshape(tokens, group, chunk)
            ).astype(bf16)
            acc_ref[:, cols] = dot_nt(dup_ref[...], w1_ref[cols, :])

        @pl.loop(0, tokens // step)
        def _(n):
            lines = pl.ds(pl.multiple_of(n * step * group, step * group), step * group)
            normal, inverse = norm_parts(
                dx_ref[pl.ds(n * step, step), pl.ds(win0, group), :].reshape(step * group, width)
            )
            grad = acc_ref[lines, :]
            scaled = grad * gain2_ref[...]
            back = inverse * (
                scaled
                - jnp.mean(scaled, axis=-1, keepdims=True)
                - normal * jnp.mean(scaled * normal, axis=-1, keepdims=True)
            )
            cot = dy_ref[pl.ds(n * step, step), pl.ds(win0, group), :].astype(f32)
            cot = cot.reshape(step * group, width)
            total = cot + back
            dx_ref[pl.ds(n * step, step), pl.ds(win0, group), :] = total.reshape(step, group, width)
            sa_ref[lines, :] = total.astype(bf16)
            add_small("ob", fold_rows(cot))
            add_small("pb", fold_rows(total))
            add_small("g2", fold_rows(grad * normal))
            add_small("s2", fold_rows(grad))

        mixed = mixed_ref[:, pl.ds(win0, group), :].reshape(rows, width)
        part3 = dot_tn(mixed, sa_ref[...])

        @pl.when(g == 0)
        def _():
            dwproj_ref[...] = part3

        @pl.when(g != 0)
        def _():
            dwproj_ref[...] += part3

    @pl.loop(0, groups)
    def _(g):
        win0 = pl.multiple_of(g * group, group)
        wide_ref[...] = dx_ref[:, pl.ds(win0, group), :]
        for s in range(2):
            g2 = g * 2 + s
            half8 = wide_ref[:, sub * s : sub * (s + 1), :].reshape(rows8, width).astype(bf16)
            half_w = dot_nn(perm_ref[...], half8).astype(bf16)
            mixed_w_ref[...] = dot_nt(half_w, wproj_ref[...]).astype(bf16)

            @pl.loop(0, sub)
            def _(w):
                line = pl.ds(pl.multiple_of(w * pad, pad), pad)
                for t in range(quads):
                    cols_q = slice(128 * t, 128 * (t + 1))
                    cols_k = slice(width + 128 * t, width + 128 * (t + 1))
                    cols_v = slice(2 * width + 128 * t, 2 * width + 128 * (t + 1))
                    q4 = qkv_ref[g2, line, cols_q]
                    k4 = qkv_ref[g2, line, cols_k]
                    v4 = qkv_ref[g2, line, cols_v]
                    go4 = mixed_w_ref[line, cols_q]
                    queries = stacked(q4)
                    grads = stacked(go4)
                    scores = dot_nt(k4, queries)[0:key_rows] + bias_ref[t]
                    probs = jnp.exp(scores - lse_ref[g2, w, t : t + 1, :])
                    prob_grad = dot_nt(v4, grads)[0:key_rows]
                    delta = jnp.sum(probs * prob_grad, axis=0, keepdims=True)
                    score_grad = probs * (prob_grad - delta)
                    dbias_ref[t] += score_grad
                    prob_half = grow(probs).astype(bf16)
                    score_half = grow(score_grad).astype(bf16)
                    value_grad = dot_nn(prob_half, grads)
                    key_grad = dot_nn(score_half, queries)
                    query_grad = diagonal(dot_tn(score_half, k4)) * scale
                    add_small("qb", fold_rows(query_grad), 128 * t)
                    add_small("vb", fold_rows(value_grad), 128 * t)
                    qkv_ref[g2, line, cols_q] = query_grad.astype(bf16)
                    qkv_ref[g2, line, cols_k] = key_grad.astype(bf16)
                    qkv_ref[g2, line, cols_v] = value_grad.astype(bf16)

            @pl.loop(0, 3 * width // chunk)
            def _(n):
                cols = pl.ds(pl.multiple_of(n * chunk, chunk), chunk)
                part = dot_tn(act_w_ref[g2], qkv_ref[g2, :, cols])

                @pl.when(g2 == 0)
                def _():
                    dwqkv_ref[:, cols] = part

                @pl.when(g2 != 0)
                def _():
                    dwqkv_ref[:, cols] += part

            for n in range(width // chunk):
                cols = slice(n * chunk, (n + 1) * chunk)
                mixed_w_ref[:, cols] = dot_nt(qkv_ref[g2], wqkv_ref[cols, :]).astype(bf16)
            wide_ref[:, sub * s : sub * (s + 1), :] = dot_nn(back_ref[...], mixed_w_ref[...]).reshape(
                tokens, sub, width
            )

        @pl.loop(0, tokens // step)
        def _(n):
            part = x_ref[pl.ds(n * step, step), pl.ds(win0, group), :].astype(f32)
            normal, inverse = norm_parts(part.reshape(step * group, width))
            grad = wide_ref[pl.ds(n * step, step)].reshape(step * group, width)
            scaled = grad * gain1_ref[...]
            back = inverse * (
                scaled
                - jnp.mean(scaled, axis=-1, keepdims=True)
                - normal * jnp.mean(scaled * normal, axis=-1, keepdims=True)
            )
            dx_ref[pl.ds(n * step, step), pl.ds(win0, group), :] += back.reshape(step, group, width)
            add_small("g1", fold_rows(grad * normal))
            add_small("s1", fold_rows(grad))


def local_pass(x, dy, wqkv, wproj, w1, w2, vectors, bias, heads, shards):
    tokens, windows, width = x.shape
    hidden = w1.shape[1]
    dims = (tokens, windows, width, heads, hidden, shards)
    chips = shards // 2
    sub = 8
    pad = 64
    rows = tokens * 2 * sub
    small_size = 8 * width + hidden
    subs = windows // sub
    shapes = (
        jax.ShapeDtypeStruct(x.shape, bf16),
        jax.ShapeDtypeStruct(x.shape, f32),
        jax.ShapeDtypeStruct((width, 3 * width), f32),
        jax.ShapeDtypeStruct((width, width), f32),
        jax.ShapeDtypeStruct((width, hidden), f32),
        jax.ShapeDtypeStruct((width, hidden), f32),
        jax.ShapeDtypeStruct((8, small_size), f32),
        jax.ShapeDtypeStruct(bias.shape, f32),
    )
    vmem = pl.BlockSpec(memory_space=pltpu.VMEM)
    return pl.pallas_call(
        functools.partial(compute_kernel, dims),
        out_shape=shapes,
        in_specs=[vmem] * 2 + [pl.BlockSpec(memory_space=pl.ANY)] * 4 + [vmem] * 10,
        out_specs=[vmem] * len(shapes),
        scratch_shapes=[
            pltpu.VMEM((sub * pad, tokens * sub), bf16),
            pltpu.VMEM((tokens * sub, sub * pad), bf16),
            pltpu.VMEM((subs, sub * pad, width), bf16),
            pltpu.VMEM((subs, sub * pad, 3 * width), bf16),
            pltpu.VMEM((sub * pad, width), bf16),
            pltpu.VMEM(x.shape, bf16),
            pltpu.VMEM((subs, sub, heads // 4, 256), f32),
            pltpu.VMEM((tokens, 2 * sub, width), f32),
            pltpu.VMEM((rows, width), bf16),
            pltpu.VMEM((width, rows), bf16),
            pltpu.VMEM((width, rows), bf16),
            pltpu.VMEM((rows, 256), f32),
            pltpu.VMEM((rows, 256), f32),
            pltpu.VMEM((rows, hidden), bf16),
            pltpu.VMEM((rows, hidden), bf16),
            pltpu.VMEM((rows, width), f32),
            pltpu.VMEM((width, 3 * width), bf16),
            pltpu.VMEM((width, width), bf16),
            pltpu.VMEM((width, hidden), bf16),
            pltpu.VMEM((hidden, width), bf16),
            pltpu.SemaphoreType.DMA((4,)),
            pltpu.SemaphoreType.DMA((4, chips)),
            pltpu.SemaphoreType.DMA((4, chips)),
            pltpu.SemaphoreType.DMA((4, chips - 1)),
            pltpu.SemaphoreType.DMA((4, chips - 1)),
        ],
        compiler_params=pltpu.CompilerParams(
            vmem_limit_bytes=67043328, collective_id=0, has_side_effects=True
        ),
    )(x, dy, wqkv, wproj, w1, w2, *vectors, bias)


def on_device(
    shards,
    block_input,
    out_grad,
    qkv_weight,
    query_bias,
    value_bias,
    proj_weight,
    proj_bias,
    hidden_weight,
    hidden_bias,
    output_weight,
    output_bias,
    first_gain,
    first_shift,
    second_gain,
    second_shift,
    bias_table,
    table_index,
):
    windows, tokens, width = block_input.shape
    table_rows, heads = bias_table.shape
    hidden = hidden_bias.shape[0]
    scale = (width // heads) ** (-0.5)
    pairs = tokens * tokens
    one_hot = (
        table_index.T.reshape(pairs, 1) == lax.broadcasted_iota(jnp.int32, (pairs, table_rows), 1)
    ).astype(f32)
    by_pair = jnp.dot(one_hot, bias_table, precision=lax.Precision.HIGHEST)
    by_key = by_pair.reshape(tokens, tokens, heads).transpose(0, 2, 1)
    by_key = jnp.pad(by_key, ((0, 0), (0, 0), (0, 64 - tokens)))
    by_key = jnp.pad(by_key, ((0, 56 - tokens), (0, 0), (0, 0)), constant_values=-1e30)
    quads = heads // 4
    bias = by_key.reshape(56, quads, 256).transpose(1, 0, 2)
    zeros = jnp.zeros((width,), f32)
    ones = jnp.ones((2 * width,), f32)
    vectors = [
        v.reshape(1, -1)
        for v in (
            jnp.concatenate([query_bias, zeros, value_bias]),
            jnp.concatenate([jnp.full((width,), scale, f32), ones]),
            proj_bias,
            hidden_bias,
            output_bias,
            first_gain,
            first_shift,
            second_gain,
            second_shift,
        )
    ]
    y, dx, dwqkv, dwproj, dw1, dw2t, small, dbias = local_pass(
        jnp.transpose(block_input, (1, 0, 2)),
        jnp.transpose(out_grad, (1, 0, 2)),
        qkv_weight,
        proj_weight,
        hidden_weight,
        output_weight,
        vectors,
        bias,
        heads,
        shards,
    )
    dbias = dbias.transpose(1, 0, 2).reshape(56, heads, 64)[:tokens, :, :tokens]
    dbias = dbias.transpose(1, 0, 2).reshape(heads, pairs)
    bias_table_grad = jnp.dot(dbias, one_hot, precision=lax.Precision.HIGHEST).T
    shares = [
        lax.psum_scatter(g.astype(bf16), "shard", scatter_dimension=0, tiled=True)
        for g in (dwqkv, dwproj, dw1, dw2t.T)
    ]
    shares = [lax.psum(s, "rep").astype(f32) for s in shares]
    small, bias_table_grad = lax.psum(
        (jnp.sum(small, axis=0), bias_table_grad), ("shard", "rep")
    )
    cuts = [width, width, width, hidden, width, width, width, width, width]
    parts = []
    at = 0
    for size in cuts:
        parts.append(small[at : at + size])
        at += size
    qb, vb, pb, hb, ob, g1, s1, g2, s2 = parts
    return (
        jnp.transpose(y, (1, 0, 2)),
        jnp.transpose(dx, (1, 0, 2)),
        shares[0],
        qb,
        vb,
        shares[1],
        pb,
        shares[2],
        hb,
        shares[3],
        ob,
        g1,
        s1,
        g2,
        s2,
        bias_table_grad,
    )


def solution(mesh):
    rows = P(("shard", "rep"), None, None)
    cut = P("shard", None)
    full = P()
    return jax.shard_map(
        functools.partial(on_device, mesh.shape["shard"]),
        mesh=mesh,
        in_specs=(
            rows,
            rows,
            cut,
            full,
            full,
            cut,
            full,
            cut,
            full,
            cut,
            full,
            full,
            full,
            full,
            full,
            full,
            full,
        ),
        out_specs=(
            rows,
            rows,
            cut,
            full,
            full,
            cut,
            full,
            cut,
            full,
            cut,
            full,
            full,
            full,
            full,
            full,
            full,
        ),
        check_vma=False,
    )
```

```python
import functools

import jax
import jax.numpy as jnp
from jax import lax
from jax.experimental import pallas as pl
from jax.experimental.pallas import tpu as pltpu
from jax.sharding import PartitionSpec as P

epsilon = 1e-05
f32 = jnp.float32
bf16 = jnp.bfloat16


def dot_nn(a, b):
    return lax.dot_general(a, b, (((1,), (0,)), ((), ())), preferred_element_type=f32)


def dot_nt(a, b):
    return lax.dot_general(a, b, (((1,), (1,)), ((), ())), preferred_element_type=f32)


def dot_tn(a, b):
    return lax.dot_general(a, b, (((0,), (0,)), ((), ())), preferred_element_type=f32)


def norm_parts(values):
    center = values - jnp.mean(values, axis=-1, keepdims=True)
    inverse = lax.rsqrt(jnp.mean(center * center, axis=-1, keepdims=True) + epsilon)
    return center * inverse, inverse


def fold_rows(values):
    rows, cols = values.shape
    return jnp.sum(values.reshape(rows // 8, 8, cols), axis=0)


def gelu_pair(upper):
    bell = jnp.exp(upper * upper * -0.5)
    t = 1.0 / (1.0 + 0.23164189 * jnp.abs(upper))
    poly = t * (
        0.127414796
        + t * (-0.142248368 + t * (0.7107068705 + t * (-0.7265760135 + t * 0.5307027145)))
    )
    tail = poly * bell
    phi = jnp.where(upper >= 0.0, 1.0 - tail, tail)
    return upper * phi, phi + upper * bell * 0.3989422804014327


def compute_kernel(
    dims,
    x_hbm,
    dy_hbm,
    wqkv_shard,
    wproj_shard,
    w1_shard,
    w2_shard,
    query_bias_ref,
    value_bias_ref,
    proj_bias_ref,
    hidden_bias_ref,
    output_bias_ref,
    gain1_ref,
    shift1_ref,
    gain2_ref,
    shift2_ref,
    table_ref,
    index_ref,
    y_hbm,
    dx_hbm,
    mixed_hbm,
    work0_ref,
    work1_ref,
    work2_ref,
    total_ref,
    in_ref,
    y_ref,
    dx_ref,
    dwqkv_ref,
    dwproj_ref,
    dw1_ref,
    dw2t_ref,
    small_ref,
    dbias_ref,
    bias_ref,
    perm_ref,
    back_ref,
    act_w_ref,
    qkv_ref,
    mixed_w_ref,
    mixed_ref,
    lse_ref,
    wide_ref,
    sa_ref,
    sat_ref,
    dyt_ref,
    u0_ref,
    u1_ref,
    da_ref,
    act_ref,
    dup_ref,
    wqkv_ref,
    wproj_ref,
    w1_ref,
    w2_ref,
    out0_ref,
    in0_ref,
    in1_ref,
    in2_ref,
    far0_ref,
    far1_ref,
    far2_ref,
    half0_ref,
    half1_ref,
    half2_ref,
    total_in_ref,
    own_sem,
    pair_send,
    pair_recv,
    chip_send,
    chip_recv,
    load_sem,
    y_sem,
    mixed_sem,
    dx_sem,
    core_send,
    core_recv,
    far_send,
    far_recv,
    half_send,
    half_recv,
    join_send,
    join_recv,
    total_send,
    total_recv,
):
    tokens, windows, width, heads, hidden, shards, reps = dims
    me = lax.axis_index("shard")
    chips = shards // 2
    core = lax.rem(me, 2)
    chip = me // 2
    pair = chip * 2 + 1 - core

    def block(ref, index):
        size = ref.shape[0] // shards
        return ref.at[pl.ds(pl.multiple_of(index * size, size), size), :]

    def peer(k):
        return lax.rem(chip + k, chips) * 2 + core

    def owner(k, side):
        return lax.rem(chip + chips - k, chips) * 2 + side

    gathers = (
        (wqkv_shard, wqkv_ref),
        (wproj_shard, wproj_ref),
        (w1_shard, w1_ref),
        (w2_shard, w2_ref),
    )

    def own_copy(i):
        shard, full = gathers[i]
        return pltpu.make_async_copy(shard, block(full, me), own_sem.at[i])

    def chip_copy(i, k):
        shard, full = gathers[i]
        return pltpu.make_async_remote_copy(
            src_ref=shard,
            dst_ref=block(full, me),
            send_sem=chip_send.at[i, k - 1],
            recv_sem=chip_recv.at[i, k - 1],
            device_id={"shard": peer(k)},
            device_id_type=pl.DeviceIdType.MESH,
        )

    def pair_copy(i, k):
        shard, full = gathers[i]
        return pltpu.make_async_remote_copy(
            src_ref=shard if k == 0 else block(full, owner(k, core)),
            dst_ref=block(full, owner(k, core)),
            send_sem=pair_send.at[i, k],
            recv_sem=pair_recv.at[i, k],
            device_id={"shard": pair},
            device_id_type=pl.DeviceIdType.MESH,
        )

    def gather_start(i):
        own_copy(i).start()
        for k in range(1, chips):
            chip_copy(i, k).start()
        pair_copy(i, 0).start()

    def gather_finish(i):
        for k in range(1, chips):
            chip_copy(i, k).wait_recv()
            pair_copy(i, k).start()
        own_copy(i).wait()
        for k in range(chips):
            pair_copy(i, k).wait_recv()

    def gather_drain(i):
        for k in range(1, chips):
            chip_copy(i, k).wait_send()
        for k in range(chips):
            pair_copy(i, k).wait_send()

    rep = lax.axis_index("rep")
    bits = reps.bit_length() - 1

    def rep_bit(b):
        return lax.rem(rep // (1 << b), 2)

    def rep_peer(b):
        return rep + (1 - 2 * rep_bit(b)) * (1 << b)

    barrier = pltpu.get_barrier_semaphore()
    for target in [pair] + [peer(k) for k in range(1, chips)]:
        pl.semaphore_signal(
            barrier, inc=1, device_id={"shard": target}, device_id_type=pl.DeviceIdType.MESH
        )
    for b in range(bits):
        pl.semaphore_signal(
            barrier, inc=1, device_id={"rep": rep_peer(b)}, device_id_type=pl.DeviceIdType.MESH
        )
    pl.semaphore_wait(barrier, chips + bits)
    gather_start(0)
    gather_start(1)

    head_size = width // heads
    scale = head_size ** (-0.5)
    pad = 64
    key_rows = 56
    sub = 8
    group = 2 * sub
    groups = windows // group
    quad = 128 // head_size
    quads = heads // quad
    rows8 = tokens * sub
    rows = tokens * group
    rows_w = sub * pad
    chunk = 256
    step = 7
    lane_head = lax.broadcasted_iota(jnp.int32, (pad, 128), 1) // head_size
    head_masks = [(lane_head == h).astype(f32) for h in range(quad)]
    head_masks_half = [m.astype(bf16) for m in head_masks]

    base = {}
    at = 0
    for name, size in (
        ("qb", width),
        ("vb", width),
        ("pb", width),
        ("hb", hidden),
        ("ob", width),
        ("g1", width),
        ("s1", width),
        ("g2", width),
        ("s2", width),
    ):
        base[name] = (at, size)
        at += size

    def add_small(name, value, offset=0):
        start = base[name][0] + offset
        cols = pl.ds(start, value.shape[1])
        small_ref[:, cols] = small_ref[:, cols] + value

    def load(source, g, slot):
        return pltpu.make_async_copy(
            source.at[:, pl.ds(pl.multiple_of(g * group, group), group), :],
            in_ref.at[slot],
            load_sem.at[slot],
        )

    def store(source, target, g, sem):
        return pltpu.make_async_copy(
            source, target.at[:, pl.ds(pl.multiple_of(g * group, group), group), :], sem
        )

    def mixed_load(g):
        return pltpu.make_async_copy(
            mixed_hbm.at[:, pl.ds(pl.multiple_of(g * group, group), group), :], mixed_ref, mixed_sem
        )

    load(x_hbm, 0, 0).start()

    parts = hidden // (shards * chunk)
    owned = width // shards
    works = (work0_ref, work1_ref, work2_ref)
    ins = (in0_ref, in1_ref, in2_ref)
    fars = (far0_ref, far1_ref, far2_ref)
    halves = (half0_ref, half1_ref, half2_ref)

    def unit_pieces(u, s):
        own = pl.ds(pl.multiple_of(s * owned, owned), owned)
        if u == 2:
            for i in range(3):
                cols = slice(width * i, width * (i + 1))
                yield owned * i, owned, 0, width, (lambda cols=cols: dwqkv_ref[own, cols])
            return
        per = width // chunk
        for i in range(shards):
            n = i * parts + u
            cols = slice(n * chunk, (n + 1) * chunk)
            yield (
                owned * (i // per),
                owned,
                chunk * (i % per),
                chunk,
                (lambda cols=cols: dw1_ref[own, cols]),
            )
        at_row = owned * (shards // per)
        lanes = pl.ds(pl.multiple_of((s * parts + u) * chunk, chunk), chunk)
        yield at_row, chunk, 0, width, (lambda: dw2t_ref[:, lanes].T)
        if u == 1:
            yield at_row + chunk, owned, 0, width, (lambda: dwproj_ref[own, :])

    def unit_out(u, j):
        rows_u = works[u].shape[0]
        if u == 0:
            return mixed_w_ref.at[0:rows_u] if j == 0 else out0_ref.at[j - 1]
        first = 0 if u == 1 else chips * width
        return act_ref.at[0:rows_u, first + j * width : first + (j + 1) * width]

    def core_copy(u, j):
        return pltpu.make_async_remote_copy(
            src_ref=unit_out(u, j),
            dst_ref=ins[u].at[j],
            send_sem=core_send.at[u, j],
            recv_sem=core_recv.at[u, j],
            device_id={"shard": pair},
            device_id_type=pl.DeviceIdType.MESH,
        )

    def far_copy(u, k):
        return pltpu.make_async_remote_copy(
            src_ref=ins[u].at[lax.rem(chip + k, chips)],
            dst_ref=fars[u].at[k - 1],
            send_sem=far_send.at[u, k - 1],
            recv_sem=far_recv.at[u, k - 1],
            device_id={"shard": peer(k)},
            device_id_type=pl.DeviceIdType.MESH,
        )

    def halvings(u):
        rows_u = works[u].shape[0]
        count = 0
        while count < bits and rows_u % (16 << (count + 1)) == 0:
            count += 1
        return count

    def region(u, b):
        rows_u = works[u].shape[0]
        start = 0
        for i in range(min(b, halvings(u))):
            rows_u //= 2
            start = start + rep_bit(i) * rows_u
        if not isinstance(start, int):
            start = pl.multiple_of(start, 16)
        return start, rows_u

    def half_base(u, b):
        base_row = 0
        for i in range(b):
            _, length = region(u, i)
            base_row += length // 2 if i < halvings(u) else length
        return base_row

    def half_copy(u, b):
        start, length = region(u, b)
        if b < halvings(u):
            length //= 2
            start = pl.multiple_of(start + (1 - rep_bit(b)) * length, 16)
        return pltpu.make_async_remote_copy(
            src_ref=ins[u].at[chip, pl.ds(start, length), :],
            dst_ref=halves[u].at[pl.ds(half_base(u, b), length), :],
            send_sem=half_send.at[u, b],
            recv_sem=half_recv.at[u, b],
            device_id={"rep": rep_peer(b)},
            device_id_type=pl.DeviceIdType.MESH,
        )

    def half_add(u, b):
        half_copy(u, b).wait()
        start, length = region(u, b + 1)
        got = halves[u][pl.ds(half_base(u, b), length), :].astype(f32)
        lines = pl.ds(start, length)
        out = (ins[u][chip, lines, :].astype(f32) + got).astype(bf16)
        if b < bits - 1:
            ins[u][chip, lines, :] = out
        else:
            works[u][lines, :] = out

    def join_copy(u, b):
        start, length = region(u, b + 1)
        lines = pl.ds(start, length)
        return pltpu.make_async_remote_copy(
            src_ref=works[u].at[lines, :],
            dst_ref=works[u].at[lines, :],
            send_sem=join_send.at[u, b],
            recv_sem=join_recv.at[u, b],
            device_id={"rep": rep_peer(b)},
            device_id_type=pl.DeviceIdType.MESH,
        )

    def unit_stage(u, stage):
        if stage == 0:
            for j in range(chips):
                target = unit_out(u, j)
                for r0, nr, c0, nc, value in unit_pieces(u, 2 * j + 1 - core):
                    target[r0 : r0 + nr, c0 : c0 + nc] = value().astype(bf16)
                core_copy(u, j).start()
            return
        if stage == 1:
            for j in range(chips):
                core_copy(u, j).wait()
            for k in range(1, chips):
                j = lax.rem(chip + k, chips)
                for r0, nr, c0, nc, value in unit_pieces(u, 2 * j + core):
                    got = ins[u][j, r0 : r0 + nr, c0 : c0 + nc].astype(f32)
                    ins[u][j, r0 : r0 + nr, c0 : c0 + nc] = (value() + got).astype(bf16)
                far_copy(u, k).start()
            for r0, nr, c0, nc, value in unit_pieces(u, me):
                got = ins[u][chip, r0 : r0 + nr, c0 : c0 + nc].astype(f32)
                ins[u][chip, r0 : r0 + nr, c0 : c0 + nc] = (value() + got).astype(bf16)
            return
        if stage == 2:
            for k in range(1, chips):
                far_copy(u, k).wait()
            total = ins[u][chip].astype(f32)
            for k in range(1, chips):
                total = total + fars[u][k - 1].astype(f32)
            ins[u][chip] = total.astype(bf16)
        if 2 < stage <= 2 + bits:
            half_add(u, stage - 3)
        if 2 <= stage < 2 + bits:
            half_copy(u, stage - 2).start()
            return
        joins = [b for b in range(bits) if b < halvings(u)][::-1]
        at_join = stage - 2 - bits
        if 0 < at_join <= len(joins):
            join_copy(u, joins[at_join - 1]).wait()
        if at_join < len(joins):
            join_copy(u, joins[at_join]).start()

    stages = 3 + 2 * bits

    def unit_run(u, first, last=None):
        for stage in range(first, stages if last is None else last + 1):
            unit_stage(u, stage)

    def total_copy(b):
        rows_t = total_ref.shape[0]
        if b == 0:
            target = {"shard": pair}
        elif b == 1:
            target = {"shard": peer(1)}
        else:
            target = {"rep": rep_peer(b - 2)}
        return pltpu.make_async_remote_copy(
            src_ref=total_ref,
            dst_ref=total_in_ref.at[b],
            send_sem=total_send.at[b],
            recv_sem=total_recv.at[b],
            device_id=target,
            device_id_type=pl.DeviceIdType.MESH,
        )

    def total_add(b):
        total_copy(b).wait()
        total_ref[...] = total_ref[...] + total_in_ref[b]

    small_ref[...] = jnp.zeros(small_ref.shape, f32)
    dbias_ref[...] = jnp.zeros(dbias_ref.shape, f32)

    @pl.loop(0, rows_w // 64)
    def _(n):
        start = pl.multiple_of(n * 64, 64)
        to = lax.broadcasted_iota(jnp.int32, (64, rows8), 0) + start
        source = lax.broadcasted_iota(jnp.int32, (64, rows8), 1)
        hit = (to // pad == source % sub) & (to % pad == source // sub)
        perm_ref[pl.ds(start, 64), :] = hit.astype(f32).astype(bf16)

    @pl.loop(0, rows8 // 56)
    def _(n):
        start = pl.multiple_of(n * 56, 8)
        to = lax.broadcasted_iota(jnp.int32, (56, rows_w), 0) + start
        source = lax.broadcasted_iota(jnp.int32, (56, rows_w), 1)
        hit = (source // pad == to % sub) & (source % pad == to // sub)
        back_ref[pl.ds(start, 56), :] = hit.astype(f32).astype(bf16)

    table_lanes = table_ref.shape[1]
    row_iota = lax.broadcasted_iota(jnp.int32, (table_lanes, 128), 0)
    low_lanes = lax.broadcasted_iota(jnp.int32, (key_rows, 128), 1) < pad

    def named(j):
        return (row_iota == index_ref[pl.ds(j, 1), :]).astype(f32).astype(bf16)

    table = table_ref[...]
    high = table.astype(bf16)
    middle = (table - high.astype(f32)).astype(bf16)
    low = (table - high.astype(f32) - middle.astype(f32)).astype(bf16)
    upper_heads = heads // 2
    sides = (u0_ref, u1_ref)
    for side in sides:
        side[0 : upper_heads * key_rows, :] = jnp.full((upper_heads * key_rows, 128), -1e30, f32)

    def plane(h):
        row = (h % upper_heads) * key_rows
        return sides[h // upper_heads].at[row : row + key_rows, :]

    @pl.loop(0, tokens)
    def _(j):
        hit = named(j)
        line = (dot_nn(high, hit) + dot_nn(middle, hit)) + dot_nn(low, hit)
        for side in range(2):
            sides[side][pl.ds(j, upper_heads, stride=key_rows), :] = line[
                side * upper_heads : (side + 1) * upper_heads
            ]

    for t in range(quads):
        for h in range(quad // 2):
            left = plane(t * quad + 2 * h)[...]
            right = plane(t * quad + 2 * h + 1)[...]
            bias_ref[t, :, 128 * h : 128 * (h + 1)] = jnp.where(
                low_lanes, left, pltpu.roll(right, pad, 1)
            )

    def stacked(tile):
        return jnp.concatenate([tile * m for m in head_masks_half], axis=0)

    def diagonal(tall):
        total = tall[0:pad] * head_masks[0]
        for h in range(1, quad):
            total = total + tall[h * pad : (h + 1) * pad] * head_masks[h]
        return total

    def grow(values):
        return jnp.concatenate([values, jnp.zeros((pad - key_rows, values.shape[1]), f32)], axis=0)

    @pl.loop(0, groups)
    def _(g):
        win0 = pl.multiple_of(g * group, group)
        slot = lax.rem(g, 2)
        load(x_hbm, g, slot).wait()

        @pl.when(g < groups - 1)
        def _():
            load(x_hbm, g + 1, 1 - slot).start()

        @pl.when(g == groups - 1)
        def _():
            load(dy_hbm, 0, 1 - slot).start()

        @pl.loop(0, tokens // step)
        def _(n):
            part = in_ref[slot, pl.ds(n * step, step)].astype(f32)
            flat = part.reshape(step * group, width)
            normal, _ = norm_parts(flat)
            wide_ref[pl.ds(n * step, step)] = (normal * gain1_ref[...] + shift1_ref[...]).reshape(
                step, group, width
            )

        for s in range(2):
            g2 = g * 2 + s
            act8 = wide_ref[:, sub * s : sub * (s + 1), :].reshape(rows8, width).astype(bf16)
            act_w_ref[g2] = dot_nn(perm_ref[...], act8).astype(bf16)
            if s == 0:

                @pl.when(g == 0)
                def _():
                    gather_finish(0)
                    gather_finish(1)
                    gather_start(2)
                    gather_start(3)

            for n in range(3 * width // chunk):
                cols = slice(n * chunk, (n + 1) * chunk)
                out = dot_nn(act_w_ref[g2], wqkv_ref[:, cols])
                if n < width // chunk:
                    out = (out + query_bias_ref[:, cols]) * scale
                if n >= 2 * width // chunk:
                    first = n * chunk - 2 * width
                    out = out + value_bias_ref[:, first : first + chunk]
                qkv_ref[g2, :, cols] = out.astype(bf16)

            @pl.loop(0, sub)
            def _(w):
                line = pl.ds(pl.multiple_of(w * pad, pad), pad)
                for t in range(quads):
                    q4 = qkv_ref[g2, line, 128 * t : 128 * (t + 1)]
                    k4 = qkv_ref[g2, line, width + 128 * t : width + 128 * (t + 1)]
                    v4 = qkv_ref[g2, line, 2 * width + 128 * t : 2 * width + 128 * (t + 1)]
                    scores = dot_nt(k4, stacked(q4))[0:key_rows] + bias_ref[t]
                    top = jnp.max(scores, axis=0, keepdims=True)
                    weight = jnp.exp(scores - top)
                    total = jnp.sum(weight, axis=0, keepdims=True)
                    lse_ref[g2, w, t : t + 1, :] = top + jnp.log(total)
                    probs = grow(weight * (1.0 / total)).astype(bf16)
                    mixed_w_ref[line, 128 * t : 128 * (t + 1)] = diagonal(dot_tn(probs, v4)).astype(
                        bf16
                    )

            wide_ref[:, sub * s : sub * (s + 1), :] = dot_nn(back_ref[...], mixed_w_ref[...]).reshape(
                tokens, sub, width
            )

        @pl.when(g != 0)
        def _():
            store(mixed_ref, mixed_hbm, g - 1, mixed_sem).wait()

        mixed_ref[...] = wide_ref[...].astype(bf16)
        store(mixed_ref, mixed_hbm, g, mixed_sem).start()
        mixed = mixed_ref[...].reshape(rows, width)
        for n in range(width // chunk):
            cols = slice(n * chunk, (n + 1) * chunk)
            out = dot_nn(mixed, wproj_ref[:, cols]) + proj_bias_ref[:, cols]
            dx_ref[:, pl.ds(win0, group), cols] = in_ref[slot, :, :, cols].astype(
                f32
            ) + out.reshape(tokens, group, chunk)

    gather_finish(2)
    gather_finish(3)
    for i in range(4):
        gather_drain(i)
    store(mixed_ref, mixed_hbm, groups - 1, mixed_sem).wait()

    @pl.loop(0, groups)
    def _(g):
        win0 = pl.multiple_of(g * group, group)
        slot = lax.rem(groups + g, 2)
        load(dy_hbm, g, slot).wait()

        @pl.when(g < groups - 1)
        def _():
            load(dy_hbm, g + 1, 1 - slot).start()

        @pl.when(g == groups - 1)
        def _():
            load(x_hbm, 0, 1 - slot).start()

        @pl.when(g != 0)
        def _():
            store(y_ref, y_hbm, g - 1, y_sem).wait()

        mixed_load(g).start()

        @pl.loop(0, tokens // step)
        def _(n):
            part = dx_ref[pl.ds(n * step, step), pl.ds(win0, group), :].reshape(step * group, width)
            normal, _ = norm_parts(part)
            lines = pl.ds(pl.multiple_of(n * step * group, step * group), step * group)
            sa_ref[lines, :] = (normal * gain2_ref[...] + shift2_ref[...]).astype(bf16)

        sat_ref[...] = sa_ref[...].T
        dyt_ref[...] = in_ref[slot].reshape(rows, width).T

        @pl.loop(0, hidden // chunk)
        def _(i):
            n = lax.rem(i, shards) * parts + i // shards
            start = pl.multiple_of(n * chunk, chunk)
            cols = pl.ds(start, chunk)
            u = dot_nn(sa_ref[...], w1_ref[:, cols])
            u0_ref[...] = u[:, 0:128]
            u1_ref[...] = u[:, 128:256]
            da_ref[...] = dot_nt(in_ref[slot].reshape(rows, width), w2_ref[cols, :])

            @pl.loop(0, tokens // step)
            def _(m):
                lines = pl.ds(pl.multiple_of(m * step * group, step * group), step * group)
                value, slope = gelu_pair(
                    jnp.concatenate([u0_ref[lines, :], u1_ref[lines, :]], axis=1)
                    + hidden_bias_ref[:, cols]
                )
                act_ref[lines, cols] = value.astype(bf16)
                dup = (da_ref[lines, :] * slope).astype(bf16)
                dup_ref[lines, cols] = dup
                add_small("hb", fold_rows(dup.astype(f32)), start)

            part1 = dot_nn(sat_ref[...], dup_ref[:, cols])
            part2 = dot_nn(dyt_ref[...], act_ref[:, cols])

            @pl.when(g == 0)
            def _():
                dw1_ref[:, cols] = part1
                dw2t_ref[:, cols] = part2

            @pl.when(g != 0)
            def _():
                dw1_ref[:, cols] += part1
                dw2t_ref[:, cols] += part2

            @pl.when((g == groups - 1) & (i == shards - 1))
            def _():
                unit_stage(0, 0)

        for n in range(width // chunk):
            cols = slice(n * chunk, (n + 1) * chunk)
            out = dot_nn(act_ref[...], w2_ref[:, cols]) + output_bias_ref[:, cols]
            y_ref[:, :, cols] = (
                dx_ref[:, pl.ds(win0, group), cols] + out.reshape(tokens, group, chunk)
            ).astype(bf16)
            wide_ref[:, :, cols] = dot_nt(dup_ref[...], w1_ref[cols, :]).reshape(
                tokens, group, chunk
            )

        store(y_ref, y_hbm, g, y_sem).start()

        @pl.loop(0, tokens // step)
        def _(n):
            lines = pl.ds(pl.multiple_of(n * step * group, step * group), step * group)
            normal, inverse = norm_parts(
                dx_ref[pl.ds(n * step, step), pl.ds(win0, group), :].reshape(step * group, width)
            )
            grad = wide_ref[pl.ds(n * step, step)].reshape(step * group, width)
            scaled = grad * gain2_ref[...]
            back = inverse * (
                scaled
                - jnp.mean(scaled, axis=-1, keepdims=True)
                - normal * jnp.mean(scaled * normal, axis=-1, keepdims=True)
            )
            cot = in_ref[slot, pl.ds(n * step, step)].astype(f32).reshape(step * group, width)
            total = cot + back
            dx_ref[pl.ds(n * step, step), pl.ds(win0, group), :] = total.reshape(step, group, width)
            sa_ref[lines, :] = total.astype(bf16)
            add_small("ob", fold_rows(cot))
            add_small("pb", fold_rows(total))
            add_small("g2", fold_rows(grad * normal))
            add_small("s2", fold_rows(grad))

        mixed_load(g).wait()
        part3 = dot_tn(mixed_ref[...].reshape(rows, width), sa_ref[...])

        @pl.when(g == 0)
        def _():
            dwproj_ref[...] = part3

        @pl.when(g != 0)
        def _():
            dwproj_ref[...] += part3

    store(y_ref, y_hbm, groups - 1, y_sem).wait()
    unit_stage(0, 1)
    unit_stage(1, 0)

    plan = {
        0: ((1, 1),),
        1: ((0, 2),),
        2: ((0, 3),),
        3: ((0, 4), (1, 2)),
        4: ((0, 5), (1, 3)),
        5: ((0, 6), (1, 4)),
    }
    plan_last = 5

    @pl.loop(0, groups)
    def _(g):
        win0 = pl.multiple_of(g * group, group)
        wide_ref[...] = dx_ref[:, pl.ds(win0, group), :]
        for s in range(2):
            g2 = g * 2 + s
            half8 = wide_ref[:, sub * s : sub * (s + 1), :].reshape(rows8, width).astype(bf16)
            half_w = dot_nn(perm_ref[...], half8).astype(bf16)
            mixed_w_ref[...] = dot_nt(half_w, wproj_ref[...]).astype(bf16)

            for point, calls in plan.items():
                if point % 2 == s:

                    @pl.when(g2 == point)
                    def _():
                        for u, stage in calls:
                            unit_stage(u, stage)

            @pl.loop(0, sub)
            def _(w):
                line = pl.ds(pl.multiple_of(w * pad, pad), pad)
                for t in range(quads):
                    cols_q = slice(128 * t, 128 * (t + 1))
                    cols_k = slice(width + 128 * t, width + 128 * (t + 1))
                    cols_v = slice(2 * width + 128 * t, 2 * width + 128 * (t + 1))
                    q4 = qkv_ref[g2, line, cols_q]
                    k4 = qkv_ref[g2, line, cols_k]
                    v4 = qkv_ref[g2, line, cols_v]
                    go4 = mixed_w_ref[line, cols_q]
                    queries = stacked(q4)
                    grads = stacked(go4)
                    scores = dot_nt(k4, queries)[0:key_rows] + bias_ref[t]
                    probs = jnp.exp(scores - lse_ref[g2, w, t : t + 1, :])
                    prob_grad = dot_nt(v4, grads)[0:key_rows]
                    delta = jnp.sum(probs * prob_grad, axis=0, keepdims=True)
                    score_grad = probs * (prob_grad - delta)
                    dbias_ref[t] += score_grad
                    prob_half = grow(probs).astype(bf16)
                    score_half = grow(score_grad).astype(bf16)
                    value_grad = dot_nn(prob_half, grads)
                    key_grad = dot_nn(score_half, queries)
                    query_grad = diagonal(dot_tn(score_half, k4)) * scale
                    add_small("qb", fold_rows(query_grad), 128 * t)
                    add_small("vb", fold_rows(value_grad), 128 * t)
                    qkv_ref[g2, line, cols_q] = query_grad.astype(bf16)
                    qkv_ref[g2, line, cols_k] = key_grad.astype(bf16)
                    qkv_ref[g2, line, cols_v] = value_grad.astype(bf16)

            @pl.loop(0, 3 * width // chunk)
            def _(n):
                cols = pl.ds(pl.multiple_of(n * chunk, chunk), chunk)
                part = dot_tn(act_w_ref[g2], qkv_ref[g2, :, cols])

                @pl.when(g2 == 0)
                def _():
                    dwqkv_ref[:, cols] = part

                @pl.when(g2 != 0)
                def _():
                    dwqkv_ref[:, cols] += part

    unit_stage(2, 0)
    unit_stage(0, 7)
    unit_stage(1, 5)

    for t in range(quads):
        for h in range(quad // 2):
            both = dbias_ref[t, :, 128 * h : 128 * (h + 1)]
            plane(t * quad + 2 * h)[...] = jnp.where(low_lanes, both, 0.0)
            plane(t * quad + 2 * h + 1)[...] = jnp.where(
                low_lanes, pltpu.roll(both, pad, 1), 0.0
            )
    total_ref[...] = jnp.zeros(total_ref.shape, f32)

    @pl.loop(0, tokens)
    def _(j):
        hit = named(j)
        line = jnp.concatenate(
            [side[pl.ds(j, upper_heads, stride=key_rows), :] for side in sides], axis=0
        )
        upper_half = line.astype(bf16)
        lower_half = (line - upper_half.astype(f32)).astype(bf16)
        total_ref[0:heads, 0:table_lanes] = total_ref[0:heads, 0:table_lanes] + (
            dot_nt(upper_half, hit) + dot_nt(lower_half, hit)
        )

    @pl.loop(0, groups)
    def _(g):
        win0 = pl.multiple_of(g * group, group)
        slot = lax.rem(2 * groups + g, 2)
        load(x_hbm, g, slot).wait()

        @pl.when(g < groups - 1)
        def _():
            load(x_hbm, g + 1, 1 - slot).start()

        for s in range(2):
            g2 = g * 2 + s
            for n in range(width // chunk):
                cols = slice(n * chunk, (n + 1) * chunk)
                mixed_w_ref[:, cols] = dot_nt(qkv_ref[g2], wqkv_ref[cols, :]).astype(bf16)
            wide_ref[:, sub * s : sub * (s + 1), :] = dot_nn(back_ref[...], mixed_w_ref[...]).reshape(
                tokens, sub, width
            )

        for point, calls in {
            0: ((2, 1), (0, 8), (1, 6)),
            1: ((2, 2), (1, 7)),
            2: ((2, 3), (1, 8)),
        }.items():

            @pl.when(g == point)
            def _():
                for u, stage in calls:
                    unit_stage(u, stage)

        @pl.loop(0, tokens // step)
        def _(n):
            part = in_ref[slot, pl.ds(n * step, step)].astype(f32)
            normal, inverse = norm_parts(part.reshape(step * group, width))
            grad = wide_ref[pl.ds(n * step, step)].reshape(step * group, width)
            scaled = grad * gain1_ref[...]
            back = inverse * (
                scaled
                - jnp.mean(scaled, axis=-1, keepdims=True)
                - normal * jnp.mean(scaled * normal, axis=-1, keepdims=True)
            )
            dx_ref[pl.ds(n * step, step), pl.ds(win0, group), :] += back.reshape(step, group, width)
            add_small("g1", fold_rows(grad * normal))
            add_small("s1", fold_rows(grad))

        store(dx_ref.at[:, pl.ds(win0, group), :], dx_hbm, g, dx_sem.at[g]).start()

    for i in range(small_ref.shape[1] // width):
        total_ref[heads + i : heads + i + 1, :] = jnp.sum(
            small_ref[:, i * width : (i + 1) * width], axis=0, keepdims=True
        )
    steps = 2 + bits
    total_copy(0).start()
    for stage in range(4, stages):
        unit_stage(2, stage)
        b = stage - 4
        if b < steps:
            total_add(b)
            if b + 1 < steps:
                total_copy(b + 1).start()
    for u in (0, 1):
        unit_run(u, 9)
    for b in range(stages - 4, steps):
        total_add(b)
        if b + 1 < steps:
            total_copy(b + 1).start()
    for g in range(groups):
        store(dx_ref.at[:, g * group : (g + 1) * group, :], dx_hbm, g, dx_sem.at[g]).wait()


def local_pass(x, dy, wqkv, wproj, w1, w2, vectors, table, index, shards, reps):
    tokens, windows, width = x.shape
    hidden = w1.shape[1]
    heads = table.shape[0]
    dims = (tokens, windows, width, heads, hidden, shards, reps)
    chips = shards // 2
    bits = reps.bit_length() - 1
    sub = 8
    group = 2 * sub
    pad = 64
    rows = tokens * group
    small_size = 8 * width + hidden
    subs = windows // sub
    owned = width // shards
    unit_rows = (
        (width * hidden) // (shards * width),
        (width * hidden) // (shards * width) + owned,
        3 * owned,
    )
    total_rows = -(-(heads + small_size // width) // 8) * 8
    shapes = (
        [
            jax.ShapeDtypeStruct(x.shape, bf16),
            jax.ShapeDtypeStruct(x.shape, f32),
            jax.ShapeDtypeStruct(x.shape, bf16),
        ]
        + [jax.ShapeDtypeStruct((r, width), bf16) for r in unit_rows]
        + [jax.ShapeDtypeStruct((total_rows, width), f32)]
    )
    vmem = pl.BlockSpec(memory_space=pltpu.VMEM)
    hbm = pl.BlockSpec(memory_space=pl.ANY)

    def half_rows(r):
        total = 0
        for _ in range(bits):
            if r % 32 == 0:
                r //= 2
            total += r
        return total

    return pl.pallas_call(
        functools.partial(compute_kernel, dims),
        out_shape=shapes,
        in_specs=[hbm] * 6 + [vmem] * 11,
        out_specs=[hbm] * 3 + [vmem] * 4,
        scratch_shapes=[
            pltpu.VMEM((2, tokens, group, width), bf16),
            pltpu.VMEM((tokens, group, width), bf16),
            pltpu.VMEM(x.shape, f32),
            pltpu.VMEM((width, 3 * width), f32),
            pltpu.VMEM((width, width), f32),
            pltpu.VMEM((width, hidden), f32),
            pltpu.VMEM((width, hidden), f32),
            pltpu.VMEM((8, small_size), f32),
            pltpu.VMEM((heads // 4, 56, 256), f32),
            pltpu.VMEM((heads // 4, 56, 256), f32),
            pltpu.VMEM((sub * pad, tokens * sub), bf16),
            pltpu.VMEM((tokens * sub, sub * pad), bf16),
            pltpu.VMEM((subs, sub * pad, width), bf16),
            pltpu.VMEM((subs, sub * pad, 3 * width), bf16),
            pltpu.VMEM((sub * pad, width), bf16),
            pltpu.VMEM((tokens, group, width), bf16),
            pltpu.VMEM((subs, sub, heads // 4, 256), f32),
            pltpu.VMEM((tokens, group, width), f32),
            pltpu.VMEM((rows, width), bf16),
            pltpu.VMEM((width, rows), bf16),
            pltpu.VMEM((width, rows), bf16),
            pltpu.VMEM((rows, 128), f32),
            pltpu.VMEM((rows, 128), f32),
            pltpu.VMEM((rows, 256), f32),
            pltpu.VMEM((rows, hidden), bf16),
            pltpu.VMEM((rows, hidden), bf16),
            pltpu.VMEM((width, 3 * width), bf16),
            pltpu.VMEM((width, width), bf16),
            pltpu.VMEM((width, hidden), bf16),
            pltpu.VMEM((hidden, width), bf16),
            pltpu.VMEM((chips - 1, unit_rows[0], width), bf16),
            *[pltpu.VMEM((chips, r, width), bf16) for r in unit_rows],
            *[pltpu.VMEM((chips - 1, r, width), bf16) for r in unit_rows],
            *[pltpu.VMEM((half_rows(r), width), bf16) for r in unit_rows],
            pltpu.VMEM((2 + bits, total_rows, width), f32),
            pltpu.SemaphoreType.DMA((4,)),
            pltpu.SemaphoreType.DMA((4, chips)),
            pltpu.SemaphoreType.DMA((4, chips)),
            pltpu.SemaphoreType.DMA((4, chips - 1)),
            pltpu.SemaphoreType.DMA((4, chips - 1)),
            pltpu.SemaphoreType.DMA((2,)),
            pltpu.SemaphoreType.DMA,
            pltpu.SemaphoreType.DMA,
            pltpu.SemaphoreType.DMA((windows // group,)),
            pltpu.SemaphoreType.DMA((3, chips)),
            pltpu.SemaphoreType.DMA((3, chips)),
            pltpu.SemaphoreType.DMA((3, chips - 1)),
            pltpu.SemaphoreType.DMA((3, chips - 1)),
            pltpu.SemaphoreType.DMA((3, bits)),
            pltpu.SemaphoreType.DMA((3, bits)),
            pltpu.SemaphoreType.DMA((3, bits)),
            pltpu.SemaphoreType.DMA((3, bits)),
            pltpu.SemaphoreType.DMA((2 + bits,)),
            pltpu.SemaphoreType.DMA((2 + bits,)),
        ],
        compiler_params=pltpu.CompilerParams(
            vmem_limit_bytes=67043328, collective_id=0, has_side_effects=True
        ),
    )(x, dy, wqkv, wproj, w1, w2, *vectors, table, index)


def on_device(
    shards,
    reps,
    block_input,
    out_grad,
    qkv_weight,
    query_bias,
    value_bias,
    proj_weight,
    proj_bias,
    hidden_weight,
    hidden_bias,
    output_weight,
    output_bias,
    first_gain,
    first_shift,
    second_gain,
    second_shift,
    bias_table,
    table_index,
):
    windows, tokens, width = block_input.shape
    table_rows, heads = bias_table.shape
    hidden = hidden_bias.shape[0]
    chunk = 256
    vectors = [
        v.reshape(1, -1)
        for v in (
            query_bias,
            value_bias,
            proj_bias,
            hidden_bias,
            output_bias,
            first_gain,
            first_shift,
            second_gain,
            second_shift,
        )
    ]
    table = jnp.pad(bias_table.T, ((0, 0), (0, 256 - table_rows)))
    index = jnp.pad(
        table_index.T, ((0, 56 - tokens), (0, 128 - tokens)), constant_values=-1
    )
    y, dx, _, work0, work1, work2, total = local_pass(
        jnp.transpose(block_input, (1, 0, 2)),
        jnp.transpose(out_grad, (1, 0, 2)),
        qkv_weight,
        proj_weight,
        hidden_weight,
        output_weight,
        vectors,
        table,
        index,
        shards,
        reps,
    )
    owned = width // shards
    parts = hidden // (shards * chunk)
    per = width // chunk
    first_rows = owned * (shards // per)
    works = (work0, work1)
    dw1 = jnp.stack(
        [w[:first_rows].reshape(shards // per, owned, per, chunk) for w in works[:parts]]
    )
    dw1 = dw1.transpose(2, 1, 3, 0, 4).reshape(owned, hidden)
    dw2 = jnp.concatenate([w[first_rows : first_rows + chunk] for w in works[:parts]], axis=0)
    dwproj = work1[first_rows + chunk :]
    dwqkv = work2.reshape(3, owned, width).transpose(1, 0, 2).reshape(owned, 3 * width)
    sums = total[heads : heads + (8 * width + hidden) // width].reshape(-1)
    cuts = [width, width, width, hidden, width, width, width, width, width]
    split = []
    at = 0
    for size in cuts:
        split.append(sums[at : at + size])
        at += size
    qb, vb, pb, hb, ob, g1, s1, g2, s2 = split
    return (
        jnp.transpose(y, (1, 0, 2)),
        jnp.transpose(dx, (1, 0, 2)),
        dwqkv.astype(f32),
        qb,
        vb,
        dwproj.astype(f32),
        pb,
        dw1.astype(f32),
        hb,
        dw2.astype(f32),
        ob,
        g1,
        s1,
        g2,
        s2,
        total[:heads, :table_rows].T,
    )


def solution(mesh):
    rows = P(("shard", "rep"), None, None)
    cut = P("shard", None)
    full = P()
    return jax.shard_map(
        functools.partial(on_device, mesh.shape["shard"], mesh.shape["rep"]),
        mesh=mesh,
        in_specs=(
            rows,
            rows,
            cut,
            full,
            full,
            cut,
            full,
            cut,
            full,
            cut,
            full,
            full,
            full,
            full,
            full,
            full,
            full,
        ),
        out_specs=(
            rows,
            rows,
            cut,
            full,
            full,
            cut,
            full,
            cut,
            full,
            cut,
            full,
            full,
            full,
            full,
            full,
            full,
        ),
        check_vma=False,
    )
```

```python
import functools

import jax
import jax.numpy as jnp
from jax import lax
from jax.experimental import pallas as pl
from jax.experimental.pallas import tpu as pltpu
from jax.sharding import PartitionSpec as P

epsilon = 1e-05
f32 = jnp.float32
bf16 = jnp.bfloat16


def dot_nn(a, b):
    return lax.dot_general(a, b, (((1,), (0,)), ((), ())), preferred_element_type=f32)


def dot_nt(a, b):
    return lax.dot_general(a, b, (((1,), (1,)), ((), ())), preferred_element_type=f32)


def dot_tn(a, b):
    return lax.dot_general(a, b, (((0,), (0,)), ((), ())), preferred_element_type=f32)


def norm_parts(values):
    center = values - jnp.mean(values, axis=-1, keepdims=True)
    inverse = lax.rsqrt(jnp.mean(center * center, axis=-1, keepdims=True) + epsilon)
    return center * inverse, inverse


def fold_rows(values):
    rows, cols = values.shape
    return jnp.sum(values.reshape(rows // 8, 8, cols), axis=0)


def gelu_pair(upper):
    phi = 0.5 + 0.5 * lax.erf(upper * 0.7071067811865476)
    bell = jnp.exp(upper * upper * -0.5) * 0.3989422804014327
    return upper * phi, phi + upper * bell


def compute_kernel(
    dims,
    x_hbm,
    dy_hbm,
    wqkv_shard,
    wproj_shard,
    w1_shard,
    w2_shard,
    query_bias_ref,
    value_bias_ref,
    proj_bias_ref,
    hidden_bias_ref,
    output_bias_ref,
    gain1_ref,
    shift1_ref,
    gain2_ref,
    shift2_ref,
    table_ref,
    index_ref,
    y_hbm,
    dx_hbm,
    mixed_hbm,
    act_w_hbm,
    work0_ref,
    work1_ref,
    work2_ref,
    work3_ref,
    work4_ref,
    work5_ref,
    total_ref,
    in_ref,
    y_ref,
    dx_ref,
    dwqkv_ref,
    dwproj_ref,
    dw1_ref,
    dw2t_ref,
    small_ref,
    dbias_ref,
    bias_ref,
    perm_ref,
    back_ref,
    act_w_ref,
    qkv_ref,
    mixed_w_ref,
    mixed_ref,
    lse_ref,
    wide_ref,
    sa_ref,
    sat_ref,
    dyt_ref,
    u_ref,
    da_ref,
    plane_ref,
    names_ref,
    rows_ref,
    act_ref,
    dup_ref,
    wqkv_ref,
    wproj_ref,
    w1_ref,
    w2_ref,
    out0_ref,
    in0_ref,
    in1_ref,
    in2_ref,
    in3_ref,
    in4_ref,
    in5_ref,
    far0_ref,
    far1_ref,
    far2_ref,
    far3_ref,
    far4_ref,
    far5_ref,
    half0_ref,
    half1_ref,
    half2_ref,
    half3_ref,
    half4_ref,
    half5_ref,
    total_in_ref,
    own_sem,
    pair_send,
    pair_recv,
    chip_send,
    chip_recv,
    load_sem,
    y_sem,
    mixed_sem,
    act_w_sem,
    dx_sem,
    core_send,
    core_recv,
    far_send,
    far_recv,
    half_send,
    half_recv,
    join_send,
    join_recv,
    total_send,
    total_recv,
):
    tokens, windows, width, heads, hidden, shards, reps = dims
    me = lax.axis_index("shard")
    chips = shards // 2
    core = lax.rem(me, 2)
    chip = me // 2
    pair = chip * 2 + 1 - core

    def peer(k):
        return lax.rem(chip + k, chips) * 2 + core

    def owner(k, side):
        return lax.rem(chip + chips - k, chips) * 2 + side

    gathers = (
        (wqkv_shard, wqkv_ref, slice(0, wqkv_ref.shape[1] // 2)),
        (wqkv_shard, wqkv_ref, slice(wqkv_ref.shape[1] // 2, wqkv_ref.shape[1])),
        (wproj_shard, wproj_ref, slice(0, wproj_ref.shape[1])),
        (w1_shard, w1_ref, slice(0, w1_ref.shape[1])),
        (w2_shard, w2_ref, slice(0, w2_ref.shape[1])),
    )

    def block(ref, index, cols):
        size = ref.shape[0] // shards
        return ref.at[pl.ds(pl.multiple_of(index * size, size), size), cols]

    def own_copy(i):
        shard, full, cols = gathers[i]
        return pltpu.make_async_copy(shard.at[:, cols], block(full, me, cols), own_sem.at[i])

    def chip_copy(i, k):
        shard, full, cols = gathers[i]
        return pltpu.make_async_remote_copy(
            src_ref=shard.at[:, cols],
            dst_ref=block(full, me, cols),
            send_sem=chip_send.at[i, k - 1],
            recv_sem=chip_recv.at[i, k - 1],
            device_id={"shard": peer(k)},
            device_id_type=pl.DeviceIdType.MESH,
        )

    def pair_copy(i, k):
        shard, full, cols = gathers[i]
        return pltpu.make_async_remote_copy(
            src_ref=shard.at[:, cols] if k == 0 else block(full, owner(k, core), cols),
            dst_ref=block(full, owner(k, core), cols),
            send_sem=pair_send.at[i, k],
            recv_sem=pair_recv.at[i, k],
            device_id={"shard": pair},
            device_id_type=pl.DeviceIdType.MESH,
        )

    def gather_start(i):
        own_copy(i).start()
        for k in range(1, chips):
            chip_copy(i, k).start()
        pair_copy(i, 0).start()

    def gather_relay(i):
        for k in range(1, chips):
            chip_copy(i, k).wait_recv()
            pair_copy(i, k).start()

    def gather_finish(i):
        own_copy(i).wait()
        for k in range(chips):
            pair_copy(i, k).wait_recv()

    def gather_drain(i):
        for k in range(1, chips):
            chip_copy(i, k).wait_send()
        for k in range(chips):
            pair_copy(i, k).wait_send()

    rep = lax.axis_index("rep")
    bits = reps.bit_length() - 1

    near = min(bits, 3)
    near_size = 1 << near
    far_bits = list(range(near, bits))

    def flipped(index, distance, span):
        for b in range(span):
            if distance >> b & 1:
                index = index + (1 - 2 * lax.rem(index // (1 << b), 2)) * (1 << b)
        return index

    shard_span = shards.bit_length() - 1
    barrier = pltpu.get_barrier_semaphore()
    greeted = [{"shard": flipped(me, d, shard_span)} for d in range(1, shards)]
    greeted += [{"rep": flipped(rep, d, near)} for d in range(1, near_size)]
    greeted += [{"rep": flipped(rep, 1 << b, bits)} for b in far_bits]
    for target in greeted:
        pl.semaphore_signal(
            barrier, inc=1, device_id=target, device_id_type=pl.DeviceIdType.MESH
        )
    pl.semaphore_wait(barrier, len(greeted))
    gather_start(0)
    gather_start(1)

    head_size = width // heads
    scale = head_size ** (-0.5)
    pad = 64
    key_rows = 56
    sub = 8
    group = 2 * sub
    groups = windows // group
    quad = 128 // head_size
    quads = heads // quad
    rows8 = tokens * sub
    rows = tokens * group
    rows_w = sub * pad
    chunk = width
    step = 7
    lane_head = lax.broadcasted_iota(jnp.int32, (pad, 128), 1) // head_size
    head_masks = [lane_head == h for h in range(quad)]
    head_masks_half = [m.astype(f32).astype(bf16) for m in head_masks]

    base = {}
    at = 0
    for name, size in (
        ("qb", width),
        ("vb", width),
        ("pb", width),
        ("hb", hidden),
        ("ob", width),
        ("g1", width),
        ("s1", width),
        ("g2", width),
        ("s2", width),
    ):
        base[name] = (at, size)
        at += size

    def add_small(name, value, offset=0):
        start = base[name][0] + offset
        cols = pl.ds(start, value.shape[1])
        small_ref[:, cols] = small_ref[:, cols] + value

    def load(source, g, slot):
        return pltpu.make_async_copy(
            source.at[:, pl.ds(pl.multiple_of(g * group, group), group), :],
            in_ref.at[slot],
            load_sem.at[slot],
        )

    def store(source, target, g, sem):
        return pltpu.make_async_copy(
            source, target.at[:, pl.ds(pl.multiple_of(g * group, group), group), :], sem
        )

    def mixed_load(g):
        return pltpu.make_async_copy(
            mixed_hbm.at[:, pl.ds(pl.multiple_of(g * group, group), group), :], mixed_ref, mixed_sem
        )

    def act_w_store(g2, slot):
        return pltpu.make_async_copy(act_w_ref.at[slot], act_w_hbm.at[g2], act_w_sem.at[slot])

    def act_w_load(g2, slot):
        return pltpu.make_async_copy(act_w_hbm.at[g2], act_w_ref.at[slot], act_w_sem.at[slot])

    load(x_hbm, 0, 0).start()

    owned = width // shards
    works = (work0_ref, work1_ref, work2_ref, work3_ref, work4_ref, work5_ref)
    ins = (in0_ref, in1_ref, in2_ref, in3_ref, in4_ref, in5_ref)
    fars = (far0_ref, far1_ref, far2_ref, far3_ref, far4_ref, far5_ref)
    halves = (half0_ref, half1_ref, half2_ref, half3_ref, half4_ref, half5_ref)

    def unit_pieces(u, s):
        own = pl.ds(pl.multiple_of(s * owned, owned), owned)
        if u == 0:
            for i in range(hidden // width):
                cols = slice(width * i, width * (i + 1))
                yield owned * i, owned, (lambda cols=cols: dw1_ref[own, cols])
        elif u == 1:
            size = hidden // shards
            for i in range(size // 256):
                lanes = pl.ds(pl.multiple_of(s * size + i * 256, 256), 256)
                yield i * 256, 256, (lambda lanes=lanes: dw2t_ref[:, lanes].T)
        elif u == 2:
            yield 0, owned, (lambda: dwproj_ref[own, :])
        else:
            cols = slice(width * (u - 3), width * (u - 2))
            yield 0, owned, (lambda: dwqkv_ref[own, cols])

    def unit_out(u, j):
        rows_u = works[u].shape[0]
        if u == 0:
            return mixed_w_ref.at[0:rows_u] if j == 0 else out0_ref.at[j - 1]
        if u == 1:
            return act_ref.at[0:rows_u, j * width : (j + 1) * width]
        first = (u - 2) * owned
        return act_ref.at[
            first : first + owned, (chips + j) * width : (chips + j + 1) * width
        ]

    def core_copy(u, j):
        return pltpu.make_async_remote_copy(
            src_ref=unit_out(u, j),
            dst_ref=ins[u].at[j],
            send_sem=core_send.at[u, j],
            recv_sem=core_recv.at[u, j],
            device_id={"shard": pair},
            device_id_type=pl.DeviceIdType.MESH,
        )

    def levels(u):
        if u < 2 and near == 3:
            return [(0, 1), (1, 2)]
        return [(0, near)]

    def level_index(u, at_level):
        low, count = levels(u)[at_level]
        return lax.rem(rep // (1 << low), 1 << count)

    def held(u, at_level):
        size = works[u].shape[0]
        start = 0
        for k in range(at_level):
            size >>= levels(u)[k][1]
            start = start + level_index(u, k) * size
        return start, size

    def lines_of(start, size):
        return pl.ds(start if isinstance(start, int) else pl.multiple_of(start, 16), size)

    def own_piece(u):
        return lines_of(*held(u, len(levels(u))))

    def peers_of(u, at_level):
        slot = 0
        row = 0
        for k in range(at_level):
            others = (1 << levels(u)[k][1]) - 1
            slot += others
            row += others * held(u, k + 1)[1]
        low, count = levels(u)[at_level]
        size = held(u, at_level + 1)[1]
        return [
            (d, slot + d - 1, row + (d - 1) * size, {"rep": flipped(rep, d << low, bits)})
            for d in range(1, 1 << count)
        ]

    def far_copy(u, k):
        return pltpu.make_async_remote_copy(
            src_ref=ins[u].at[lax.rem(chip + k, chips)],
            dst_ref=fars[u].at[k - 1],
            send_sem=far_send.at[u, k - 1],
            recv_sem=far_recv.at[u, k - 1],
            device_id={"shard": peer(k)},
            device_id_type=pl.DeviceIdType.MESH,
        )

    def spread_copy(u, at_level, link):
        d, slot, row, partner = link
        start, _ = held(u, at_level)
        size = held(u, at_level + 1)[1]
        index = flipped(level_index(u, at_level), d, levels(u)[at_level][1])
        return pltpu.make_async_remote_copy(
            src_ref=ins[u].at[chip, lines_of(start + index * size, size), :],
            dst_ref=halves[u].at[pl.ds(row, size), :],
            send_sem=half_send.at[u, slot],
            recv_sem=half_recv.at[u, slot],
            device_id=partner,
            device_id_type=pl.DeviceIdType.MESH,
        )

    def double_copy(u, b):
        slot = near_size - 1 + b - near
        size = works[u].shape[0] // near_size
        return pltpu.make_async_remote_copy(
            src_ref=ins[u].at[chip, own_piece(u), :],
            dst_ref=halves[u].at[pl.ds(slot * size, size), :],
            send_sem=half_send.at[u, slot],
            recv_sem=half_recv.at[u, slot],
            device_id={"rep": flipped(rep, 1 << b, bits)},
            device_id_type=pl.DeviceIdType.MESH,
        )

    def join_copy(u, at_level, link):
        d, slot, row, partner = link
        lines = lines_of(*held(u, at_level + 1))
        return pltpu.make_async_remote_copy(
            src_ref=works[u].at[lines, :],
            dst_ref=works[u].at[lines, :],
            send_sem=join_send.at[u, slot],
            recv_sem=join_recv.at[u, slot],
            device_id=partner,
            device_id_type=pl.DeviceIdType.MESH,
        )

    def level_start(u, at_level):
        for link in peers_of(u, at_level):
            spread_copy(u, at_level, link).start()

    def join_start(u, at_level):
        for link in peers_of(u, at_level):
            join_copy(u, at_level, link).start()

    def unit_stage(u, stage):
        if stage == 0:
            for j in range(chips):
                target = unit_out(u, j)
                for r0, nr, value in unit_pieces(u, 2 * j + 1 - core):
                    target[r0 : r0 + nr, :] = value().astype(bf16)
                core_copy(u, j).start()
            return
        if stage == 1:
            for j in range(chips):
                core_copy(u, j).wait()
            for k in range(1, chips + 1):
                j = lax.rem(chip + k, chips)
                for r0, nr, value in unit_pieces(u, 2 * j + core):
                    got = ins[u][j, r0 : r0 + nr, :].astype(f32)
                    ins[u][j, r0 : r0 + nr, :] = (value() + got).astype(bf16)
                if k == chips - 1:
                    for n in range(1, chips):
                        far_copy(u, n).start()
            return
        if stage == 2:
            for k in range(1, chips):
                far_copy(u, k).wait()
            total = ins[u][chip].astype(f32)
            for k in range(1, chips):
                total = total + fars[u][k - 1].astype(f32)
            ins[u][chip] = total.astype(bf16)
            level_start(u, 0)
            return
        count = len(levels(u))
        at_level = stage - 3
        if at_level < count:
            lines = lines_of(*held(u, at_level + 1))
            size = held(u, at_level + 1)[1]
            total = ins[u][chip, lines, :].astype(f32)
            for link in peers_of(u, at_level):
                spread_copy(u, at_level, link).wait()
                total = total + halves[u][link[2] : link[2] + size, :].astype(f32)
            if at_level + 1 < count:
                ins[u][chip, lines, :] = total.astype(bf16)
                level_start(u, at_level + 1)
            elif far_bits:
                ins[u][chip, lines, :] = total.astype(bf16)
                double_copy(u, far_bits[0]).start()
            else:
                works[u][lines, :] = total.astype(bf16)
                join_start(u, count - 1)
            return
        at_double = at_level - count
        if at_double < len(far_bits):
            b = far_bits[at_double]
            double_copy(u, b).wait()
            size = works[u].shape[0] // near_size
            row = (near_size - 1 + b - near) * size
            total = ins[u][chip, own_piece(u), :].astype(f32) + halves[u][
                row : row + size, :
            ].astype(f32)
            if b != far_bits[-1]:
                ins[u][chip, own_piece(u), :] = total.astype(bf16)
                double_copy(u, b + 1).start()
            else:
                works[u][own_piece(u), :] = total.astype(bf16)
                join_start(u, count - 1)
            return
        at_join = count - 1 - (at_double - len(far_bits))
        if at_join >= 0:
            for link in peers_of(u, at_join):
                join_copy(u, at_join, link).wait()
            if at_join > 0:
                join_start(u, at_join - 1)

    stages = 7 + len(far_bits)

    total_steps = 2 + len(far_bits)

    def total_copies(part, step):
        first, last = part
        if step == 0:
            links = [(d - 1, {"shard": flipped(me, d, shard_span)}) for d in range(1, shards)]
        elif step == 1:
            links = [
                (shards + d - 2, {"rep": flipped(rep, d, near)}) for d in range(1, near_size)
            ]
        else:
            b = far_bits[step - 2]
            links = [(shards + near_size + step - 4, {"rep": flipped(rep, 1 << b, bits)})]
        which = 0 if first == 0 else 1
        return [
            (
                at_slot,
                pltpu.make_async_remote_copy(
                    src_ref=total_ref.at[first:last],
                    dst_ref=total_in_ref.at[at_slot, first:last],
                    send_sem=total_send.at[which, at_slot],
                    recv_sem=total_recv.at[which, at_slot],
                    device_id=target,
                    device_id_type=pl.DeviceIdType.MESH,
                ),
            )
            for at_slot, target in links
        ]

    def total_start(part, step):
        for _, copy in total_copies(part, step):
            copy.start()

    def total_finish(part, step):
        first, last = part
        values = [total_ref[first:last]]
        for at_slot, copy in total_copies(part, step):
            copy.wait()
            values.append(total_in_ref[at_slot, first:last])
        while len(values) > 1:
            values = [values[i] + values[i + 1] for i in range(0, len(values), 2)]
        total_ref[first:last] = values[0]
        if step + 1 < total_steps:
            total_start(part, step + 1)

    small_ref[...] = jnp.zeros(small_ref.shape, f32)
    dbias_ref[...] = jnp.zeros(dbias_ref.shape, f32)
    sat_ref[width:, :] = (
        lax.broadcasted_iota(jnp.int32, (16, rows), 0) == 0
    ).astype(f32).astype(bf16)

    @pl.loop(0, width // 32)
    def _(n):
        lines = pl.ds(pl.multiple_of(n * 32, 32), 32)
        dwqkv_ref[lines, :] = jnp.zeros((32, 3 * width), f32)
        dwproj_ref[lines, :] = jnp.zeros((32, width), f32)
        dw1_ref[lines, :] = jnp.zeros((32, hidden), f32)
        dw2t_ref[lines, :] = jnp.zeros((32, hidden), f32)

    @pl.loop(0, rows_w // 64)
    def _(n):
        start = pl.multiple_of(n * 64, 64)
        to = lax.broadcasted_iota(jnp.int32, (64, rows8), 0) + start
        source = lax.broadcasted_iota(jnp.int32, (64, rows8), 1)
        hit = (to // pad == source % sub) & (to % pad == source // sub)
        perm_ref[pl.ds(start, 64), :] = hit.astype(f32).astype(bf16)

    @pl.loop(0, rows8 // 56)
    def _(n):
        start = pl.multiple_of(n * 56, 8)
        to = lax.broadcasted_iota(jnp.int32, (56, rows_w), 0) + start
        source = lax.broadcasted_iota(jnp.int32, (56, rows_w), 1)
        hit = (source // pad == to % sub) & (source % pad == to // sub)
        back_ref[pl.ds(start, 56), :] = hit.astype(f32).astype(bf16)

    table_tall = heads // 2
    table_rows = table_ref.shape[1]
    table_lanes = -(-table_rows // 128) * 128
    row_iota = lax.broadcasted_iota(jnp.int32, (table_lanes, 128), 0).astype(f32)
    low_lanes = lax.broadcasted_iota(jnp.int32, (key_rows, 128), 1) < pad
    rows_ref[...] = jnp.zeros(rows_ref.shape, f32)
    rows_ref[:, 0:table_rows] = table_ref[...]
    names_ref[...] = jnp.full(names_ref.shape, -1.0, f32)
    names_ref[0:tokens, 0:tokens] = index_ref[...].astype(f32)
    names_ref[...] = names_ref[...].T

    def named(j):
        return (row_iota == names_ref[pl.ds(j, 1), :]).astype(f32).astype(bf16)

    table = rows_ref[...]
    high = table.astype(bf16)
    middle = (table - high.astype(f32)).astype(bf16)
    low = (table - high.astype(f32) - middle.astype(f32)).astype(bf16)
    plane_ref[...] = jnp.full(plane_ref.shape, -1e30, f32)

    def plane(h):
        return plane_ref.at[h * key_rows : (h + 1) * key_rows, :]

    @pl.loop(0, tokens)
    def _(j):
        hit = named(j)
        line = (dot_nn(high, hit) + dot_nn(middle, hit)) + dot_nn(low, hit)
        plane_ref[pl.ds(j, heads, stride=key_rows), :] = line

    for t in range(quads):
        for h in range(quad // 2):
            left = plane(t * quad + 2 * h)[...]
            right = plane(t * quad + 2 * h + 1)[...]
            bias_ref[t, :, 128 * h : 128 * (h + 1)] = jnp.where(
                low_lanes, left, pltpu.roll(right, pad, 1)
            )

    def stacked(tile):
        return jnp.concatenate([tile * m for m in head_masks_half], axis=0)

    def diagonal(tall):
        total = tall[0:pad]
        for h in range(1, quad):
            total = jnp.where(head_masks[h], tall[h * pad : (h + 1) * pad], total)
        return total

    def grow(values):
        return jnp.concatenate([values, jnp.zeros((pad - key_rows, values.shape[1]), f32)], axis=0)

    @pl.loop(0, groups)
    def _(g):
        slot = lax.rem(g, 2)
        load(x_hbm, g, slot).wait()
        load(x_hbm, lax.rem(g + 1, groups), 1 - slot).start()

        @pl.when(g == groups - 1)
        def _():
            gather_relay(0)

        @pl.loop(0, tokens // step)
        def _(n):
            part = in_ref[slot, pl.ds(n * step, step)].astype(f32)
            flat = part.reshape(step * group, width)
            normal, _ = norm_parts(flat)
            wide_ref[pl.ds(n * step, step)] = (normal * gain1_ref[...] + shift1_ref[...]).reshape(
                step, group, width
            )

        for s in range(2):
            act8 = wide_ref[:, sub * s : sub * (s + 1), :].reshape(rows8, width).astype(bf16)

            @pl.when(g != 0)
            def _():
                act_w_store(2 * g - 2 + s, s).wait()

            act_w_ref[s] = dot_nn(perm_ref[...], act8).astype(bf16)
            act_w_store(2 * g + s, s).start()

    for s in range(2):
        act_w_store(2 * groups - 2 + s, s).wait()
    act_w_load(0, 0).start()
    gather_relay(1)
    for i in range(2, 5):
        gather_start(i)
    for i in range(2):
        gather_finish(i)

    @pl.loop(0, groups)
    def _(g):
        win0 = pl.multiple_of(g * group, group)
        slot = lax.rem(groups + g, 2)
        load(x_hbm, g, slot).wait()

        @pl.when(g < groups - 1)
        def _():
            load(x_hbm, g + 1, 1 - slot).start()

        @pl.when(g == groups - 1)
        def _():
            load(dy_hbm, 0, 1 - slot).start()
            gather_relay(3)

        @pl.loop(0, 2)
        def _(s):
            g2 = g * 2 + s
            act_w_load(g2, s).wait()

            @pl.when(g2 < 2 * groups - 1)
            def _():
                act_w_load(g2 + 1, 1 - s).start()

            for n in range(3):
                cols = slice(n * width, (n + 1) * width)
                out = dot_nn(act_w_ref[s], wqkv_ref[:, cols])
                if n == 0:
                    out = (out + query_bias_ref[...]) * scale
                if n == 2:
                    out = out + value_bias_ref[...]
                qkv_ref[g2, :, cols] = out.astype(bf16)

            @pl.loop(0, sub // 4)
            def _(wi):
                items = []
                for e in range(4):
                    w = wi * 4 + e
                    line = pl.ds(pl.multiple_of(w * pad, pad), pad)
                    items += [(w, line, t) for t in range(quads)]
                for first in range(0, len(items), 8):
                    batch = items[first : first + 8]
                    scores = [
                        dot_nt(
                            qkv_ref[g2, line, width + 128 * t : width + 128 * (t + 1)],
                            stacked(qkv_ref[g2, line, 128 * t : 128 * (t + 1)]),
                        )[0:key_rows]
                        + bias_ref[t]
                        for w, line, t in batch
                    ]
                    tops = [jnp.max(x, axis=0, keepdims=True) for x in scores]
                    weights = [jnp.exp(x - top) for x, top in zip(scores, tops)]
                    totals = [jnp.sum(x, axis=0, keepdims=True) for x in weights]
                    for (w, line, t), top, total in zip(batch, tops, totals):
                        lse_ref[g2, w, t : t + 1, :] = top + jnp.log(total)
                    probs = [
                        grow(x * (1.0 / total)).astype(bf16) for x, total in zip(weights, totals)
                    ]
                    mixes = [
                        dot_tn(
                            x, qkv_ref[g2, line, 2 * width + 128 * t : 2 * width + 128 * (t + 1)]
                        )
                        for x, (w, line, t) in zip(probs, batch)
                    ]
                    for x, (w, line, t) in zip(mixes, batch):
                        mixed_w_ref[line, 128 * t : 128 * (t + 1)] = diagonal(x).astype(bf16)

            wide_ref[:, pl.ds(pl.multiple_of(sub * s, sub), sub), :] = dot_nn(
                back_ref[...], mixed_w_ref[...]
            ).reshape(tokens, sub, width)

        @pl.when(g != 0)
        def _():
            store(mixed_ref, mixed_hbm, g - 1, mixed_sem).wait()

        @pl.when(g == 0)
        def _():
            gather_relay(2)
            gather_finish(2)

        @pl.when(g == groups - 1)
        def _():
            gather_relay(4)

        mixed_ref[...] = wide_ref[...].astype(bf16)
        store(mixed_ref, mixed_hbm, g, mixed_sem).start()
        out = dot_nn(mixed_ref[...].reshape(rows, width), wproj_ref[...]) + proj_bias_ref[...]
        dx_ref[:, pl.ds(win0, group), :] = in_ref[slot].astype(f32) + out.reshape(
            tokens, group, width
        )

    gather_finish(3)
    gather_finish(4)
    for i in range(5):
        gather_drain(i)
    store(mixed_ref, mixed_hbm, groups - 1, mixed_sem).wait()

    @pl.loop(0, groups)
    def _(g):
        win0 = pl.multiple_of(g * group, group)
        slot = lax.rem(2 * groups + g, 2)
        load(dy_hbm, g, slot).wait()

        @pl.when(g < groups - 1)
        def _():
            load(dy_hbm, g + 1, 1 - slot).start()

        @pl.when(g == groups - 1)
        def _():
            load(x_hbm, 0, 1 - slot).start()

        @pl.when(g != 0)
        def _():
            store(y_ref, y_hbm, g - 1, y_sem).wait()

        mixed_load(g).start()

        @pl.loop(0, tokens // step)
        def _(n):
            part = dx_ref[pl.ds(n * step, step), pl.ds(win0, group), :].reshape(step * group, width)
            normal, _ = norm_parts(part)
            lines = pl.ds(pl.multiple_of(n * step * group, step * group), step * group)
            sa_ref[lines, :] = (normal * gain2_ref[...] + shift2_ref[...]).astype(bf16)

        sat_ref[0:width, :] = sa_ref[...].T
        dyt_ref[...] = in_ref[slot].reshape(rows, width).T

        count = hidden // chunk
        columns = [slice(i * chunk, (i + 1) * chunk) for i in range(count)]

        def rise(i):
            u_ref[...] = dot_nn(sa_ref[...], w1_ref[:, columns[i]])
            da_ref[...] = dot_nt(in_ref[slot].reshape(rows, width), w2_ref[columns[i], :])

        def bend(i):
            for m in range(tokens // step):
                lines = slice(m * step * group, (m + 1) * step * group)
                value, slope = gelu_pair(u_ref[lines, :] + hidden_bias_ref[:, columns[i]])
                act_ref[lines, columns[i]] = value.astype(bf16)
                dup_ref[lines, columns[i]] = (da_ref[lines, :] * slope).astype(bf16)

        def gather_grads(i):
            cols = columns[i]
            part1 = dot_nn(sat_ref[...], dup_ref[:, cols])
            dw1_ref[:, cols] += part1[0:width]
            add_small("hb", part1[width : width + 8], cols.start)
            dw2t_ref[:, cols] += dot_nn(dyt_ref[...], act_ref[:, cols])

        rise(0)
        for i in range(count):
            bend(i)
            if i > 0:
                gather_grads(i - 1)
            if i + 1 < count:
                rise(i + 1)
        gather_grads(count - 1)

        @pl.when(g == groups - 1)
        def _():
            unit_stage(0, 0)

        out = dot_nn(act_ref[...], w2_ref[...]) + output_bias_ref[...]
        y_ref[...] = (
            dx_ref[:, pl.ds(win0, group), :] + out.reshape(tokens, group, width)
        ).astype(bf16)
        wide_ref[...] = dot_nt(dup_ref[...], w1_ref[...]).reshape(tokens, group, width)

        @pl.when(g == groups - 1)
        def _():
            unit_stage(1, 0)

        store(y_ref, y_hbm, g, y_sem).start()

        @pl.loop(0, tokens // step)
        def _(n):
            lines = pl.ds(pl.multiple_of(n * step * group, step * group), step * group)
            normal, inverse = norm_parts(
                dx_ref[pl.ds(n * step, step), pl.ds(win0, group), :].reshape(step * group, width)
            )
            grad = wide_ref[pl.ds(n * step, step)].reshape(step * group, width)
            scaled = grad * gain2_ref[...]
            back = inverse * (
                scaled
                - jnp.mean(scaled, axis=-1, keepdims=True)
                - normal * jnp.mean(scaled * normal, axis=-1, keepdims=True)
            )
            cot = in_ref[slot, pl.ds(n * step, step)].astype(f32).reshape(step * group, width)
            total = cot + back
            dx_ref[pl.ds(n * step, step), pl.ds(win0, group), :] = total.reshape(step, group, width)
            sa_ref[lines, :] = total.astype(bf16)
            add_small("ob", fold_rows(cot))
            add_small("pb", fold_rows(total))
            add_small("g2", fold_rows(grad * normal))
            add_small("s2", fold_rows(grad))

        @pl.when(g == groups - 1)
        def _():
            unit_stage(0, 1)

        mixed_load(g).wait()
        dwproj_ref[...] += dot_tn(mixed_ref[...].reshape(rows, width), sa_ref[...])

    store(y_ref, y_hbm, groups - 1, y_sem).wait()
    unit_stage(1, 1)
    unit_stage(2, 0)
    act_w_load(0, 0).start()

    plan = {
        0: ((2, 1),),
        3: ((0, 2),),
        4: ((1, 2),),
        5: ((2, 2),),
        6: ((0, 3),),
        7: ((1, 3),),
        8: ((2, 3),),
        9: ((0, 4),),
        11: ((1, 4), (2, 4)),
    }

    def progress(g2, half):
        for point, calls in plan.items():
            if point % 2 == half:

                @pl.when(g2 == point // 2)
                def _():
                    for u, stage in calls:
                        unit_stage(u, stage)

    subs = 2 * groups

    @pl.loop(0, subs)
    def _(g2):
        s = lax.rem(g2, 2)
        half8 = dx_ref[:, pl.ds(pl.multiple_of(g2 * sub, sub), sub), :]
        half_w = dot_nn(perm_ref[...], half8.reshape(rows8, width).astype(bf16)).astype(bf16)
        mixed_w_ref[...] = dot_nt(half_w, wproj_ref[...]).astype(bf16)
        progress(g2, 0)

        @pl.loop(0, sub // 2)
        def _(wi):
            items = []
            for e in range(2):
                w = wi * 2 + e
                line = pl.ds(pl.multiple_of(w * pad, pad), pad)
                for t in range(quads):
                    cols = [
                        slice(i * width + 128 * t, i * width + 128 * (t + 1)) for i in range(3)
                    ]
                    items.append((w, line, t, cols))
            for first in range(0, len(items), 8):
                batch = items[first : first + 8]
                queries = [stacked(qkv_ref[g2, line, c[0]]) for w, line, t, c in batch]
                scores = [
                    dot_nt(qkv_ref[g2, line, c[1]], x)[0:key_rows] + bias_ref[t]
                    for x, (w, line, t, c) in zip(queries, batch)
                ]
                grads = [stacked(mixed_w_ref[line, c[0]]) for w, line, t, c in batch]
                prob_grads = [
                    dot_nt(qkv_ref[g2, line, c[2]], x)[0:key_rows]
                    for x, (w, line, t, c) in zip(grads, batch)
                ]
                probs = [
                    jnp.exp(x - lse_ref[g2, w, t : t + 1, :])
                    for x, (w, line, t, c) in zip(scores, batch)
                ]
                prob_halves = [grow(x).astype(bf16) for x in probs]
                value_grads = [dot_nn(x, y) for x, y in zip(prob_halves, grads)]
                deltas = [
                    jnp.sum(x * y, axis=0, keepdims=True) for x, y in zip(probs, prob_grads)
                ]
                score_grads = [
                    x * (y - delta) for x, y, delta in zip(probs, prob_grads, deltas)
                ]
                for x, (w, line, t, c) in zip(score_grads, batch):
                    dbias_ref[t] += x
                halves_ = [grow(x).astype(bf16) for x in score_grads]
                key_grads = [dot_nn(x, y) for x, y in zip(halves_, queries)]
                query_grads = [
                    dot_tn(x, qkv_ref[g2, line, c[1]])
                    for x, (w, line, t, c) in zip(halves_, batch)
                ]
                for k, (w, line, t, c) in enumerate(batch):
                    qkv_ref[g2, line, c[0]] = (diagonal(query_grads[k]) * scale).astype(bf16)
                    qkv_ref[g2, line, c[1]] = key_grads[k].astype(bf16)
                    qkv_ref[g2, line, c[2]] = value_grads[k].astype(bf16)

        progress(g2, 1)
        act_w_load(g2, s).wait()

        @pl.when(g2 < subs - 1)
        def _():
            act_w_load(g2 + 1, 1 - s).start()

        sat_ref[0:width, 0:rows_w] = act_w_ref[s].T
        for n in range(3):
            cols = slice(n * width, (n + 1) * width)
            part = dot_nn(sat_ref[:, 0:rows_w], qkv_ref[g2, :, cols])
            dwqkv_ref[:, cols] += part[0:width]
            if n == 0:
                add_small("qb", part[width : width + 8])
            if n == 2:
                add_small("vb", part[width : width + 8])

            @pl.when(g2 == subs - 1)
            def _():
                unit_stage(3 + n, 0)
                if n == 2:
                    unit_stage(3, 1)

    for t in range(quads):
        for h in range(quad // 2):
            both = dbias_ref[t, :, 128 * h : 128 * (h + 1)]
            plane(t * quad + 2 * h)[...] = jnp.where(low_lanes, both, 0.0)
            plane(t * quad + 2 * h + 1)[...] = jnp.where(
                low_lanes, pltpu.roll(both, pad, 1), 0.0
            )
    total_ref[...] = jnp.zeros(total_ref.shape, f32)

    @pl.loop(0, tokens)
    def _(j):
        hit = named(j)
        line = plane_ref[pl.ds(j, heads, stride=key_rows), :]
        upper_half = line.astype(bf16)
        lower_half = (line - upper_half.astype(f32)).astype(bf16)
        found = dot_nt(upper_half, hit) + dot_nt(lower_half, hit)
        for side in range(2):
            lanes = slice(side * table_lanes, (side + 1) * table_lanes)
            total_ref[0:table_tall, lanes] = (
                total_ref[0:table_tall, lanes] + found[side * table_tall : (side + 1) * table_tall]
            )

    for u in range(4, 6):
        unit_stage(u, 1)
    early = (0, table_tall + (small_ref.shape[1] - 4 * width) // width)
    late = (early[1], early[1] + 8)

    def put_sums(first, last):
        for i in range(first, last):
            total_ref[table_tall + i : table_tall + i + 1, :] = jnp.sum(
                small_ref[:, i * width : (i + 1) * width], axis=0, keepdims=True
            )

    put_sums(0, early[1] - table_tall)
    total_start(early, 0)
    plan2 = {
        0: ((0, 5),),
        1: ((3, 2),),
        2: ((1, 5), (4, 2), (-1, 0)),
        3: ((5, 2),),
        4: ((0, 6),),
        5: ((3, 3),),
    }

    @pl.loop(0, groups)
    def _(g):
        win0 = pl.multiple_of(g * group, group)
        slot = lax.rem(3 * groups + g, 2)
        load(x_hbm, g, slot).wait()

        @pl.when(g < groups - 1)
        def _():
            load(x_hbm, g + 1, 1 - slot).start()

        for s in range(2):
            g2 = g * 2 + s
            mixed_w_ref[...] = dot_nt(qkv_ref[g2], wqkv_ref[...]).astype(bf16)
            wide_ref[:, sub * s : sub * (s + 1), :] = dot_nn(back_ref[...], mixed_w_ref[...]).reshape(
                tokens, sub, width
            )
            for point, calls in plan2.items():
                if point % 2 == s:

                    @pl.when(g == point // 2)
                    def _():
                        for u, stage in calls:
                            if u < 0:
                                total_finish(early, stage)
                            else:
                                unit_stage(u, stage)

        @pl.loop(0, tokens // step)
        def _(n):
            part = in_ref[slot, pl.ds(n * step, step)].astype(f32)
            normal, inverse = norm_parts(part.reshape(step * group, width))
            grad = wide_ref[pl.ds(n * step, step)].reshape(step * group, width)
            scaled = grad * gain1_ref[...]
            back = inverse * (
                scaled
                - jnp.mean(scaled, axis=-1, keepdims=True)
                - normal * jnp.mean(scaled * normal, axis=-1, keepdims=True)
            )
            dx_ref[pl.ds(n * step, step), pl.ds(win0, group), :] += back.reshape(step, group, width)
            add_small("g1", fold_rows(grad * normal))
            add_small("s1", fold_rows(grad))

        @pl.when(g != 0)
        def _():
            store(y_ref, dx_hbm, g - 1, dx_sem).wait()

        y_ref[...] = dx_ref[:, pl.ds(win0, group), :].astype(bf16)
        store(y_ref, dx_hbm, g, dx_sem).start()

    put_sums(early[1] - table_tall, small_ref.shape[1] // width)
    total_start(late, 0)
    done = {0: 6, 1: 5, 2: 4, 3: 3, 4: 2, 5: 2}
    for stage in range(2, stages):
        for u in range(6):
            if stage > done[u]:
                unit_stage(u, stage)
        if stage == 3:
            total_finish(late, 0)
            total_finish(early, 1)
    for step_at in range(1, total_steps):
        total_finish(late, step_at)
        if step_at > 1:
            total_finish(early, step_at)
    store(y_ref, dx_hbm, groups - 1, dx_sem).wait()


def local_pass(x, dy, wqkv, wproj, w1, w2, vectors, table, index, shards, reps):
    tokens, windows, width = x.shape
    hidden = w1.shape[1]
    heads = table.shape[0]
    dims = (tokens, windows, width, heads, hidden, shards, reps)
    chips = shards // 2
    bits = reps.bit_length() - 1
    sub = 8
    group = 2 * sub
    pad = 64
    rows = tokens * group
    small_size = 8 * width + hidden
    subs = windows // sub
    owned = width // shards
    unit_rows = (hidden // shards, hidden // shards, owned, owned, owned, owned)
    near_size = 1 << min(bits, 3)
    slots = near_size - 1 + bits - min(bits, 3)
    total_rows = heads // 2 + small_size // width + 4
    shapes = (
        [
            jax.ShapeDtypeStruct(x.shape, bf16),
            jax.ShapeDtypeStruct(x.shape, bf16),
            jax.ShapeDtypeStruct(x.shape, bf16),
            jax.ShapeDtypeStruct((subs, sub * pad, width), bf16),
        ]
        + [jax.ShapeDtypeStruct((r, width), bf16) for r in unit_rows]
        + [jax.ShapeDtypeStruct((total_rows, width), f32)]
    )
    vmem = pl.BlockSpec(memory_space=pltpu.VMEM)
    hbm = pl.BlockSpec(memory_space=pl.ANY)

    return pl.pallas_call(
        functools.partial(compute_kernel, dims),
        out_shape=shapes,
        in_specs=[hbm] * 6 + [vmem] * 11,
        out_specs=[hbm] * 4 + [vmem] * 7,
        scratch_shapes=[
            pltpu.VMEM((2, tokens, group, width), bf16),
            pltpu.VMEM((tokens, group, width), bf16),
            pltpu.VMEM(x.shape, f32),
            pltpu.VMEM((width, 3 * width), f32),
            pltpu.VMEM((width, width), f32),
            pltpu.VMEM((width, hidden), f32),
            pltpu.VMEM((width, hidden), f32),
            pltpu.VMEM((8, small_size), f32),
            pltpu.VMEM((heads // 4, 56, 256), f32),
            pltpu.VMEM((heads // 4, 56, 256), f32),
            pltpu.VMEM((sub * pad, tokens * sub), bf16),
            pltpu.VMEM((tokens * sub, sub * pad), bf16),
            pltpu.VMEM((2, sub * pad, width), bf16),
            pltpu.VMEM((subs, sub * pad, 3 * width), bf16),
            pltpu.VMEM((sub * pad, width), bf16),
            pltpu.VMEM((tokens, group, width), bf16),
            pltpu.VMEM((subs, sub, heads // 4, 256), f32),
            pltpu.VMEM((tokens, group, width), f32),
            pltpu.VMEM((rows, width), bf16),
            pltpu.VMEM((width + 16, rows), bf16),
            pltpu.VMEM((width, rows), bf16),
            pltpu.VMEM((rows, width), f32),
            pltpu.VMEM((rows, width), f32),
            pltpu.VMEM((heads * 56, 128), f32),
            pltpu.VMEM((128, 128), f32),
            pltpu.VMEM((heads, -(-table.shape[1] // 128) * 128), f32),
            pltpu.VMEM((rows, hidden), bf16),
            pltpu.VMEM((rows, hidden), bf16),
            pltpu.VMEM((width, 3 * width), bf16),
            pltpu.VMEM((width, width), bf16),
            pltpu.VMEM((width, hidden), bf16),
            pltpu.VMEM((hidden, width), bf16),
            pltpu.VMEM((chips - 1, unit_rows[0], width), bf16),
            *[pltpu.VMEM((chips, r, width), bf16) for r in unit_rows],
            *[pltpu.VMEM((chips - 1, r, width), bf16) for r in unit_rows],
            *[pltpu.VMEM((slots * r // near_size, width), bf16) for r in unit_rows],
            pltpu.VMEM((shards - 1 + slots, total_rows, width), f32),
            pltpu.SemaphoreType.DMA((5,)),
            pltpu.SemaphoreType.DMA((5, chips)),
            pltpu.SemaphoreType.DMA((5, chips)),
            pltpu.SemaphoreType.DMA((5, chips - 1)),
            pltpu.SemaphoreType.DMA((5, chips - 1)),
            pltpu.SemaphoreType.DMA((2,)),
            pltpu.SemaphoreType.DMA,
            pltpu.SemaphoreType.DMA,
            pltpu.SemaphoreType.DMA((2,)),
            pltpu.SemaphoreType.DMA,
            pltpu.SemaphoreType.DMA((6, chips)),
            pltpu.SemaphoreType.DMA((6, chips)),
            pltpu.SemaphoreType.DMA((6, chips - 1)),
            pltpu.SemaphoreType.DMA((6, chips - 1)),
            pltpu.SemaphoreType.DMA((6, slots)),
            pltpu.SemaphoreType.DMA((6, slots)),
            pltpu.SemaphoreType.DMA((6, slots)),
            pltpu.SemaphoreType.DMA((6, slots)),
            pltpu.SemaphoreType.DMA((2, shards - 1 + slots)),
            pltpu.SemaphoreType.DMA((2, shards - 1 + slots)),
        ],
        compiler_params=pltpu.CompilerParams(
            vmem_limit_bytes=67043328, collective_id=0, has_side_effects=True
        ),
    )(x, dy, wqkv, wproj, w1, w2, *vectors, table, index)


def spread_kernel(heads, sizes, *refs):
    works = refs[:6]
    total_ref = refs[6]
    dwqkv_ref, dwproj_ref, dw1_ref, dw2_ref, table_ref = refs[7:12]
    width = dwproj_ref.shape[1]
    owned = dwproj_ref.shape[0]
    for i in range(dw1_ref.shape[1] // width):
        dw1_ref[:, i * width : (i + 1) * width] = works[0][i * owned : (i + 1) * owned, :].astype(f32)
    dw2_ref[...] = works[1][...].astype(f32)
    dwproj_ref[...] = works[2][...].astype(f32)
    for i in range(3):
        dwqkv_ref[:, i * width : (i + 1) * width] = works[3 + i][...].astype(f32)
    tall = heads // 2
    rows_t = table_ref.shape[1]
    lanes = total_ref.shape[1] // 2
    table_ref[0:tall, :] = total_ref[0:tall, 0:rows_t]
    table_ref[tall:heads, :] = total_ref[0:tall, lanes : lanes + rows_t]
    row = tall
    for ref, size in zip(refs[12:], sizes):
        for i in range(size // width):
            ref[:, i * width : (i + 1) * width] = total_ref[row : row + 1, :]
            row += 1


def spread(works, total, width, hidden, heads, table_rows):
    owned = works[2].shape[0]
    sizes = (width, width, width, hidden, width, width, width, width, width)
    shapes = [
        (owned, 3 * width),
        (owned, width),
        (owned, hidden),
        works[1].shape,
        (heads, table_rows),
    ] + [(1, size) for size in sizes]
    vmem = pl.BlockSpec(memory_space=pltpu.VMEM)
    return pl.pallas_call(
        functools.partial(spread_kernel, heads, sizes),
        out_shape=[jax.ShapeDtypeStruct(shape, f32) for shape in shapes],
        in_specs=[vmem] * 7,
        out_specs=[vmem] * len(shapes),
    )(*works, total)


def on_device(
    shards,
    reps,
    block_input,
    out_grad,
    qkv_weight,
    query_bias,
    value_bias,
    proj_weight,
    proj_bias,
    hidden_weight,
    hidden_bias,
    output_weight,
    output_bias,
    first_gain,
    first_shift,
    second_gain,
    second_shift,
    bias_table,
    table_index,
):
    windows, tokens, width = block_input.shape
    table_rows, heads = bias_table.shape
    hidden = hidden_bias.shape[0]
    vectors = [
        v.reshape(1, -1)
        for v in (
            query_bias,
            value_bias,
            proj_bias,
            hidden_bias,
            output_bias,
            first_gain,
            first_shift,
            second_gain,
            second_shift,
        )
    ]
    y, dx, _, _, *works, total = local_pass(
        jnp.transpose(block_input, (1, 0, 2)),
        jnp.transpose(out_grad, (1, 0, 2)),
        qkv_weight,
        proj_weight,
        hidden_weight,
        output_weight,
        vectors,
        bias_table.T,
        table_index,
        shards,
        reps,
    )
    (dwqkv, dwproj, dw1, dw2, table_grad, qb, vb, pb, hb, ob, g1, s1, g2, s2) = spread(
        works, total, width, hidden, heads, table_rows
    )
    return (
        jnp.transpose(y, (1, 0, 2)),
        jnp.transpose(dx, (1, 0, 2)).astype(f32),
        dwqkv,
        qb.reshape(-1),
        vb.reshape(-1),
        dwproj,
        pb.reshape(-1),
        dw1,
        hb.reshape(-1),
        dw2,
        ob.reshape(-1),
        g1.reshape(-1),
        s1.reshape(-1),
        g2.reshape(-1),
        s2.reshape(-1),
        table_grad.T,
    )


def solution(mesh):
    rows = P(("shard", "rep"), None, None)
    cut = P("shard", None)
    full = P()
    return jax.shard_map(
        functools.partial(on_device, mesh.shape["shard"], mesh.shape["rep"]),
        mesh=mesh,
        in_specs=(
            rows,
            rows,
            cut,
            full,
            full,
            cut,
            full,
            cut,
            full,
            cut,
            full,
            full,
            full,
            full,
            full,
            full,
            full,
        ),
        out_specs=(
            rows,
            rows,
            cut,
            full,
            full,
            cut,
            full,
            cut,
            full,
            cut,
            full,
            full,
            full,
            full,
            full,
            full,
        ),
        check_vma=False,
    )
```

```python
import functools

import jax
import jax.numpy as jnp
from jax import lax
from jax.experimental import pallas as pl
from jax.experimental.pallas import tpu as pltpu
from jax.sharding import PartitionSpec as P

epsilon = 1e-05
f32 = jnp.float32
bf16 = jnp.bfloat16


def dot_nn(a, b):
    return lax.dot_general(a, b, (((1,), (0,)), ((), ())), preferred_element_type=f32)


def dot_nt(a, b):
    return lax.dot_general(a, b, (((1,), (1,)), ((), ())), preferred_element_type=f32)


def dot_tn(a, b):
    return lax.dot_general(a, b, (((0,), (0,)), ((), ())), preferred_element_type=f32)


def norm_parts(values):
    center = values - jnp.mean(values, axis=-1, keepdims=True)
    inverse = lax.rsqrt(jnp.mean(center * center, axis=-1, keepdims=True) + epsilon)
    return center * inverse, inverse


def fold_rows(values):
    rows, cols = values.shape
    return jnp.sum(values.reshape(rows // 8, 8, cols), axis=0)


def gelu_pair(upper):
    phi = 0.5 + 0.5 * lax.erf(upper * 0.7071067811865476)
    bell = jnp.exp(upper * upper * -0.5) * 0.3989422804014327
    return upper * phi, phi + upper * bell


def compute_kernel(
    dims,
    x_hbm,
    dy_hbm,
    wqkv_shard,
    wproj_shard,
    w1_shard,
    w2_shard,
    query_bias_ref,
    value_bias_ref,
    proj_bias_ref,
    hidden_bias_ref,
    output_bias_ref,
    gain1_ref,
    shift1_ref,
    gain2_ref,
    shift2_ref,
    table_ref,
    index_ref,
    y_hbm,
    dx_hbm,
    mixed_hbm,
    act_w_hbm,
    normal_w_hbm,
    work0_ref,
    work1_ref,
    work2_ref,
    work3_ref,
    work4_ref,
    work5_ref,
    total_ref,
    in_ref,
    y_ref,
    dx_ref,
    dwqkv_ref,
    dwproj_ref,
    dw1_ref,
    dw2t_ref,
    small_ref,
    dbias_ref,
    bias_ref,
    perm_ref,
    back_ref,
    act_w_ref,
    column_ref,
    qkv_ref,
    mixed_w_ref,
    mixed_ref,
    lse_ref,
    wide_ref,
    sa_ref,
    sat_ref,
    dyt_ref,
    u_ref,
    da_ref,
    plane_ref,
    names_ref,
    rows_ref,
    act_ref,
    dup_ref,
    wqkv_ref,
    wproj_ref,
    w1_ref,
    w2_ref,
    out0_ref,
    in0_ref,
    in1_ref,
    in2_ref,
    in3_ref,
    in4_ref,
    in5_ref,
    far0_ref,
    far1_ref,
    far2_ref,
    far3_ref,
    far4_ref,
    far5_ref,
    half0_ref,
    half1_ref,
    half2_ref,
    half3_ref,
    half4_ref,
    half5_ref,
    total_in_ref,
    own_sem,
    pair_send,
    pair_recv,
    chip_send,
    chip_recv,
    load_sem,
    y_sem,
    mixed_sem,
    act_w_sem,
    normal_w_sem,
    dx_sem,
    core_send,
    core_recv,
    far_send,
    far_recv,
    half_send,
    half_recv,
    join_send,
    join_recv,
    total_send,
    total_recv,
):
    tokens, windows, width, heads, hidden, shards, reps = dims
    me = lax.axis_index("shard")
    chips = shards // 2
    core = lax.rem(me, 2)
    chip = me // 2
    pair = chip * 2 + 1 - core

    def peer(k):
        return lax.rem(chip + k, chips) * 2 + core

    def owner(k, side):
        return lax.rem(chip + chips - k, chips) * 2 + side

    gathers = (
        (wqkv_shard, wqkv_ref, slice(0, wqkv_ref.shape[1] // 2)),
        (wqkv_shard, wqkv_ref, slice(wqkv_ref.shape[1] // 2, wqkv_ref.shape[1])),
        (wproj_shard, wproj_ref, slice(0, wproj_ref.shape[1])),
        (w1_shard, w1_ref, slice(0, w1_ref.shape[1])),
        (w2_shard, w2_ref, slice(0, w2_ref.shape[1])),
    )

    def block(ref, index, cols):
        size = ref.shape[0] // shards
        return ref.at[pl.ds(pl.multiple_of(index * size, size), size), cols]

    def own_copy(i):
        shard, full, cols = gathers[i]
        return pltpu.make_async_copy(shard.at[:, cols], block(full, me, cols), own_sem.at[i])

    def chip_copy(i, k):
        shard, full, cols = gathers[i]
        return pltpu.make_async_remote_copy(
            src_ref=shard.at[:, cols],
            dst_ref=block(full, me, cols),
            send_sem=chip_send.at[i, k - 1],
            recv_sem=chip_recv.at[i, k - 1],
            device_id={"shard": peer(k)},
            device_id_type=pl.DeviceIdType.MESH,
        )

    def pair_copy(i, k):
        shard, full, cols = gathers[i]
        return pltpu.make_async_remote_copy(
            src_ref=shard.at[:, cols] if k == 0 else block(full, owner(k, core), cols),
            dst_ref=block(full, owner(k, core), cols),
            send_sem=pair_send.at[i, k],
            recv_sem=pair_recv.at[i, k],
            device_id={"shard": pair},
            device_id_type=pl.DeviceIdType.MESH,
        )

    def gather_start(i):
        own_copy(i).start()
        for k in range(1, chips):
            chip_copy(i, k).start()
        pair_copy(i, 0).start()

    def gather_relay(i):
        for k in range(1, chips):
            chip_copy(i, k).wait_recv()
            pair_copy(i, k).start()

    def gather_finish(i):
        own_copy(i).wait()
        for k in range(chips):
            pair_copy(i, k).wait_recv()

    def gather_drain(i):
        for k in range(1, chips):
            chip_copy(i, k).wait_send()
        for k in range(chips):
            pair_copy(i, k).wait_send()

    rep = lax.axis_index("rep")
    bits = reps.bit_length() - 1

    near = min(bits, 3)
    near_size = 1 << near
    far_bits = list(range(near, bits))

    def flipped(index, distance, span):
        for b in range(span):
            if distance >> b & 1:
                index = index + (1 - 2 * lax.rem(index // (1 << b), 2)) * (1 << b)
        return index

    shard_span = shards.bit_length() - 1
    barrier = pltpu.get_barrier_semaphore()
    greeted = [{"shard": flipped(me, d, shard_span)} for d in range(1, shards)]
    greeted += [{"rep": flipped(rep, d, near)} for d in range(1, near_size)]
    greeted += [{"rep": flipped(rep, 1 << b, bits)} for b in far_bits]
    for target in greeted:
        pl.semaphore_signal(
            barrier, inc=1, device_id=target, device_id_type=pl.DeviceIdType.MESH
        )
    pl.semaphore_wait(barrier, len(greeted))
    gather_start(0)
    gather_start(1)

    head_size = width // heads
    scale = head_size ** (-0.5)
    pad = 64
    key_rows = 56
    sub = 8
    group = 2 * sub
    groups = windows // group
    quad = 128 // head_size
    quads = heads // quad
    rows8 = tokens * sub
    rows = tokens * group
    rows_w = sub * pad
    chunk = width
    step = 7
    lane_head = lax.broadcasted_iota(jnp.int32, (pad, 128), 1) // head_size
    head_masks = [lane_head == h for h in range(quad)]
    head_masks_half = [m.astype(f32).astype(bf16) for m in head_masks]

    base = {}
    at = 0
    for name, size in (
        ("qb", width),
        ("vb", width),
        ("pb", width),
        ("hb", hidden),
        ("ob", width),
        ("g1", width),
        ("s1", width),
        ("g2", width),
        ("s2", width),
    ):
        base[name] = (at, size)
        at += size

    def add_small(name, value, offset=0):
        start = base[name][0] + offset
        cols = pl.ds(start, value.shape[1])
        small_ref[:, cols] = small_ref[:, cols] + value

    def load(source, g, slot):
        return pltpu.make_async_copy(
            source.at[:, pl.ds(pl.multiple_of(g * group, group), group), :],
            in_ref.at[slot],
            load_sem.at[slot],
        )

    def store(source, target, g, sem):
        return pltpu.make_async_copy(
            source, target.at[:, pl.ds(pl.multiple_of(g * group, group), group), :], sem
        )

    def mixed_load(g):
        return pltpu.make_async_copy(
            mixed_hbm.at[:, pl.ds(pl.multiple_of(g * group, group), group), :], mixed_ref, mixed_sem
        )

    def act_w_store(g2, slot):
        return pltpu.make_async_copy(act_w_ref.at[slot], act_w_hbm.at[g2], act_w_sem.at[slot])

    def act_w_load(g2, slot):
        return pltpu.make_async_copy(act_w_hbm.at[g2], act_w_ref.at[slot], act_w_sem.at[slot])

    def normal_stage(slot):
        return mixed_w_ref if slot == 0 else out0_ref.at[0]

    def normal_w_store(g2, slot):
        return pltpu.make_async_copy(
            normal_stage(slot), normal_w_hbm.at[g2], normal_w_sem.at[slot]
        )

    def normal_w_load(g2, slot):
        return pltpu.make_async_copy(
            normal_w_hbm.at[g2], act_w_ref.at[slot], normal_w_sem.at[slot]
        )

    load(x_hbm, 0, 0).start()

    owned = width // shards
    works = (work0_ref, work1_ref, work2_ref, work3_ref, work4_ref, work5_ref)
    ins = (in0_ref, in1_ref, in2_ref, in3_ref, in4_ref, in5_ref)
    fars = (far0_ref, far1_ref, far2_ref, far3_ref, far4_ref, far5_ref)
    halves = (half0_ref, half1_ref, half2_ref, half3_ref, half4_ref, half5_ref)

    def unit_pieces(u, s):
        own = pl.ds(pl.multiple_of(s * owned, owned), owned)
        if u == 0:
            for i in range(hidden // width):
                cols = slice(width * i, width * (i + 1))
                yield owned * i, owned, (lambda cols=cols: dw1_ref[own, cols])
        elif u == 1:
            size = hidden // shards
            for i in range(size // 256):
                lanes = pl.ds(pl.multiple_of(s * size + i * 256, 256), 256)
                yield i * 256, 256, (lambda lanes=lanes: dw2t_ref[:, lanes].T)
        elif u == 2:
            yield 0, owned, (lambda: dwproj_ref[own, :])
        else:
            cols = slice(width * (u - 3), width * (u - 2))
            name = ("qb", "s1", "vb")[u - 3]
            sums = small_ref[0:1, base[name][0] : base[name][0] + width]
            yield 0, owned, (
                lambda: dwqkv_ref[own, cols] * column_ref[0, own, 0:1]
                + column_ref[1, own, 0:1] * sums
            )

    def unit_out(u, j):
        rows_u = works[u].shape[0]
        if u == 0:
            return mixed_w_ref.at[0:rows_u] if j == 0 else out0_ref.at[j - 1]
        if u == 1:
            return act_ref.at[0:rows_u, j * width : (j + 1) * width]
        first = (u - 2) * owned
        return act_ref.at[
            first : first + owned, (chips + j) * width : (chips + j + 1) * width
        ]

    def core_copy(u, j):
        return pltpu.make_async_remote_copy(
            src_ref=unit_out(u, j),
            dst_ref=ins[u].at[j],
            send_sem=core_send.at[u, j],
            recv_sem=core_recv.at[u, j],
            device_id={"shard": pair},
            device_id_type=pl.DeviceIdType.MESH,
        )

    def levels(u):
        if u < 2 and near == 3:
            return [(0, 1), (1, 2)]
        return [(0, near)]

    def level_index(u, at_level):
        low, count = levels(u)[at_level]
        return lax.rem(rep // (1 << low), 1 << count)

    def held(u, at_level):
        size = works[u].shape[0]
        start = 0
        for k in range(at_level):
            size >>= levels(u)[k][1]
            start = start + level_index(u, k) * size
        return start, size

    def lines_of(start, size):
        return pl.ds(start if isinstance(start, int) else pl.multiple_of(start, 16), size)

    def own_piece(u):
        return lines_of(*held(u, len(levels(u))))

    def peers_of(u, at_level):
        slot = 0
        row = 0
        for k in range(at_level):
            others = (1 << levels(u)[k][1]) - 1
            slot += others
            row += others * held(u, k + 1)[1]
        low, count = levels(u)[at_level]
        size = held(u, at_level + 1)[1]
        return [
            (d, slot + d - 1, row + (d - 1) * size, {"rep": flipped(rep, d << low, bits)})
            for d in range(1, 1 << count)
        ]

    def far_copy(u, k):
        return pltpu.make_async_remote_copy(
            src_ref=ins[u].at[lax.rem(chip + k, chips)],
            dst_ref=fars[u].at[k - 1],
            send_sem=far_send.at[u, k - 1],
            recv_sem=far_recv.at[u, k - 1],
            device_id={"shard": peer(k)},
            device_id_type=pl.DeviceIdType.MESH,
        )

    def spread_copy(u, at_level, link):
        d, slot, row, partner = link
        start, _ = held(u, at_level)
        size = held(u, at_level + 1)[1]
        index = flipped(level_index(u, at_level), d, levels(u)[at_level][1])
        return pltpu.make_async_remote_copy(
            src_ref=ins[u].at[chip, lines_of(start + index * size, size), :],
            dst_ref=halves[u].at[pl.ds(row, size), :],
            send_sem=half_send.at[u, slot],
            recv_sem=half_recv.at[u, slot],
            device_id=partner,
            device_id_type=pl.DeviceIdType.MESH,
        )

    def double_copy(u, b):
        slot = near_size - 1 + b - near
        size = works[u].shape[0] // near_size
        return pltpu.make_async_remote_copy(
            src_ref=ins[u].at[chip, own_piece(u), :],
            dst_ref=halves[u].at[pl.ds(slot * size, size), :],
            send_sem=half_send.at[u, slot],
            recv_sem=half_recv.at[u, slot],
            device_id={"rep": flipped(rep, 1 << b, bits)},
            device_id_type=pl.DeviceIdType.MESH,
        )

    def join_copy(u, at_level, link):
        d, slot, row, partner = link
        lines = lines_of(*held(u, at_level + 1))
        return pltpu.make_async_remote_copy(
            src_ref=works[u].at[lines, :],
            dst_ref=works[u].at[lines, :],
            send_sem=join_send.at[u, slot],
            recv_sem=join_recv.at[u, slot],
            device_id=partner,
            device_id_type=pl.DeviceIdType.MESH,
        )

    def level_start(u, at_level):
        for link in peers_of(u, at_level):
            spread_copy(u, at_level, link).start()

    def join_start(u, at_level):
        for link in peers_of(u, at_level):
            join_copy(u, at_level, link).start()

    def unit_stage(u, stage):
        if stage == 0:
            for j in range(chips):
                target = unit_out(u, j)
                for r0, nr, value in unit_pieces(u, 2 * j + 1 - core):
                    target[r0 : r0 + nr, :] = value().astype(bf16)
                core_copy(u, j).start()
            return
        if stage == 1:
            for j in range(chips):
                core_copy(u, j).wait()
            for k in range(1, chips + 1):
                j = lax.rem(chip + k, chips)
                for r0, nr, value in unit_pieces(u, 2 * j + core):
                    got = ins[u][j, r0 : r0 + nr, :].astype(f32)
                    ins[u][j, r0 : r0 + nr, :] = (value() + got).astype(bf16)
                if k == chips - 1:
                    for n in range(1, chips):
                        far_copy(u, n).start()
            return
        if stage == 2:
            for k in range(1, chips):
                far_copy(u, k).wait()
            total = ins[u][chip].astype(f32)
            for k in range(1, chips):
                total = total + fars[u][k - 1].astype(f32)
            ins[u][chip] = total.astype(bf16)
            level_start(u, 0)
            return
        count = len(levels(u))
        at_level = stage - 3
        if at_level < count:
            lines = lines_of(*held(u, at_level + 1))
            size = held(u, at_level + 1)[1]
            total = ins[u][chip, lines, :].astype(f32)
            for link in peers_of(u, at_level):
                spread_copy(u, at_level, link).wait()
                total = total + halves[u][link[2] : link[2] + size, :].astype(f32)
            if at_level + 1 < count:
                ins[u][chip, lines, :] = total.astype(bf16)
                level_start(u, at_level + 1)
            elif far_bits:
                ins[u][chip, lines, :] = total.astype(bf16)
                double_copy(u, far_bits[0]).start()
            else:
                works[u][lines, :] = total.astype(bf16)
                join_start(u, count - 1)
            return
        at_double = at_level - count
        if at_double < len(far_bits):
            b = far_bits[at_double]
            double_copy(u, b).wait()
            size = works[u].shape[0] // near_size
            row = (near_size - 1 + b - near) * size
            total = ins[u][chip, own_piece(u), :].astype(f32) + halves[u][
                row : row + size, :
            ].astype(f32)
            if b != far_bits[-1]:
                ins[u][chip, own_piece(u), :] = total.astype(bf16)
                double_copy(u, b + 1).start()
            else:
                works[u][own_piece(u), :] = total.astype(bf16)
                join_start(u, count - 1)
            return
        at_join = count - 1 - (at_double - len(far_bits))
        if at_join >= 0:
            for link in peers_of(u, at_join):
                join_copy(u, at_join, link).wait()
            if at_join > 0:
                join_start(u, at_join - 1)

    stages = 7 + len(far_bits)

    total_steps = 3 + len(far_bits)
    share = total_ref.shape[0] // shards

    def total_share(index):
        return total_ref.at[pl.ds(pl.multiple_of(index * share, share), share), :]

    def total_copies(step):
        if step == 0 or step == total_steps - 1:
            first = 0 if step == 0 else shards - 2 + near_size + len(far_bits)
            links = [
                (first + d - 1, flipped(me, d, shard_span), {"shard": flipped(me, d, shard_span)})
                for d in range(1, shards)
            ]
        elif step == 1:
            links = [
                (shards + d - 2, me, {"rep": flipped(rep, d, near)}) for d in range(1, near_size)
            ]
        else:
            b = far_bits[step - 2]
            links = [(shards + near_size + step - 4, me, {"rep": flipped(rep, 1 << b, bits)})]
        return [
            (
                at_slot,
                other,
                pltpu.make_async_remote_copy(
                    src_ref=total_share(other if step == 0 else me),
                    dst_ref=total_in_ref.at[at_slot],
                    send_sem=total_send.at[at_slot],
                    recv_sem=total_recv.at[at_slot],
                    device_id=target,
                    device_id_type=pl.DeviceIdType.MESH,
                ),
            )
            for at_slot, other, target in links
        ]

    def total_start(step):
        for _, _, copy in total_copies(step):
            copy.start()

    def total_finish(step):
        if step == total_steps - 1:
            for at_slot, other, copy in total_copies(step):
                copy.wait()
                total_share(other)[...] = total_in_ref[at_slot]
            return
        values = [total_share(me)[...]]
        for at_slot, _, copy in total_copies(step):
            copy.wait()
            values.append(total_in_ref[at_slot])
        while len(values) > 1:
            values = [values[i] + values[i + 1] for i in range(0, len(values), 2)]
        total_share(me)[...] = values[0]
        total_start(step + 1)

    small_ref[...] = jnp.zeros(small_ref.shape, f32)
    dbias_ref[...] = jnp.zeros(dbias_ref.shape, f32)
    for i, ref in enumerate((gain1_ref, shift1_ref)):
        column_ref[i] = jnp.broadcast_to(ref[...], (128, width)).T
    sat_ref[width:, :] = (
        lax.broadcasted_iota(jnp.int32, (16, rows), 0) == 0
    ).astype(f32).astype(bf16)

    @pl.loop(0, width // 32)
    def _(n):
        lines = pl.ds(pl.multiple_of(n * 32, 32), 32)
        dwqkv_ref[lines, :] = jnp.zeros((32, 3 * width), f32)
        dwproj_ref[lines, :] = jnp.zeros((32, width), f32)
        dw1_ref[lines, :] = jnp.zeros((32, hidden), f32)
        dw2t_ref[lines, :] = jnp.zeros((32, hidden), f32)

    @pl.loop(0, rows_w // 64)
    def _(n):
        start = pl.multiple_of(n * 64, 64)
        to = lax.broadcasted_iota(jnp.int32, (64, rows8), 0) + start
        source = lax.broadcasted_iota(jnp.int32, (64, rows8), 1)
        hit = (to // pad == source % sub) & (to % pad == source // sub)
        perm_ref[pl.ds(start, 64), :] = hit.astype(f32).astype(bf16)

    @pl.loop(0, rows8 // 56)
    def _(n):
        start = pl.multiple_of(n * 56, 8)
        to = lax.broadcasted_iota(jnp.int32, (56, rows_w), 0) + start
        source = lax.broadcasted_iota(jnp.int32, (56, rows_w), 1)
        hit = (source // pad == to % sub) & (source % pad == to // sub)
        back_ref[pl.ds(start, 56), :] = hit.astype(f32).astype(bf16)

    table_tall = heads // 2
    table_rows = table_ref.shape[1]
    table_lanes = -(-table_rows // 128) * 128
    row_iota = lax.broadcasted_iota(jnp.int32, (table_lanes, 128), 0).astype(f32)
    low_lanes = lax.broadcasted_iota(jnp.int32, (key_rows, 128), 1) < pad
    rows_ref[...] = jnp.zeros(rows_ref.shape, f32)
    rows_ref[:, 0:table_rows] = table_ref[...]
    names_ref[...] = jnp.full(names_ref.shape, -1.0, f32)
    names_ref[0:tokens, 0:tokens] = index_ref[...].astype(f32)
    names_ref[...] = names_ref[...].T

    def named(j):
        return (row_iota == names_ref[pl.ds(j, 1), :]).astype(f32).astype(bf16)

    table = rows_ref[...]
    high = table.astype(bf16)
    middle = (table - high.astype(f32)).astype(bf16)
    low = (table - high.astype(f32) - middle.astype(f32)).astype(bf16)
    plane_ref[...] = jnp.full(plane_ref.shape, -1e30, f32)

    def plane(h):
        return plane_ref.at[h * key_rows : (h + 1) * key_rows, :]

    @pl.loop(0, tokens)
    def _(j):
        hit = named(j)
        line = (dot_nn(high, hit) + dot_nn(middle, hit)) + dot_nn(low, hit)
        plane_ref[pl.ds(j, heads, stride=key_rows), :] = line

    for t in range(quads):
        for h in range(quad // 2):
            left = plane(t * quad + 2 * h)[...]
            right = plane(t * quad + 2 * h + 1)[...]
            bias_ref[t, :, 128 * h : 128 * (h + 1)] = jnp.where(
                low_lanes, left, pltpu.roll(right, pad, 1)
            )

    def stacked(tile):
        return jnp.concatenate([tile * m for m in head_masks_half], axis=0)

    def diagonal(tall):
        total = tall[0:pad]
        for h in range(1, quad):
            total = jnp.where(head_masks[h], tall[h * pad : (h + 1) * pad], total)
        return total

    def grow(values):
        return jnp.concatenate([values, jnp.zeros((pad - key_rows, values.shape[1]), f32)], axis=0)

    @pl.loop(0, groups)
    def _(g):
        slot = lax.rem(g, 2)
        load(x_hbm, g, slot).wait()
        load(x_hbm, lax.rem(g + 1, groups), 1 - slot).start()

        @pl.when(g == groups - 1)
        def _():
            gather_relay(0)

        @pl.loop(0, tokens // step)
        def _(n):
            part = in_ref[slot, pl.ds(n * step, step)].astype(f32)
            flat = part.reshape(step * group, width)
            normal, _ = norm_parts(flat)
            wide_ref[pl.ds(n * step, step)] = (normal * gain1_ref[...] + shift1_ref[...]).reshape(
                step, group, width
            )
            lines = pl.ds(pl.multiple_of(n * step * group, step * group), step * group)
            u_ref[lines, :] = normal

        for s in range(2):
            act8 = wide_ref[:, sub * s : sub * (s + 1), :].reshape(rows8, width).astype(bf16)

            @pl.when(g != 0)
            def _():
                act_w_store(2 * g - 2 + s, s).wait()
                normal_w_store(2 * g - 2 + s, s).wait()

            act_w_ref[s] = dot_nn(perm_ref[...], act8).astype(bf16)
            act_w_store(2 * g + s, s).start()
            normal8 = u_ref[...].reshape(tokens, group, width)[:, sub * s : sub * (s + 1), :]
            normal_stage(s)[...] = dot_nn(
                perm_ref[...], normal8.reshape(rows8, width).astype(bf16)
            ).astype(bf16)
            normal_w_store(2 * g + s, s).start()

    for s in range(2):
        act_w_store(2 * groups - 2 + s, s).wait()
        normal_w_store(2 * groups - 2 + s, s).wait()
    act_w_load(0, 0).start()
    gather_relay(1)
    for i in range(2, 5):
        gather_start(i)
    for i in range(2):
        gather_finish(i)

    @pl.loop(0, groups)
    def _(g):
        win0 = pl.multiple_of(g * group, group)
        slot = lax.rem(groups + g, 2)
        load(x_hbm, g, slot).wait()

        @pl.when(g < groups - 1)
        def _():
            load(x_hbm, g + 1, 1 - slot).start()

        @pl.when(g == groups - 1)
        def _():
            load(dy_hbm, 0, 1 - slot).start()
            gather_relay(3)

        @pl.loop(0, 2)
        def _(s):
            g2 = g * 2 + s
            act_w_load(g2, s).wait()

            @pl.when(g2 < 2 * groups - 1)
            def _():
                act_w_load(g2 + 1, 1 - s).start()

            for n in range(3):
                cols = slice(n * width, (n + 1) * width)
                out = dot_nn(act_w_ref[s], wqkv_ref[:, cols])
                if n == 0:
                    out = (out + query_bias_ref[...]) * scale
                if n == 2:
                    out = out + value_bias_ref[...]
                qkv_ref[g2, :, cols] = out.astype(bf16)

            @pl.loop(0, sub // 4)
            def _(wi):
                items = []
                for e in range(4):
                    w = wi * 4 + e
                    line = pl.ds(pl.multiple_of(w * pad, pad), pad)
                    items += [(w, line, t) for t in range(quads)]
                for first in range(0, len(items), 8):
                    batch = items[first : first + 8]
                    scores = [
                        dot_nt(
                            qkv_ref[g2, line, width + 128 * t : width + 128 * (t + 1)],
                            stacked(qkv_ref[g2, line, 128 * t : 128 * (t + 1)]),
                        )[0:key_rows]
                        + bias_ref[t]
                        for w, line, t in batch
                    ]
                    tops = [jnp.max(x, axis=0, keepdims=True) for x in scores]
                    weights = [jnp.exp(x - top) for x, top in zip(scores, tops)]
                    totals = [jnp.sum(x, axis=0, keepdims=True) for x in weights]
                    for (w, line, t), top, total in zip(batch, tops, totals):
                        lse_ref[g2, w, t : t + 1, :] = top + jnp.log(total)
                    probs = [
                        grow(x * (1.0 / total)).astype(bf16) for x, total in zip(weights, totals)
                    ]
                    mixes = [
                        dot_tn(
                            x, qkv_ref[g2, line, 2 * width + 128 * t : 2 * width + 128 * (t + 1)]
                        )
                        for x, (w, line, t) in zip(probs, batch)
                    ]
                    for x, (w, line, t) in zip(mixes, batch):
                        mixed_w_ref[line, 128 * t : 128 * (t + 1)] = diagonal(x).astype(bf16)

            wide_ref[:, pl.ds(pl.multiple_of(sub * s, sub), sub), :] = dot_nn(
                back_ref[...], mixed_w_ref[...]
            ).reshape(tokens, sub, width)

        @pl.when(g != 0)
        def _():
            store(mixed_ref, mixed_hbm, g - 1, mixed_sem).wait()

        @pl.when(g == 0)
        def _():
            gather_relay(2)
            gather_finish(2)

        @pl.when(g == groups - 1)
        def _():
            gather_relay(4)

        mixed_ref[...] = wide_ref[...].astype(bf16)
        store(mixed_ref, mixed_hbm, g, mixed_sem).start()
        out = dot_nn(mixed_ref[...].reshape(rows, width), wproj_ref[...]) + proj_bias_ref[...]
        dx_ref[:, pl.ds(win0, group), :] = in_ref[slot].astype(f32) + out.reshape(
            tokens, group, width
        )

    gather_finish(3)
    gather_finish(4)
    for i in range(5):
        gather_drain(i)
    store(mixed_ref, mixed_hbm, groups - 1, mixed_sem).wait()

    @pl.loop(0, groups)
    def _(g):
        win0 = pl.multiple_of(g * group, group)
        slot = lax.rem(2 * groups + g, 2)
        load(dy_hbm, g, slot).wait()

        @pl.when(g < groups - 1)
        def _():
            load(dy_hbm, g + 1, 1 - slot).start()

        @pl.when(g == groups - 1)
        def _():
            load(x_hbm, 0, 1 - slot).start()

        @pl.when(g != 0)
        def _():
            store(y_ref, y_hbm, g - 1, y_sem).wait()

        mixed_load(g).start()

        @pl.loop(0, tokens // step)
        def _(n):
            part = dx_ref[pl.ds(n * step, step), pl.ds(win0, group), :].reshape(step * group, width)
            normal, _ = norm_parts(part)
            lines = pl.ds(pl.multiple_of(n * step * group, step * group), step * group)
            sa_ref[lines, :] = (normal * gain2_ref[...] + shift2_ref[...]).astype(bf16)

        sat_ref[0:width, :] = sa_ref[...].T
        dyt_ref[...] = in_ref[slot].reshape(rows, width).T

        count = hidden // chunk
        columns = [slice(i * chunk, (i + 1) * chunk) for i in range(count)]

        def rise(i):
            u_ref[...] = dot_nn(sa_ref[...], w1_ref[:, columns[i]])
            da_ref[...] = dot_nt(in_ref[slot].reshape(rows, width), w2_ref[columns[i], :])

        def bend(i):
            for m in range(tokens // step):
                lines = slice(m * step * group, (m + 1) * step * group)
                value, slope = gelu_pair(u_ref[lines, :] + hidden_bias_ref[:, columns[i]])
                act_ref[lines, columns[i]] = value.astype(bf16)
                dup_ref[lines, columns[i]] = (da_ref[lines, :] * slope).astype(bf16)

        def gather_grads(i):
            cols = columns[i]
            part1 = dot_nn(sat_ref[...], dup_ref[:, cols])
            dw1_ref[:, cols] += part1[0:width]
            add_small("hb", part1[width : width + 8], cols.start)
            dw2t_ref[:, cols] += dot_nn(dyt_ref[...], act_ref[:, cols])

        rise(0)
        for i in range(count):
            bend(i)
            if i > 0:
                gather_grads(i - 1)
            if i + 1 < count:
                rise(i + 1)
        gather_grads(count - 1)

        @pl.when(g == groups - 1)
        def _():
            unit_stage(0, 0)

        out = dot_nn(act_ref[...], w2_ref[...]) + output_bias_ref[...]
        y_ref[...] = (
            dx_ref[:, pl.ds(win0, group), :] + out.reshape(tokens, group, width)
        ).astype(bf16)
        wide_ref[...] = dot_nt(dup_ref[...], w1_ref[...]).reshape(tokens, group, width)

        @pl.when(g == groups - 1)
        def _():
            unit_stage(1, 0)

        store(y_ref, y_hbm, g, y_sem).start()

        @pl.loop(0, tokens // step)
        def _(n):
            lines = pl.ds(pl.multiple_of(n * step * group, step * group), step * group)
            normal, inverse = norm_parts(
                dx_ref[pl.ds(n * step, step), pl.ds(win0, group), :].reshape(step * group, width)
            )
            grad = wide_ref[pl.ds(n * step, step)].reshape(step * group, width)
            scaled = grad * gain2_ref[...]
            back = inverse * (
                scaled
                - jnp.mean(scaled, axis=-1, keepdims=True)
                - normal * jnp.mean(scaled * normal, axis=-1, keepdims=True)
            )
            cot = in_ref[slot, pl.ds(n * step, step)].astype(f32).reshape(step * group, width)
            total = cot + back
            dx_ref[pl.ds(n * step, step), pl.ds(win0, group), :] = total.reshape(step, group, width)
            sa_ref[lines, :] = total.astype(bf16)
            add_small("ob", fold_rows(cot))
            add_small("pb", fold_rows(total))
            add_small("g2", fold_rows(grad * normal))
            add_small("s2", fold_rows(grad))

        @pl.when(g == groups - 1)
        def _():
            unit_stage(0, 1)

        mixed_load(g).wait()
        dwproj_ref[...] += dot_tn(mixed_ref[...].reshape(rows, width), sa_ref[...])

    store(y_ref, y_hbm, groups - 1, y_sem).wait()
    unit_stage(1, 1)
    unit_stage(2, 0)
    normal_w_load(0, 0).start()

    plan = {0: ((2, 1),), 5: ((0, 2),), 6: ((1, 2),), 7: ((2, 2),), 8: ((0, 3),), 9: ((1, 3),), 10: ((2, 3),), 11: ((0, 4),)}

    def progress(g2, half):
        for point, calls in plan.items():
            if point % 2 == half:

                @pl.when(g2 == point // 2)
                def _():
                    for u, stage in calls:
                        unit_stage(u, stage)

    subs = 2 * groups

    @pl.loop(0, subs)
    def _(g2):
        s = lax.rem(g2, 2)
        half8 = dx_ref[:, pl.ds(pl.multiple_of(g2 * sub, sub), sub), :]
        half_w = dot_nn(perm_ref[...], half8.reshape(rows8, width).astype(bf16)).astype(bf16)
        mixed_w_ref[...] = dot_nt(half_w, wproj_ref[...]).astype(bf16)
        progress(g2, 0)

        @pl.loop(0, sub // 2)
        def _(wi):
            items = []
            for e in range(2):
                w = wi * 2 + e
                line = pl.ds(pl.multiple_of(w * pad, pad), pad)
                for t in range(quads):
                    cols = [
                        slice(i * width + 128 * t, i * width + 128 * (t + 1)) for i in range(3)
                    ]
                    items.append((w, line, t, cols))
            for first in range(0, len(items), 8):
                batch = items[first : first + 8]
                queries = [stacked(qkv_ref[g2, line, c[0]]) for w, line, t, c in batch]
                scores = [
                    dot_nt(qkv_ref[g2, line, c[1]], x)[0:key_rows] + bias_ref[t]
                    for x, (w, line, t, c) in zip(queries, batch)
                ]
                grads = [stacked(mixed_w_ref[line, c[0]]) for w, line, t, c in batch]
                prob_grads = [
                    dot_nt(qkv_ref[g2, line, c[2]], x)[0:key_rows]
                    for x, (w, line, t, c) in zip(grads, batch)
                ]
                probs = [
                    jnp.exp(x - lse_ref[g2, w, t : t + 1, :])
                    for x, (w, line, t, c) in zip(scores, batch)
                ]
                prob_halves = [grow(x).astype(bf16) for x in probs]
                value_grads = [dot_nn(x, y) for x, y in zip(prob_halves, grads)]
                deltas = [
                    jnp.sum(x * y, axis=0, keepdims=True) for x, y in zip(probs, prob_grads)
                ]
                score_grads = [
                    x * (y - delta) for x, y, delta in zip(probs, prob_grads, deltas)
                ]
                for x, (w, line, t, c) in zip(score_grads, batch):
                    dbias_ref[t] += x
                halves_ = [grow(x).astype(bf16) for x in score_grads]
                key_grads = [dot_nn(x, y) for x, y in zip(halves_, queries)]
                query_grads = [
                    dot_tn(x, qkv_ref[g2, line, c[1]])
                    for x, (w, line, t, c) in zip(halves_, batch)
                ]
                for k, (w, line, t, c) in enumerate(batch):
                    qkv_ref[g2, line, c[0]] = (diagonal(query_grads[k]) * scale).astype(bf16)
                    qkv_ref[g2, line, c[1]] = key_grads[k].astype(bf16)
                    qkv_ref[g2, line, c[2]] = value_grads[k].astype(bf16)

        progress(g2, 1)
        normal_w_load(g2, s).wait()

        @pl.when(g2 < subs - 1)
        def _():
            normal_w_load(g2 + 1, 1 - s).start()

        sat_ref[0:width, 0:rows_w] = act_w_ref[s].T
        for n in range(3):
            cols = slice(n * width, (n + 1) * width)
            part = dot_nn(sat_ref[:, 0:rows_w], qkv_ref[g2, :, cols])
            dwqkv_ref[:, cols] += part[0:width]
            add_small(("qb", "s1", "vb")[n], part[width : width + 8])

            @pl.when(g2 == subs - 1)
            def _():
                unit_stage(3 + n, 0)
                if n == 2:
                    unit_stage(3, 1)

    for t in range(quads):
        for h in range(quad // 2):
            both = dbias_ref[t, :, 128 * h : 128 * (h + 1)]
            plane(t * quad + 2 * h)[...] = jnp.where(low_lanes, both, 0.0)
            plane(t * quad + 2 * h + 1)[...] = jnp.where(
                low_lanes, pltpu.roll(both, pad, 1), 0.0
            )
    total_ref[...] = jnp.zeros(total_ref.shape, f32)

    @pl.loop(0, tokens)
    def _(j):
        hit = named(j)
        line = plane_ref[pl.ds(j, heads, stride=key_rows), :]
        upper_half = line.astype(bf16)
        lower_half = (line - upper_half.astype(f32)).astype(bf16)
        found = dot_nt(upper_half, hit) + dot_nt(lower_half, hit)
        for side in range(2):
            lanes = slice(side * table_lanes, (side + 1) * table_lanes)
            total_ref[0:table_tall, lanes] = (
                total_ref[0:table_tall, lanes] + found[side * table_tall : (side + 1) * table_tall]
            )

    for u in range(4, 6):
        unit_stage(u, 1)
    weighted = jnp.zeros((width, 128), f32)
    for n in range(3 * width // 128):
        lanes = slice(n * 128, (n + 1) * 128)
        weighted = weighted + dwqkv_ref[:, lanes] * wqkv_ref[:, lanes].astype(f32)
    add_small("g1", fold_rows(weighted.T))
    merged_sums = jnp.concatenate(
        [small_ref[:, base[n][0] : base[n][0] + width] for n in ("qb", "s1", "vb")], axis=1
    )
    sums_high = merged_sums.astype(bf16)
    sums_low = (merged_sums - sums_high.astype(f32)).astype(bf16)
    small_ref[:, base["s1"][0] : base["s1"][0] + width] = dot_nt(
        sums_high, wqkv_ref[...]
    ) + dot_nt(sums_low, wqkv_ref[...])

    def put_sums(first, last):
        for i in range(first, last):
            total_ref[table_tall + i : table_tall + i + 1, :] = jnp.sum(
                small_ref[:, i * width : (i + 1) * width], axis=0, keepdims=True
            )

    put_sums(0, small_ref.shape[1] // width)
    total_start(0)
    plan2 = {0: ((1, 4),), 1: ((3, 2), (2, 4), (-1, 0)), 2: ((0, 5), (4, 2)), 3: ((5, 2),), 4: ((1, 5), (-1, 1)), 5: ((3, 3),)}

    @pl.loop(0, groups)
    def _(g):
        win0 = pl.multiple_of(g * group, group)
        slot = lax.rem(3 * groups + g, 2)
        load(x_hbm, g, slot).wait()

        @pl.when(g < groups - 1)
        def _():
            load(x_hbm, g + 1, 1 - slot).start()

        for s in range(2):
            g2 = g * 2 + s
            mixed_w_ref[...] = dot_nt(qkv_ref[g2], wqkv_ref[...]).astype(bf16)
            wide_ref[:, sub * s : sub * (s + 1), :] = dot_nn(back_ref[...], mixed_w_ref[...]).reshape(
                tokens, sub, width
            )
            for point, calls in plan2.items():
                if point % 2 == s:

                    @pl.when(g == point // 2)
                    def _():
                        for u, stage in calls:
                            if u < 0:
                                total_finish(stage)
                            else:
                                unit_stage(u, stage)

        @pl.loop(0, tokens // step)
        def _(n):
            part = in_ref[slot, pl.ds(n * step, step)].astype(f32)
            normal, inverse = norm_parts(part.reshape(step * group, width))
            grad = wide_ref[pl.ds(n * step, step)].reshape(step * group, width)
            scaled = grad * gain1_ref[...]
            back = inverse * (
                scaled
                - jnp.mean(scaled, axis=-1, keepdims=True)
                - normal * jnp.mean(scaled * normal, axis=-1, keepdims=True)
            )
            dx_ref[pl.ds(n * step, step), pl.ds(win0, group), :] += back.reshape(step, group, width)

        @pl.when(g != 0)
        def _():
            store(y_ref, dx_hbm, g - 1, dx_sem).wait()

        y_ref[...] = dx_ref[:, pl.ds(win0, group), :].astype(bf16)
        store(y_ref, dx_hbm, g, dx_sem).start()

    done = {0: 5, 1: 5, 2: 4, 3: 3, 4: 2, 5: 2}
    for stage in range(2, stages):
        for u in (3, 4, 5, 2, 0, 1):
            if stage > done[u]:
                unit_stage(u, stage)
    for step_at in range(2, total_steps):
        total_finish(step_at)
    store(y_ref, dx_hbm, groups - 1, dx_sem).wait()


def local_pass(x, dy, wqkv, wproj, w1, w2, vectors, table, index, shards, reps):
    tokens, windows, width = x.shape
    hidden = w1.shape[1]
    heads = table.shape[0]
    dims = (tokens, windows, width, heads, hidden, shards, reps)
    chips = shards // 2
    bits = reps.bit_length() - 1
    sub = 8
    group = 2 * sub
    pad = 64
    rows = tokens * group
    small_size = 8 * width + hidden
    subs = windows // sub
    owned = width // shards
    unit_rows = (hidden // shards, hidden // shards, owned, owned, owned, owned)
    near_size = 1 << min(bits, 3)
    slots = near_size - 1 + bits - min(bits, 3)
    total_rows = -(-(heads // 2 + small_size // width) // (8 * shards)) * 8 * shards
    shapes = (
        [
            jax.ShapeDtypeStruct(x.shape, bf16),
            jax.ShapeDtypeStruct(x.shape, bf16),
            jax.ShapeDtypeStruct(x.shape, bf16),
            jax.ShapeDtypeStruct((subs, sub * pad, width), bf16),
            jax.ShapeDtypeStruct((subs, sub * pad, width), bf16),
        ]
        + [jax.ShapeDtypeStruct((r, width), bf16) for r in unit_rows]
        + [jax.ShapeDtypeStruct((total_rows, width), f32)]
    )
    vmem = pl.BlockSpec(memory_space=pltpu.VMEM)
    hbm = pl.BlockSpec(memory_space=pl.ANY)

    return pl.pallas_call(
        functools.partial(compute_kernel, dims),
        out_shape=shapes,
        in_specs=[hbm] * 6 + [vmem] * 11,
        out_specs=[hbm] * 5 + [vmem] * 7,
        scratch_shapes=[
            pltpu.VMEM((2, tokens, group, width), bf16),
            pltpu.VMEM((tokens, group, width), bf16),
            pltpu.VMEM(x.shape, f32),
            pltpu.VMEM((width, 3 * width), f32),
            pltpu.VMEM((width, width), f32),
            pltpu.VMEM((width, hidden), f32),
            pltpu.VMEM((width, hidden), f32),
            pltpu.VMEM((8, small_size), f32),
            pltpu.VMEM((heads // 4, 56, 256), f32),
            pltpu.VMEM((heads // 4, 56, 256), f32),
            pltpu.VMEM((sub * pad, tokens * sub), bf16),
            pltpu.VMEM((tokens * sub, sub * pad), bf16),
            pltpu.VMEM((2, sub * pad, width), bf16),
            pltpu.VMEM((2, width, 128), f32),
            pltpu.VMEM((subs, sub * pad, 3 * width), bf16),
            pltpu.VMEM((sub * pad, width), bf16),
            pltpu.VMEM((tokens, group, width), bf16),
            pltpu.VMEM((subs, sub, heads // 4, 256), f32),
            pltpu.VMEM((tokens, group, width), f32),
            pltpu.VMEM((rows, width), bf16),
            pltpu.VMEM((width + 16, rows), bf16),
            pltpu.VMEM((width, rows), bf16),
            pltpu.VMEM((rows, width), f32),
            pltpu.VMEM((rows, width), f32),
            pltpu.VMEM((heads * 56, 128), f32),
            pltpu.VMEM((128, 128), f32),
            pltpu.VMEM((heads, -(-table.shape[1] // 128) * 128), f32),
            pltpu.VMEM((rows, hidden), bf16),
            pltpu.VMEM((rows, hidden), bf16),
            pltpu.VMEM((width, 3 * width), bf16),
            pltpu.VMEM((width, width), bf16),
            pltpu.VMEM((width, hidden), bf16),
            pltpu.VMEM((hidden, width), bf16),
            pltpu.VMEM((chips - 1, unit_rows[0], width), bf16),
            *[pltpu.VMEM((chips, r, width), bf16) for r in unit_rows],
            *[pltpu.VMEM((chips - 1, r, width), bf16) for r in unit_rows],
            *[pltpu.VMEM((slots * r // near_size, width), bf16) for r in unit_rows],
            pltpu.VMEM((2 * shards - 2 + slots, total_rows // shards, width), f32),
            pltpu.SemaphoreType.DMA((5,)),
            pltpu.SemaphoreType.DMA((5, chips)),
            pltpu.SemaphoreType.DMA((5, chips)),
            pltpu.SemaphoreType.DMA((5, chips - 1)),
            pltpu.SemaphoreType.DMA((5, chips - 1)),
            pltpu.SemaphoreType.DMA((2,)),
            pltpu.SemaphoreType.DMA,
            pltpu.SemaphoreType.DMA,
            pltpu.SemaphoreType.DMA((2,)),
            pltpu.SemaphoreType.DMA((2,)),
            pltpu.SemaphoreType.DMA,
            pltpu.SemaphoreType.DMA((6, chips)),
            pltpu.SemaphoreType.DMA((6, chips)),
            pltpu.SemaphoreType.DMA((6, chips - 1)),
            pltpu.SemaphoreType.DMA((6, chips - 1)),
            pltpu.SemaphoreType.DMA((6, slots)),
            pltpu.SemaphoreType.DMA((6, slots)),
            pltpu.SemaphoreType.DMA((6, slots)),
            pltpu.SemaphoreType.DMA((6, slots)),
            pltpu.SemaphoreType.DMA((2 * shards - 2 + slots,)),
            pltpu.SemaphoreType.DMA((2 * shards - 2 + slots,)),
        ],
        compiler_params=pltpu.CompilerParams(
            vmem_limit_bytes=67043328, collective_id=0, has_side_effects=True
        ),
    )(x, dy, wqkv, wproj, w1, w2, *vectors, table, index)


def spread_kernel(heads, sizes, *refs):
    works = refs[:6]
    total_ref, y_in, dx_in = refs[6:9]
    dwqkv_ref, dwproj_ref, dw1_ref, dw2_ref, table_ref = refs[9:14]
    sums = refs[14:-2]
    y_ref, dx_ref = refs[-2:]
    width = dwproj_ref.shape[1]
    owned = dwproj_ref.shape[0]
    y_ref[...] = y_in[...]
    dx_ref[...] = dx_in[...].astype(f32)

    @pl.when(pl.program_id(0) == 0)
    def _():
        for i in range(dw1_ref.shape[1] // width):
            dw1_ref[:, i * width : (i + 1) * width] = works[0][
                i * owned : (i + 1) * owned, :
            ].astype(f32)
        dw2_ref[...] = works[1][...].astype(f32)
        dwproj_ref[...] = works[2][...].astype(f32)
        for i in range(3):
            dwqkv_ref[:, i * width : (i + 1) * width] = works[3 + i][...].astype(f32)
        tall = heads // 2
        rows_t = table_ref.shape[1]
        lanes = total_ref.shape[1] // 2
        table_ref[0:tall, :] = total_ref[0:tall, 0:rows_t]
        table_ref[tall:heads, :] = total_ref[0:tall, lanes : lanes + rows_t]
        row = tall
        for ref, size in zip(sums, sizes):
            for i in range(size // width):
                ref[:, i * width : (i + 1) * width] = total_ref[row : row + 1, :]
                row += 1


def spread(works, total, y, dx, hidden, heads, table_rows):
    tokens, windows, width = y.shape
    owned = works[2].shape[0]
    sizes = (width, width, width, hidden, width, width, width, width, width)
    shapes = [
        (owned, 3 * width),
        (owned, width),
        (owned, hidden),
        works[1].shape,
        (heads, table_rows),
    ] + [(1, size) for size in sizes]
    step = 7
    slab = pl.BlockSpec((step, windows, width), lambda i: (i, 0, 0))
    whole = lambda shape: pl.BlockSpec(shape, lambda i: (0, 0))
    return pl.pallas_call(
        functools.partial(spread_kernel, heads, sizes),
        grid=(tokens // step,),
        out_shape=[jax.ShapeDtypeStruct(shape, f32) for shape in shapes]
        + [jax.ShapeDtypeStruct(y.shape, bf16), jax.ShapeDtypeStruct(y.shape, f32)],
        in_specs=[whole(w.shape) for w in works] + [whole(total.shape), slab, slab],
        out_specs=[whole(shape) for shape in shapes] + [slab, slab],
    )(*works, total, y, dx)


def on_device(
    shards,
    reps,
    block_input,
    out_grad,
    qkv_weight,
    query_bias,
    value_bias,
    proj_weight,
    proj_bias,
    hidden_weight,
    hidden_bias,
    output_weight,
    output_bias,
    first_gain,
    first_shift,
    second_gain,
    second_shift,
    bias_table,
    table_index,
):
    windows, tokens, width = block_input.shape
    table_rows, heads = bias_table.shape
    hidden = hidden_bias.shape[0]
    vectors = [
        v.reshape(1, -1)
        for v in (
            query_bias,
            value_bias,
            proj_bias,
            hidden_bias,
            output_bias,
            first_gain,
            first_shift,
            second_gain,
            second_shift,
        )
    ]
    y, dx, _, _, _, *works, total = local_pass(
        jnp.transpose(block_input, (1, 0, 2)),
        jnp.transpose(out_grad, (1, 0, 2)),
        qkv_weight,
        proj_weight,
        hidden_weight,
        output_weight,
        vectors,
        bias_table.T,
        table_index,
        shards,
        reps,
    )
    (dwqkv, dwproj, dw1, dw2, table_grad, qb, vb, pb, hb, ob, g1, s1, g2, s2, y, dx) = spread(
        works, total, y, dx, hidden, heads, table_rows
    )
    return (
        jnp.transpose(y, (1, 0, 2)),
        jnp.transpose(dx, (1, 0, 2)),
        dwqkv,
        qb.reshape(-1),
        vb.reshape(-1),
        dwproj,
        pb.reshape(-1),
        dw1,
        hb.reshape(-1),
        dw2,
        ob.reshape(-1),
        g1.reshape(-1),
        s1.reshape(-1),
        g2.reshape(-1),
        s2.reshape(-1),
        table_grad.T,
    )


def solution(mesh):
    rows = P(("shard", "rep"), None, None)
    cut = P("shard", None)
    full = P()
    return jax.shard_map(
        functools.partial(on_device, mesh.shape["shard"], mesh.shape["rep"]),
        mesh=mesh,
        in_specs=(
            rows,
            rows,
            cut,
            full,
            full,
            cut,
            full,
            cut,
            full,
            cut,
            full,
            full,
            full,
            full,
            full,
            full,
            full,
        ),
        out_specs=(
            rows,
            rows,
            cut,
            full,
            full,
            cut,
            full,
            cut,
            full,
            cut,
            full,
            full,
            full,
            full,
            full,
            full,
        ),
        check_vma=False,
    )
```

```python
import functools

import jax
import jax.numpy as jnp
from jax import lax
from jax.experimental import pallas as pl
from jax.experimental.pallas import tpu as pltpu
from jax.sharding import PartitionSpec as P

epsilon = 1e-05
f32 = jnp.float32
bf16 = jnp.bfloat16


def dot_nn(a, b):
    return lax.dot_general(a, b, (((1,), (0,)), ((), ())), preferred_element_type=f32)


def dot_nt(a, b):
    return lax.dot_general(a, b, (((1,), (1,)), ((), ())), preferred_element_type=f32)


def dot_tn(a, b):
    return lax.dot_general(a, b, (((0,), (0,)), ((), ())), preferred_element_type=f32)


def norm_parts(values):
    center = values - jnp.mean(values, axis=-1, keepdims=True)
    inverse = lax.rsqrt(jnp.mean(center * center, axis=-1, keepdims=True) + epsilon)
    return center * inverse, inverse


def fold_rows(values):
    rows, cols = values.shape
    return jnp.sum(values.reshape(rows // 8, 8, cols), axis=0)


def gelu_pair(upper):
    phi = 0.5 + 0.5 * lax.erf(upper * 0.7071067811865476)
    bell = jnp.exp(upper * upper * -0.5) * 0.3989422804014327
    return upper * phi, phi + upper * bell


def compute_kernel(
    dims,
    x_hbm,
    dy_hbm,
    wqkv_shard,
    wproj_shard,
    w1_shard,
    w2_shard,
    query_bias_ref,
    value_bias_ref,
    proj_bias_ref,
    hidden_bias_ref,
    output_bias_ref,
    gain1_ref,
    shift1_ref,
    gain2_ref,
    shift2_ref,
    table_ref,
    index_ref,
    y_hbm,
    dx_hbm,
    mixed_hbm,
    act_w_hbm,
    normal_w_hbm,
    work0_ref,
    work1_ref,
    work2_ref,
    work3_ref,
    work4_ref,
    work5_ref,
    total_ref,
    in_ref,
    y_ref,
    dx_ref,
    dwqkv_ref,
    dwproj_ref,
    dw1_ref,
    dw2t_ref,
    small_ref,
    dbias_ref,
    bias_ref,
    perm_ref,
    back_ref,
    act_w_ref,
    column_ref,
    qkv_ref,
    mixed_w_ref,
    mixed_ref,
    lse_ref,
    wide_ref,
    sa_ref,
    sat_ref,
    dyt_ref,
    u_ref,
    da_ref,
    plane_ref,
    names_ref,
    rows_ref,
    act_ref,
    dup_ref,
    wqkv_ref,
    wproj_ref,
    w1_ref,
    w2_ref,
    out0_ref,
    in0_ref,
    in1_ref,
    in2_ref,
    in3_ref,
    in4_ref,
    in5_ref,
    far0_ref,
    far1_ref,
    far2_ref,
    far3_ref,
    far4_ref,
    far5_ref,
    half0_ref,
    half1_ref,
    half2_ref,
    half3_ref,
    half4_ref,
    half5_ref,
    total_in_ref,
    own_sem,
    pair_send,
    pair_recv,
    chip_send,
    chip_recv,
    load_sem,
    y_sem,
    mixed_sem,
    act_w_sem,
    normal_w_sem,
    dx_sem,
    core_send,
    core_recv,
    far_send,
    far_recv,
    half_send,
    half_recv,
    join_send,
    join_recv,
    total_send,
    total_recv,
):
    tokens, windows, width, heads, hidden, shards, reps = dims
    me = lax.axis_index("shard")
    chips = shards // 2
    core = lax.rem(me, 2)
    chip = me // 2
    pair = chip * 2 + 1 - core

    def peer(k):
        return lax.rem(chip + k, chips) * 2 + core

    def owner(k, side):
        return lax.rem(chip + chips - k, chips) * 2 + side

    gathers = (
        (wqkv_shard, wqkv_ref, slice(0, wqkv_ref.shape[1] // 2)),
        (wqkv_shard, wqkv_ref, slice(wqkv_ref.shape[1] // 2, wqkv_ref.shape[1])),
        (wproj_shard, wproj_ref, slice(0, wproj_ref.shape[1])),
        (w1_shard, w1_ref, slice(0, w1_ref.shape[1])),
        (w2_shard, w2_ref, slice(0, w2_ref.shape[1])),
    )

    def block(ref, index, cols):
        size = ref.shape[0] // shards
        return ref.at[pl.ds(pl.multiple_of(index * size, size), size), cols]

    def own_copy(i):
        shard, full, cols = gathers[i]
        return pltpu.make_async_copy(shard.at[:, cols], block(full, me, cols), own_sem.at[i])

    def chip_copy(i, k):
        shard, full, cols = gathers[i]
        return pltpu.make_async_remote_copy(
            src_ref=shard.at[:, cols],
            dst_ref=block(full, me, cols),
            send_sem=chip_send.at[i, k - 1],
            recv_sem=chip_recv.at[i, k - 1],
            device_id={"shard": peer(k)},
            device_id_type=pl.DeviceIdType.MESH,
        )

    def pair_copy(i, k):
        shard, full, cols = gathers[i]
        return pltpu.make_async_remote_copy(
            src_ref=shard.at[:, cols] if k == 0 else block(full, owner(k, core), cols),
            dst_ref=block(full, owner(k, core), cols),
            send_sem=pair_send.at[i, k],
            recv_sem=pair_recv.at[i, k],
            device_id={"shard": pair},
            device_id_type=pl.DeviceIdType.MESH,
        )

    def gather_start(i):
        own_copy(i).start()
        for k in range(1, chips):
            chip_copy(i, k).start()
        pair_copy(i, 0).start()

    def gather_relay(i):
        for k in range(1, chips):
            chip_copy(i, k).wait_recv()
            pair_copy(i, k).start()

    def gather_finish(i):
        own_copy(i).wait()
        for k in range(chips):
            pair_copy(i, k).wait_recv()

    def gather_drain(i):
        for k in range(1, chips):
            chip_copy(i, k).wait_send()
        for k in range(chips):
            pair_copy(i, k).wait_send()

    rep = lax.axis_index("rep")
    bits = reps.bit_length() - 1

    near = min(bits, 3)
    near_size = 1 << near
    far_bits = list(range(near, bits))

    def flipped(index, distance, span):
        for b in range(span):
            if distance >> b & 1:
                index = index + (1 - 2 * lax.rem(index // (1 << b), 2)) * (1 << b)
        return index

    shard_span = shards.bit_length() - 1
    barrier = pltpu.get_barrier_semaphore()
    greeted = [{"shard": flipped(me, d, shard_span)} for d in range(1, shards)]
    greeted += [{"rep": flipped(rep, d, near)} for d in range(1, near_size)]
    greeted += [{"rep": flipped(rep, 1 << b, bits)} for b in far_bits]
    for target in greeted:
        pl.semaphore_signal(
            barrier, inc=1, device_id=target, device_id_type=pl.DeviceIdType.MESH
        )
    pl.semaphore_wait(barrier, len(greeted))
    gather_start(0)
    gather_start(1)

    head_size = width // heads
    scale = head_size ** (-0.5)
    pad = 64
    key_rows = 56
    sub = 8
    group = 2 * sub
    groups = windows // group
    quad = 128 // head_size
    quads = heads // quad
    rows8 = tokens * sub
    rows = tokens * group
    rows_w = sub * pad
    chunk = width
    step = 7
    lane_head = lax.broadcasted_iota(jnp.int32, (pad, 128), 1) // head_size
    head_masks = [lane_head == h for h in range(quad)]
    head_masks_half = [m.astype(f32).astype(bf16) for m in head_masks]

    base = {}
    at = 0
    for name, size in (
        ("qb", width),
        ("vb", width),
        ("pb", width),
        ("hb", hidden),
        ("ob", width),
        ("g1", width),
        ("s1", width),
        ("g2", width),
        ("s2", width),
    ):
        base[name] = (at, size)
        at += size

    def add_small(name, value, offset=0):
        start = base[name][0] + offset
        cols = pl.ds(start, value.shape[1])
        small_ref[:, cols] = small_ref[:, cols] + value

    def load(source, g, slot):
        return pltpu.make_async_copy(
            source.at[:, pl.ds(pl.multiple_of(g * group, group), group), :],
            in_ref.at[slot],
            load_sem.at[slot],
        )

    def store(source, target, g, sem):
        return pltpu.make_async_copy(
            source, target.at[:, pl.ds(pl.multiple_of(g * group, group), group), :], sem
        )

    def mixed_load(g):
        return pltpu.make_async_copy(
            mixed_hbm.at[:, pl.ds(pl.multiple_of(g * group, group), group), :], mixed_ref, mixed_sem
        )

    def act_w_store(g2, slot):
        return pltpu.make_async_copy(act_w_ref.at[slot], act_w_hbm.at[g2], act_w_sem.at[slot])

    def act_w_load(g2, slot):
        return pltpu.make_async_copy(act_w_hbm.at[g2], act_w_ref.at[slot], act_w_sem.at[slot])

    def normal_stage(slot):
        return mixed_w_ref if slot == 0 else out0_ref.at[0]

    def normal_w_store(g2, slot):
        return pltpu.make_async_copy(
            normal_stage(slot), normal_w_hbm.at[g2], normal_w_sem.at[slot]
        )

    def normal_w_load(g2, slot):
        return pltpu.make_async_copy(
            normal_w_hbm.at[g2], act_w_ref.at[slot], normal_w_sem.at[slot]
        )

    load(x_hbm, 0, 0).start()

    owned = width // shards
    works = (work0_ref, work1_ref, work2_ref, work3_ref, work4_ref, work5_ref)
    ins = (in0_ref, in1_ref, in2_ref, in3_ref, in4_ref, in5_ref)
    fars = (far0_ref, far1_ref, far2_ref, far3_ref, far4_ref, far5_ref)
    halves = (half0_ref, half1_ref, half2_ref, half3_ref, half4_ref, half5_ref)

    def unit_pieces(u, s):
        own = pl.ds(pl.multiple_of(s * owned, owned), owned)
        if u == 0:
            for i in range(hidden // width):
                cols = slice(width * i, width * (i + 1))
                yield owned * i, owned, (lambda cols=cols: dw1_ref[own, cols])
        elif u == 1:
            size = hidden // shards
            for i in range(size // 256):
                lanes = pl.ds(pl.multiple_of(s * size + i * 256, 256), 256)
                yield i * 256, 256, (lambda lanes=lanes: dw2t_ref[:, lanes].T)
        elif u == 2:
            yield 0, owned, (lambda: dwproj_ref[own, :])
        else:
            cols = slice(width * (u - 3), width * (u - 2))
            name = ("qb", "s1", "vb")[u - 3]
            sums = small_ref[0:1, base[name][0] : base[name][0] + width]
            yield 0, owned, (
                lambda: dwqkv_ref[own, cols] * column_ref[0, own, 0:1]
                + column_ref[1, own, 0:1] * sums
            )

    def unit_out(u, j):
        rows_u = works[u].shape[0]
        if u == 0:
            return mixed_w_ref.at[0:rows_u] if j == 0 else out0_ref.at[j - 1]
        if u == 1:
            return act_ref.at[0:rows_u, j * width : (j + 1) * width]
        first = (u - 2) * owned
        return act_ref.at[
            first : first + owned, (chips + j) * width : (chips + j + 1) * width
        ]

    def core_copy(u, j):
        return pltpu.make_async_remote_copy(
            src_ref=unit_out(u, j),
            dst_ref=ins[u].at[j],
            send_sem=core_send.at[u, j],
            recv_sem=core_recv.at[u, j],
            device_id={"shard": pair},
            device_id_type=pl.DeviceIdType.MESH,
        )

    def levels(u):
        if u < 2 and near == 3:
            return [(0, 1), (1, 2)]
        return [(0, near)]

    def level_index(u, at_level):
        low, count = levels(u)[at_level]
        return lax.rem(rep // (1 << low), 1 << count)

    def held(u, at_level):
        size = works[u].shape[0]
        start = 0
        for k in range(at_level):
            size >>= levels(u)[k][1]
            start = start + level_index(u, k) * size
        return start, size

    def lines_of(start, size):
        return pl.ds(start if isinstance(start, int) else pl.multiple_of(start, 16), size)

    def own_piece(u):
        return lines_of(*held(u, len(levels(u))))

    def peers_of(u, at_level):
        slot = 0
        row = 0
        for k in range(at_level):
            others = (1 << levels(u)[k][1]) - 1
            slot += others
            row += others * held(u, k + 1)[1]
        low, count = levels(u)[at_level]
        size = held(u, at_level + 1)[1]
        return [
            (d, slot + d - 1, row + (d - 1) * size, {"rep": flipped(rep, d << low, bits)})
            for d in range(1, 1 << count)
        ]

    def far_copy(u, k):
        return pltpu.make_async_remote_copy(
            src_ref=ins[u].at[lax.rem(chip + k, chips)],
            dst_ref=fars[u].at[k - 1],
            send_sem=far_send.at[u, k - 1],
            recv_sem=far_recv.at[u, k - 1],
            device_id={"shard": peer(k)},
            device_id_type=pl.DeviceIdType.MESH,
        )

    def spread_copy(u, at_level, link):
        d, slot, row, partner = link
        start, _ = held(u, at_level)
        size = held(u, at_level + 1)[1]
        index = flipped(level_index(u, at_level), d, levels(u)[at_level][1])
        return pltpu.make_async_remote_copy(
            src_ref=ins[u].at[chip, lines_of(start + index * size, size), :],
            dst_ref=halves[u].at[pl.ds(row, size), :],
            send_sem=half_send.at[u, slot],
            recv_sem=half_recv.at[u, slot],
            device_id=partner,
            device_id_type=pl.DeviceIdType.MESH,
        )

    def double_copy(u, b):
        slot = near_size - 1 + b - near
        size = works[u].shape[0] // near_size
        return pltpu.make_async_remote_copy(
            src_ref=ins[u].at[chip, own_piece(u), :],
            dst_ref=halves[u].at[pl.ds(slot * size, size), :],
            send_sem=half_send.at[u, slot],
            recv_sem=half_recv.at[u, slot],
            device_id={"rep": flipped(rep, 1 << b, bits)},
            device_id_type=pl.DeviceIdType.MESH,
        )

    def join_copy(u, at_level, link):
        d, slot, row, partner = link
        lines = lines_of(*held(u, at_level + 1))
        return pltpu.make_async_remote_copy(
            src_ref=works[u].at[lines, :],
            dst_ref=works[u].at[lines, :],
            send_sem=join_send.at[u, slot],
            recv_sem=join_recv.at[u, slot],
            device_id=partner,
            device_id_type=pl.DeviceIdType.MESH,
        )

    def level_start(u, at_level):
        for link in peers_of(u, at_level):
            spread_copy(u, at_level, link).start()

    def join_start(u, at_level):
        for link in peers_of(u, at_level):
            join_copy(u, at_level, link).start()

    def unit_stage(u, stage):
        if stage == 0:
            for j in range(chips):
                target = unit_out(u, j)
                for r0, nr, value in unit_pieces(u, 2 * j + 1 - core):
                    target[r0 : r0 + nr, :] = value().astype(bf16)
                core_copy(u, j).start()
            return
        if stage == 1:
            for j in range(chips):
                core_copy(u, j).wait()
            for k in range(1, chips + 1):
                j = lax.rem(chip + k, chips)
                for r0, nr, value in unit_pieces(u, 2 * j + core):
                    got = ins[u][j, r0 : r0 + nr, :].astype(f32)
                    ins[u][j, r0 : r0 + nr, :] = (value() + got).astype(bf16)
                if k == chips - 1:
                    for n in range(1, chips):
                        far_copy(u, n).start()
            return
        if stage == 2:
            for k in range(1, chips):
                far_copy(u, k).wait()
            total = ins[u][chip].astype(f32)
            for k in range(1, chips):
                total = total + fars[u][k - 1].astype(f32)
            ins[u][chip] = total.astype(bf16)
            level_start(u, 0)
            return
        count = len(levels(u))
        at_level = stage - 3
        if at_level < count:
            lines = lines_of(*held(u, at_level + 1))
            size = held(u, at_level + 1)[1]
            total = ins[u][chip, lines, :].astype(f32)
            for link in peers_of(u, at_level):
                spread_copy(u, at_level, link).wait()
                total = total + halves[u][link[2] : link[2] + size, :].astype(f32)
            if at_level + 1 < count:
                ins[u][chip, lines, :] = total.astype(bf16)
                level_start(u, at_level + 1)
            elif far_bits:
                ins[u][chip, lines, :] = total.astype(bf16)
                double_copy(u, far_bits[0]).start()
            else:
                works[u][lines, :] = total.astype(bf16)
                join_start(u, count - 1)
            return
        at_double = at_level - count
        if at_double < len(far_bits):
            b = far_bits[at_double]
            double_copy(u, b).wait()
            size = works[u].shape[0] // near_size
            row = (near_size - 1 + b - near) * size
            total = ins[u][chip, own_piece(u), :].astype(f32) + halves[u][
                row : row + size, :
            ].astype(f32)
            if b != far_bits[-1]:
                ins[u][chip, own_piece(u), :] = total.astype(bf16)
                double_copy(u, b + 1).start()
            else:
                works[u][own_piece(u), :] = total.astype(bf16)
                join_start(u, count - 1)
            return
        at_join = count - 1 - (at_double - len(far_bits))
        if at_join >= 0:
            for link in peers_of(u, at_join):
                join_copy(u, at_join, link).wait()
            if at_join > 0:
                join_start(u, at_join - 1)

    stages = 7 + len(far_bits)

    total_steps = 3 + len(far_bits)
    share = total_ref.shape[0] // shards

    def total_share(index):
        return total_ref.at[pl.ds(pl.multiple_of(index * share, share), share), :]

    def total_copies(step):
        if step == 0 or step == total_steps - 1:
            first = 0 if step == 0 else shards - 2 + near_size + len(far_bits)
            links = [
                (first + d - 1, flipped(me, d, shard_span), {"shard": flipped(me, d, shard_span)})
                for d in range(1, shards)
            ]
        elif step == 1:
            links = [
                (shards + d - 2, me, {"rep": flipped(rep, d, near)}) for d in range(1, near_size)
            ]
        else:
            b = far_bits[step - 2]
            links = [(shards + near_size + step - 4, me, {"rep": flipped(rep, 1 << b, bits)})]
        return [
            (
                at_slot,
                other,
                pltpu.make_async_remote_copy(
                    src_ref=total_share(other if step == 0 else me),
                    dst_ref=total_in_ref.at[at_slot],
                    send_sem=total_send.at[at_slot],
                    recv_sem=total_recv.at[at_slot],
                    device_id=target,
                    device_id_type=pl.DeviceIdType.MESH,
                ),
            )
            for at_slot, other, target in links
        ]

    def total_start(step):
        for _, _, copy in total_copies(step):
            copy.start()

    def total_finish(step):
        if step == total_steps - 1:
            for at_slot, other, copy in total_copies(step):
                copy.wait()
                total_share(other)[...] = total_in_ref[at_slot]
            return
        values = [total_share(me)[...]]
        for at_slot, _, copy in total_copies(step):
            copy.wait()
            values.append(total_in_ref[at_slot])
        while len(values) > 1:
            values = [values[i] + values[i + 1] for i in range(0, len(values), 2)]
        total_share(me)[...] = values[0]
        total_start(step + 1)

    small_ref[...] = jnp.zeros(small_ref.shape, f32)
    dbias_ref[...] = jnp.zeros(dbias_ref.shape, f32)
    for i, ref in enumerate((gain1_ref, shift1_ref)):
        column_ref[i] = jnp.broadcast_to(ref[...], (128, width)).T
    sat_ref[width:, :] = (
        lax.broadcasted_iota(jnp.int32, (16, rows), 0) == 0
    ).astype(f32).astype(bf16)

    @pl.loop(0, width // 32)
    def _(n):
        lines = pl.ds(pl.multiple_of(n * 32, 32), 32)
        dwqkv_ref[lines, :] = jnp.zeros((32, 3 * width), f32)
        dwproj_ref[lines, :] = jnp.zeros((32, width), f32)
        dw1_ref[lines, :] = jnp.zeros((32, hidden), f32)
        dw2t_ref[lines, :] = jnp.zeros((32, hidden), f32)

    @pl.loop(0, rows_w // 64)
    def _(n):
        start = pl.multiple_of(n * 64, 64)
        to = lax.broadcasted_iota(jnp.int32, (64, rows8), 0) + start
        source = lax.broadcasted_iota(jnp.int32, (64, rows8), 1)
        hit = (to // pad == source % sub) & (to % pad == source // sub)
        perm_ref[pl.ds(start, 64), :] = hit.astype(f32).astype(bf16)

    @pl.loop(0, rows8 // 56)
    def _(n):
        start = pl.multiple_of(n * 56, 8)
        to = lax.broadcasted_iota(jnp.int32, (56, rows_w), 0) + start
        source = lax.broadcasted_iota(jnp.int32, (56, rows_w), 1)
        hit = (source // pad == to % sub) & (source % pad == to // sub)
        back_ref[pl.ds(start, 56), :] = hit.astype(f32).astype(bf16)

    table_tall = heads // 2
    table_rows = table_ref.shape[1]
    table_lanes = -(-table_rows // 128) * 128
    row_iota = lax.broadcasted_iota(jnp.int32, (table_lanes, 128), 0).astype(f32)
    low_lanes = lax.broadcasted_iota(jnp.int32, (key_rows, 128), 1) < pad
    rows_ref[...] = jnp.zeros(rows_ref.shape, f32)
    rows_ref[:, 0:table_rows] = table_ref[...]
    names_ref[...] = jnp.full(names_ref.shape, -1.0, f32)
    names_ref[0:tokens, 0:tokens] = index_ref[...].astype(f32)
    names_ref[...] = names_ref[...].T

    def named(j):
        return (row_iota == names_ref[pl.ds(j, 1), :]).astype(f32).astype(bf16)

    table = rows_ref[...]
    high = table.astype(bf16)
    middle = (table - high.astype(f32)).astype(bf16)
    low = (table - high.astype(f32) - middle.astype(f32)).astype(bf16)
    plane_ref[...] = jnp.full(plane_ref.shape, -1e30, f32)

    def plane(h):
        return plane_ref.at[h * key_rows : (h + 1) * key_rows, :]

    @pl.loop(0, tokens)
    def _(j):
        hit = named(j)
        line = (dot_nn(high, hit) + dot_nn(middle, hit)) + dot_nn(low, hit)
        plane_ref[pl.ds(j, heads, stride=key_rows), :] = line

    for t in range(quads):
        for h in range(quad // 2):
            left = plane(t * quad + 2 * h)[...]
            right = plane(t * quad + 2 * h + 1)[...]
            bias_ref[t, :, 128 * h : 128 * (h + 1)] = jnp.where(
                low_lanes, left, pltpu.roll(right, pad, 1)
            )

    def stacked(tile):
        return jnp.concatenate([tile * m for m in head_masks_half], axis=0)

    def diagonal(tall):
        total = tall[0:pad]
        for h in range(1, quad):
            total = jnp.where(head_masks[h], tall[h * pad : (h + 1) * pad], total)
        return total

    def grow(values):
        return jnp.concatenate([values, jnp.zeros((pad - key_rows, values.shape[1]), f32)], axis=0)

    @pl.loop(0, groups)
    def _(g):
        slot = lax.rem(g, 2)
        load(x_hbm, g, slot).wait()
        load(x_hbm, lax.rem(g + 1, groups), 1 - slot).start()

        @pl.when(g == groups - 1)
        def _():
            gather_relay(0)

        @pl.loop(0, tokens // step)
        def _(n):
            part = in_ref[slot, pl.ds(n * step, step)].astype(f32)
            flat = part.reshape(step * group, width)
            normal, _ = norm_parts(flat)
            wide_ref[pl.ds(n * step, step)] = (normal * gain1_ref[...] + shift1_ref[...]).reshape(
                step, group, width
            )
            lines = pl.ds(pl.multiple_of(n * step * group, step * group), step * group)
            u_ref[lines, :] = normal

        for s in range(2):
            act8 = wide_ref[:, sub * s : sub * (s + 1), :].reshape(rows8, width).astype(bf16)

            @pl.when(g != 0)
            def _():
                act_w_store(2 * g - 2 + s, s).wait()
                normal_w_store(2 * g - 2 + s, s).wait()

            act_w_ref[s] = dot_nn(perm_ref[...], act8).astype(bf16)
            act_w_store(2 * g + s, s).start()
            normal8 = u_ref[...].reshape(tokens, group, width)[:, sub * s : sub * (s + 1), :]
            normal_stage(s)[...] = dot_nn(
                perm_ref[...], normal8.reshape(rows8, width).astype(bf16)
            ).astype(bf16)
            normal_w_store(2 * g + s, s).start()

    for s in range(2):
        act_w_store(2 * groups - 2 + s, s).wait()
        normal_w_store(2 * groups - 2 + s, s).wait()
    act_w_load(0, 0).start()
    gather_relay(1)
    for i in range(2, 5):
        gather_start(i)
    for i in range(2):
        gather_finish(i)

    @pl.loop(0, groups)
    def _(g):
        win0 = pl.multiple_of(g * group, group)
        slot = lax.rem(groups + g, 2)
        load(x_hbm, g, slot).wait()

        @pl.when(g < groups - 1)
        def _():
            load(x_hbm, g + 1, 1 - slot).start()

        @pl.when(g == groups - 1)
        def _():
            load(dy_hbm, 0, 1 - slot).start()
            gather_relay(3)

        @pl.loop(0, 2)
        def _(s):
            g2 = g * 2 + s
            act_w_load(g2, s).wait()

            @pl.when(g2 < 2 * groups - 1)
            def _():
                act_w_load(g2 + 1, 1 - s).start()

            for n in range(3):
                cols = slice(n * width, (n + 1) * width)
                out = dot_nn(act_w_ref[s], wqkv_ref[:, cols])
                if n == 0:
                    out = (out + query_bias_ref[...]) * scale
                if n == 2:
                    out = out + value_bias_ref[...]
                qkv_ref[g2, :, cols] = out.astype(bf16)

            @pl.loop(0, sub // 4)
            def _(wi):
                items = []
                for e in range(4):
                    w = wi * 4 + e
                    line = pl.ds(pl.multiple_of(w * pad, pad), pad)
                    items += [(w, line, t) for t in range(quads)]
                for first in range(0, len(items), 8):
                    batch = items[first : first + 8]
                    scores = [
                        dot_nt(
                            qkv_ref[g2, line, width + 128 * t : width + 128 * (t + 1)],
                            stacked(qkv_ref[g2, line, 128 * t : 128 * (t + 1)]),
                        )[0:key_rows]
                        + bias_ref[t]
                        for w, line, t in batch
                    ]
                    tops = [jnp.max(x, axis=0, keepdims=True) for x in scores]
                    weights = [jnp.exp(x - top) for x, top in zip(scores, tops)]
                    totals = [jnp.sum(x, axis=0, keepdims=True) for x in weights]
                    for (w, line, t), top, total in zip(batch, tops, totals):
                        lse_ref[g2, w, t : t + 1, :] = top + jnp.log(total)
                    probs = [
                        grow(x * (1.0 / total)).astype(bf16) for x, total in zip(weights, totals)
                    ]
                    mixes = [
                        dot_tn(
                            x, qkv_ref[g2, line, 2 * width + 128 * t : 2 * width + 128 * (t + 1)]
                        )
                        for x, (w, line, t) in zip(probs, batch)
                    ]
                    for x, (w, line, t) in zip(mixes, batch):
                        mixed_w_ref[line, 128 * t : 128 * (t + 1)] = diagonal(x).astype(bf16)

            wide_ref[:, pl.ds(pl.multiple_of(sub * s, sub), sub), :] = dot_nn(
                back_ref[...], mixed_w_ref[...]
            ).reshape(tokens, sub, width)

        @pl.when(g != 0)
        def _():
            store(mixed_ref, mixed_hbm, g - 1, mixed_sem).wait()

        @pl.when(g == 0)
        def _():
            gather_relay(2)
            gather_finish(2)

        @pl.when(g == groups - 1)
        def _():
            gather_relay(4)

        mixed_ref[...] = wide_ref[...].astype(bf16)
        store(mixed_ref, mixed_hbm, g, mixed_sem).start()
        out = dot_nn(mixed_ref[...].reshape(rows, width), wproj_ref[...]) + proj_bias_ref[...]
        dx_ref[:, pl.ds(win0, group), :] = in_ref[slot].astype(f32) + out.reshape(
            tokens, group, width
        )

    gather_finish(3)
    gather_finish(4)
    for i in range(5):
        gather_drain(i)
    store(mixed_ref, mixed_hbm, groups - 1, mixed_sem).wait()

    @pl.loop(0, groups)
    def _(g):
        win0 = pl.multiple_of(g * group, group)
        slot = lax.rem(2 * groups + g, 2)
        load(dy_hbm, g, slot).wait()

        @pl.when(g < groups - 1)
        def _():
            load(dy_hbm, g + 1, 1 - slot).start()

        @pl.when(g == groups - 1)
        def _():
            load(x_hbm, 0, 1 - slot).start()

        @pl.when(g != 0)
        def _():
            store(y_ref, y_hbm, g - 1, y_sem).wait()

        mixed_load(g).start()

        @pl.loop(0, tokens // step)
        def _(n):
            part = dx_ref[pl.ds(n * step, step), pl.ds(win0, group), :].reshape(step * group, width)
            normal, _ = norm_parts(part)
            lines = pl.ds(pl.multiple_of(n * step * group, step * group), step * group)
            sa_ref[lines, :] = (normal * gain2_ref[...] + shift2_ref[...]).astype(bf16)

        sat_ref[0:width, :] = sa_ref[...].T
        dyt_ref[...] = in_ref[slot].reshape(rows, width).T

        count = hidden // chunk
        columns = [slice(i * chunk, (i + 1) * chunk) for i in range(count)]

        def rise(i):
            u_ref[...] = dot_nn(sa_ref[...], w1_ref[:, columns[i]])
            da_ref[...] = dot_nt(in_ref[slot].reshape(rows, width), w2_ref[columns[i], :])

        def bend(i):
            for m in range(tokens // step):
                lines = slice(m * step * group, (m + 1) * step * group)
                value, slope = gelu_pair(u_ref[lines, :] + hidden_bias_ref[:, columns[i]])
                act_ref[lines, columns[i]] = value.astype(bf16)
                dup_ref[lines, columns[i]] = (da_ref[lines, :] * slope).astype(bf16)

        def gather_grads(i):
            cols = columns[i]
            part1 = dot_nn(sat_ref[...], dup_ref[:, cols])
            dw1_ref[:, cols] += part1[0:width]
            add_small("hb", part1[width : width + 8], cols.start)
            dw2t_ref[:, cols] += dot_nn(dyt_ref[...], act_ref[:, cols])

        rise(0)
        for i in range(count):
            bend(i)
            if i > 0:
                gather_grads(i - 1)
            if i + 1 < count:
                rise(i + 1)
        gather_grads(count - 1)

        @pl.when(g == groups - 1)
        def _():
            unit_stage(0, 0)

        out = dot_nn(act_ref[...], w2_ref[...]) + output_bias_ref[...]
        y_ref[...] = (
            dx_ref[:, pl.ds(win0, group), :] + out.reshape(tokens, group, width)
        ).astype(bf16)
        wide_ref[...] = dot_nt(dup_ref[...], w1_ref[...]).reshape(tokens, group, width)

        @pl.when(g == groups - 1)
        def _():
            unit_stage(1, 0)

        store(y_ref, y_hbm, g, y_sem).start()

        @pl.loop(0, tokens // step)
        def _(n):
            lines = pl.ds(pl.multiple_of(n * step * group, step * group), step * group)
            normal, inverse = norm_parts(
                dx_ref[pl.ds(n * step, step), pl.ds(win0, group), :].reshape(step * group, width)
            )
            grad = wide_ref[pl.ds(n * step, step)].reshape(step * group, width)
            scaled = grad * gain2_ref[...]
            back = inverse * (
                scaled
                - jnp.mean(scaled, axis=-1, keepdims=True)
                - normal * jnp.mean(scaled * normal, axis=-1, keepdims=True)
            )
            cot = in_ref[slot, pl.ds(n * step, step)].astype(f32).reshape(step * group, width)
            total = cot + back
            dx_ref[pl.ds(n * step, step), pl.ds(win0, group), :] = total.reshape(step, group, width)
            sa_ref[lines, :] = total.astype(bf16)
            add_small("ob", fold_rows(cot))
            add_small("pb", fold_rows(total))
            add_small("g2", fold_rows(grad * normal))
            add_small("s2", fold_rows(grad))

        @pl.when(g == groups - 1)
        def _():
            unit_stage(0, 1)

        mixed_load(g).wait()
        dwproj_ref[...] += dot_tn(mixed_ref[...].reshape(rows, width), sa_ref[...])

    store(y_ref, y_hbm, groups - 1, y_sem).wait()
    unit_stage(1, 1)
    unit_stage(2, 0)
    normal_w_load(0, 0).start()

    plan = {0: ((2, 1),), 5: ((0, 2),), 6: ((1, 2),), 7: ((2, 2),), 8: ((0, 3),), 9: ((1, 3),), 10: ((2, 3),), 11: ((0, 4),)}

    def progress(g2, half):
        for point, calls in plan.items():
            if point % 2 == half:

                @pl.when(g2 == point // 2)
                def _():
                    for u, stage in calls:
                        unit_stage(u, stage)

    subs = 2 * groups

    @pl.loop(0, subs)
    def _(g2):
        s = lax.rem(g2, 2)
        half8 = dx_ref[:, pl.ds(pl.multiple_of(g2 * sub, sub), sub), :]
        half_w = dot_nn(perm_ref[...], half8.reshape(rows8, width).astype(bf16)).astype(bf16)
        mixed_w_ref[...] = dot_nt(half_w, wproj_ref[...]).astype(bf16)
        progress(g2, 0)

        @pl.loop(0, sub // 2)
        def _(wi):
            items = []
            for e in range(2):
                w = wi * 2 + e
                line = pl.ds(pl.multiple_of(w * pad, pad), pad)
                for t in range(quads):
                    cols = [
                        slice(i * width + 128 * t, i * width + 128 * (t + 1)) for i in range(3)
                    ]
                    items.append((w, line, t, cols))
            for first in range(0, len(items), 8):
                batch = items[first : first + 8]
                queries = [stacked(qkv_ref[g2, line, c[0]]) for w, line, t, c in batch]
                scores = [
                    dot_nt(qkv_ref[g2, line, c[1]], x)[0:key_rows] + bias_ref[t]
                    for x, (w, line, t, c) in zip(queries, batch)
                ]
                grads = [stacked(mixed_w_ref[line, c[0]]) for w, line, t, c in batch]
                prob_grads = [
                    dot_nt(qkv_ref[g2, line, c[2]], x)[0:key_rows]
                    for x, (w, line, t, c) in zip(grads, batch)
                ]
                probs = [
                    jnp.exp(x - lse_ref[g2, w, t : t + 1, :])
                    for x, (w, line, t, c) in zip(scores, batch)
                ]
                prob_halves = [grow(x).astype(bf16) for x in probs]
                value_grads = [dot_nn(x, y) for x, y in zip(prob_halves, grads)]
                deltas = [
                    jnp.sum(x * y, axis=0, keepdims=True) for x, y in zip(probs, prob_grads)
                ]
                score_grads = [
                    x * (y - delta) for x, y, delta in zip(probs, prob_grads, deltas)
                ]
                for x, (w, line, t, c) in zip(score_grads, batch):
                    dbias_ref[t] += x
                halves_ = [grow(x).astype(bf16) for x in score_grads]
                key_grads = [dot_nn(x, y) for x, y in zip(halves_, queries)]
                query_grads = [
                    dot_tn(x, qkv_ref[g2, line, c[1]])
                    for x, (w, line, t, c) in zip(halves_, batch)
                ]
                for k, (w, line, t, c) in enumerate(batch):
                    qkv_ref[g2, line, c[0]] = (diagonal(query_grads[k]) * scale).astype(bf16)
                    qkv_ref[g2, line, c[1]] = key_grads[k].astype(bf16)
                    qkv_ref[g2, line, c[2]] = value_grads[k].astype(bf16)

        progress(g2, 1)
        normal_w_load(g2, s).wait()

        @pl.when(g2 < subs - 1)
        def _():
            normal_w_load(g2 + 1, 1 - s).start()

        sat_ref[0:width, 0:rows_w] = act_w_ref[s].T
        for n in range(3):
            cols = slice(n * width, (n + 1) * width)
            part = dot_nn(sat_ref[:, 0:rows_w], qkv_ref[g2, :, cols])
            dwqkv_ref[:, cols] += part[0:width]
            add_small(("qb", "s1", "vb")[n], part[width : width + 8])

            @pl.when(g2 == subs - 1)
            def _():
                unit_stage(3 + n, 0)
                if n == 2:
                    unit_stage(3, 1)

    for t in range(quads):
        for h in range(quad // 2):
            both = dbias_ref[t, :, 128 * h : 128 * (h + 1)]
            plane(t * quad + 2 * h)[...] = jnp.where(low_lanes, both, 0.0)
            plane(t * quad + 2 * h + 1)[...] = jnp.where(
                low_lanes, pltpu.roll(both, pad, 1), 0.0
            )
    total_ref[...] = jnp.zeros(total_ref.shape, f32)

    @pl.loop(0, tokens)
    def _(j):
        hit = named(j)
        line = plane_ref[pl.ds(j, heads, stride=key_rows), :]
        upper_half = line.astype(bf16)
        lower_half = (line - upper_half.astype(f32)).astype(bf16)
        found = dot_nt(upper_half, hit) + dot_nt(lower_half, hit)
        for side in range(2):
            lanes = slice(side * table_lanes, (side + 1) * table_lanes)
            total_ref[0:table_tall, lanes] = (
                total_ref[0:table_tall, lanes] + found[side * table_tall : (side + 1) * table_tall]
            )

    for u in range(4, 6):
        unit_stage(u, 1)
    weighted = jnp.zeros((width, 128), f32)
    for n in range(3 * width // 128):
        lanes = slice(n * 128, (n + 1) * 128)
        weighted = weighted + dwqkv_ref[:, lanes] * wqkv_ref[:, lanes].astype(f32)
    add_small("g1", fold_rows(weighted.T))
    merged_sums = jnp.concatenate(
        [small_ref[:, base[n][0] : base[n][0] + width] for n in ("qb", "s1", "vb")], axis=1
    )
    sums_high = merged_sums.astype(bf16)
    sums_low = (merged_sums - sums_high.astype(f32)).astype(bf16)
    small_ref[:, base["s1"][0] : base["s1"][0] + width] = dot_nt(
        sums_high, wqkv_ref[...]
    ) + dot_nt(sums_low, wqkv_ref[...])

    def put_sums(first, last):
        for i in range(first, last):
            total_ref[table_tall + i : table_tall + i + 1, :] = jnp.sum(
                small_ref[:, i * width : (i + 1) * width], axis=0, keepdims=True
            )

    put_sums(0, small_ref.shape[1] // width)
    total_start(0)
    plan2 = {0: ((1, 4),), 1: ((3, 2), (2, 4), (-1, 0)), 2: ((0, 5), (4, 2)), 3: ((5, 2),), 4: ((1, 5), (-1, 1)), 5: ((3, 3),)}

    @pl.loop(0, groups)
    def _(g):
        win0 = pl.multiple_of(g * group, group)
        slot = lax.rem(3 * groups + g, 2)
        load(x_hbm, g, slot).wait()

        @pl.when(g < groups - 1)
        def _():
            load(x_hbm, g + 1, 1 - slot).start()

        for s in range(2):
            g2 = g * 2 + s
            mixed_w_ref[...] = dot_nt(qkv_ref[g2], wqkv_ref[...]).astype(bf16)
            wide_ref[:, sub * s : sub * (s + 1), :] = dot_nn(back_ref[...], mixed_w_ref[...]).reshape(
                tokens, sub, width
            )
            for point, calls in plan2.items():
                if point % 2 == s:

                    @pl.when(g == point // 2)
                    def _():
                        for u, stage in calls:
                            if u < 0:
                                total_finish(stage)
                            else:
                                unit_stage(u, stage)

        @pl.loop(0, tokens // step)
        def _(n):
            part = in_ref[slot, pl.ds(n * step, step)].astype(f32)
            normal, inverse = norm_parts(part.reshape(step * group, width))
            grad = wide_ref[pl.ds(n * step, step)].reshape(step * group, width)
            scaled = grad * gain1_ref[...]
            back = inverse * (
                scaled
                - jnp.mean(scaled, axis=-1, keepdims=True)
                - normal * jnp.mean(scaled * normal, axis=-1, keepdims=True)
            )
            dx_ref[pl.ds(n * step, step), pl.ds(win0, group), :] += back.reshape(step, group, width)

        @pl.when(g != 0)
        def _():
            store(y_ref, dx_hbm, g - 1, dx_sem).wait()

        y_ref[...] = dx_ref[:, pl.ds(win0, group), :].astype(bf16)
        store(y_ref, dx_hbm, g, dx_sem).start()

    done = {0: 5, 1: 5, 2: 4, 3: 3, 4: 2, 5: 2}
    for stage in range(2, stages):
        for u in (3, 4, 5, 2, 0, 1):
            if stage > done[u]:
                unit_stage(u, stage)
    for step_at in range(2, total_steps):
        total_finish(step_at)
    store(y_ref, dx_hbm, groups - 1, dx_sem).wait()


def local_pass(x, dy, wqkv, wproj, w1, w2, vectors, table, index, shards, reps):
    tokens, windows, width = x.shape
    hidden = w1.shape[1]
    heads = table.shape[0]
    dims = (tokens, windows, width, heads, hidden, shards, reps)
    chips = shards // 2
    bits = reps.bit_length() - 1
    sub = 8
    group = 2 * sub
    pad = 64
    rows = tokens * group
    small_size = 8 * width + hidden
    subs = windows // sub
    owned = width // shards
    unit_rows = (hidden // shards, hidden // shards, owned, owned, owned, owned)
    near_size = 1 << min(bits, 3)
    slots = near_size - 1 + bits - min(bits, 3)
    total_rows = -(-(heads // 2 + small_size // width) // (8 * shards)) * 8 * shards
    shapes = (
        [
            jax.ShapeDtypeStruct(x.shape, bf16),
            jax.ShapeDtypeStruct(x.shape, bf16),
            jax.ShapeDtypeStruct(x.shape, bf16),
            jax.ShapeDtypeStruct((subs, sub * pad, width), bf16),
            jax.ShapeDtypeStruct((subs, sub * pad, width), bf16),
        ]
        + [jax.ShapeDtypeStruct((r, width), bf16) for r in unit_rows]
        + [jax.ShapeDtypeStruct((total_rows, width), f32)]
    )
    vmem = pl.BlockSpec(memory_space=pltpu.VMEM)
    hbm = pl.BlockSpec(memory_space=pl.ANY)

    return pl.pallas_call(
        functools.partial(compute_kernel, dims),
        out_shape=shapes,
        in_specs=[hbm] * 6 + [vmem] * 11,
        out_specs=[hbm] * 5 + [vmem] * 7,
        scratch_shapes=[
            pltpu.VMEM((2, tokens, group, width), bf16),
            pltpu.VMEM((tokens, group, width), bf16),
            pltpu.VMEM(x.shape, f32),
            pltpu.VMEM((width, 3 * width), f32),
            pltpu.VMEM((width, width), f32),
            pltpu.VMEM((width, hidden), f32),
            pltpu.VMEM((width, hidden), f32),
            pltpu.VMEM((8, small_size), f32),
            pltpu.VMEM((heads // 4, 56, 256), f32),
            pltpu.VMEM((heads // 4, 56, 256), f32),
            pltpu.VMEM((sub * pad, tokens * sub), bf16),
            pltpu.VMEM((tokens * sub, sub * pad), bf16),
            pltpu.VMEM((2, sub * pad, width), bf16),
            pltpu.VMEM((2, width, 128), f32),
            pltpu.VMEM((subs, sub * pad, 3 * width), bf16),
            pltpu.VMEM((sub * pad, width), bf16),
            pltpu.VMEM((tokens, group, width), bf16),
            pltpu.VMEM((subs, sub, heads // 4, 256), f32),
            pltpu.VMEM((tokens, group, width), f32),
            pltpu.VMEM((rows, width), bf16),
            pltpu.VMEM((width + 16, rows), bf16),
            pltpu.VMEM((width, rows), bf16),
            pltpu.VMEM((rows, width), f32),
            pltpu.VMEM((rows, width), f32),
            pltpu.VMEM((heads * 56, 128), f32),
            pltpu.VMEM((128, 128), f32),
            pltpu.VMEM((heads, -(-table.shape[1] // 128) * 128), f32),
            pltpu.VMEM((rows, hidden), bf16),
            pltpu.VMEM((rows, hidden), bf16),
            pltpu.VMEM((width, 3 * width), bf16),
            pltpu.VMEM((width, width), bf16),
            pltpu.VMEM((width, hidden), bf16),
            pltpu.VMEM((hidden, width), bf16),
            pltpu.VMEM((chips - 1, unit_rows[0], width), bf16),
            *[pltpu.VMEM((chips, r, width), bf16) for r in unit_rows],
            *[pltpu.VMEM((chips - 1, r, width), bf16) for r in unit_rows],
            *[pltpu.VMEM((slots * r // near_size, width), bf16) for r in unit_rows],
            pltpu.VMEM((2 * shards - 2 + slots, total_rows // shards, width), f32),
            pltpu.SemaphoreType.DMA((5,)),
            pltpu.SemaphoreType.DMA((5, chips)),
            pltpu.SemaphoreType.DMA((5, chips)),
            pltpu.SemaphoreType.DMA((5, chips - 1)),
            pltpu.SemaphoreType.DMA((5, chips - 1)),
            pltpu.SemaphoreType.DMA((2,)),
            pltpu.SemaphoreType.DMA,
            pltpu.SemaphoreType.DMA,
            pltpu.SemaphoreType.DMA((2,)),
            pltpu.SemaphoreType.DMA((2,)),
            pltpu.SemaphoreType.DMA,
            pltpu.SemaphoreType.DMA((6, chips)),
            pltpu.SemaphoreType.DMA((6, chips)),
            pltpu.SemaphoreType.DMA((6, chips - 1)),
            pltpu.SemaphoreType.DMA((6, chips - 1)),
            pltpu.SemaphoreType.DMA((6, slots)),
            pltpu.SemaphoreType.DMA((6, slots)),
            pltpu.SemaphoreType.DMA((6, slots)),
            pltpu.SemaphoreType.DMA((6, slots)),
            pltpu.SemaphoreType.DMA((2 * shards - 2 + slots,)),
            pltpu.SemaphoreType.DMA((2 * shards - 2 + slots,)),
        ],
        compiler_params=pltpu.CompilerParams(
            vmem_limit_bytes=67043328, collective_id=0, has_side_effects=True
        ),
    )(x, dy, wqkv, wproj, w1, w2, *vectors, table, index)


def spread_kernel(heads, sizes, *refs):
    works = refs[:6]
    total_ref, y_in, dx_in = refs[6:9]
    dwqkv_ref, dwproj_ref, dw1_ref, dw2_ref, table_ref = refs[9:14]
    sums = refs[14:-2]
    y_ref, dx_ref = refs[-2:]
    width = dwproj_ref.shape[1]
    owned = dwproj_ref.shape[0]
    y_ref[...] = y_in[...]
    dx_ref[...] = dx_in[...].astype(f32)

    @pl.when(pl.program_id(0) == 0)
    def _():
        for i in range(dw1_ref.shape[1] // width):
            dw1_ref[:, i * width : (i + 1) * width] = works[0][
                i * owned : (i + 1) * owned, :
            ].astype(f32)
        dw2_ref[...] = works[1][...].astype(f32)
        dwproj_ref[...] = works[2][...].astype(f32)
        for i in range(3):
            dwqkv_ref[:, i * width : (i + 1) * width] = works[3 + i][...].astype(f32)
        tall = heads // 2
        rows_t = table_ref.shape[1]
        lanes = total_ref.shape[1] // 2
        table_ref[0:tall, :] = total_ref[0:tall, 0:rows_t]
        table_ref[tall:heads, :] = total_ref[0:tall, lanes : lanes + rows_t]
        row = tall
        for ref, size in zip(sums, sizes):
            for i in range(size // width):
                ref[:, i * width : (i + 1) * width] = total_ref[row : row + 1, :]
                row += 1


def spread(works, total, y, dx, hidden, heads, table_rows):
    tokens, windows, width = y.shape
    owned = works[2].shape[0]
    sizes = (width, width, width, hidden, width, width, width, width, width)
    shapes = [
        (owned, 3 * width),
        (owned, width),
        (owned, hidden),
        works[1].shape,
        (heads, table_rows),
    ] + [(1, size) for size in sizes]
    step = tokens
    slab = pl.BlockSpec((step, windows, width), lambda i: (i, 0, 0))
    whole = lambda shape: pl.BlockSpec(shape, lambda i: (0, 0))
    return pl.pallas_call(
        functools.partial(spread_kernel, heads, sizes),
        grid=(tokens // step,),
        out_shape=[jax.ShapeDtypeStruct(shape, f32) for shape in shapes]
        + [jax.ShapeDtypeStruct(y.shape, bf16), jax.ShapeDtypeStruct(y.shape, f32)],
        in_specs=[whole(w.shape) for w in works] + [whole(total.shape), slab, slab],
        out_specs=[whole(shape) for shape in shapes] + [slab, slab],
    )(*works, total, y, dx)


def on_device(
    shards,
    reps,
    block_input,
    out_grad,
    qkv_weight,
    query_bias,
    value_bias,
    proj_weight,
    proj_bias,
    hidden_weight,
    hidden_bias,
    output_weight,
    output_bias,
    first_gain,
    first_shift,
    second_gain,
    second_shift,
    bias_table,
    table_index,
):
    windows, tokens, width = block_input.shape
    table_rows, heads = bias_table.shape
    hidden = hidden_bias.shape[0]
    vectors = [
        v.reshape(1, -1)
        for v in (
            query_bias,
            value_bias,
            proj_bias,
            hidden_bias,
            output_bias,
            first_gain,
            first_shift,
            second_gain,
            second_shift,
        )
    ]
    y, dx, _, _, _, *works, total = local_pass(
        jnp.transpose(block_input, (1, 0, 2)),
        jnp.transpose(out_grad, (1, 0, 2)),
        qkv_weight,
        proj_weight,
        hidden_weight,
        output_weight,
        vectors,
        bias_table.T,
        table_index,
        shards,
        reps,
    )
    (dwqkv, dwproj, dw1, dw2, table_grad, qb, vb, pb, hb, ob, g1, s1, g2, s2, y, dx) = spread(
        works, total, y, dx, hidden, heads, table_rows
    )
    return (
        jnp.transpose(y, (1, 0, 2)),
        jnp.transpose(dx, (1, 0, 2)),
        dwqkv,
        qb.reshape(-1),
        vb.reshape(-1),
        dwproj,
        pb.reshape(-1),
        dw1,
        hb.reshape(-1),
        dw2,
        ob.reshape(-1),
        g1.reshape(-1),
        s1.reshape(-1),
        g2.reshape(-1),
        s2.reshape(-1),
        table_grad.T,
    )


def solution(mesh):
    rows = P(("shard", "rep"), None, None)
    cut = P("shard", None)
    full = P()
    return jax.shard_map(
        functools.partial(on_device, mesh.shape["shard"], mesh.shape["rep"]),
        mesh=mesh,
        in_specs=(
            rows,
            rows,
            cut,
            full,
            full,
            cut,
            full,
            cut,
            full,
            cut,
            full,
            full,
            full,
            full,
            full,
            full,
            full,
        ),
        out_specs=(
            rows,
            rows,
            cut,
            full,
            full,
            cut,
            full,
            cut,
            full,
            cut,
            full,
            full,
            full,
            full,
            full,
            full,
        ),
        check_vma=False,
    )
```

```python
import functools

import jax
import jax.numpy as jnp
from jax import lax
from jax.experimental import pallas as pl
from jax.experimental.pallas import tpu as pltpu
from jax.sharding import PartitionSpec as P

epsilon = 1e-05
f32 = jnp.float32
bf16 = jnp.bfloat16


def dot_nn(a, b):
    return lax.dot_general(a, b, (((1,), (0,)), ((), ())), preferred_element_type=f32)


def dot_nt(a, b):
    return lax.dot_general(a, b, (((1,), (1,)), ((), ())), preferred_element_type=f32)


def dot_tn(a, b):
    return lax.dot_general(a, b, (((0,), (0,)), ((), ())), preferred_element_type=f32)


def norm_parts(values):
    center = values - jnp.mean(values, axis=-1, keepdims=True)
    inverse = lax.rsqrt(jnp.mean(center * center, axis=-1, keepdims=True) + epsilon)
    return center * inverse, inverse


def fold_rows(values):
    rows, cols = values.shape
    return jnp.sum(values.reshape(rows // 8, 8, cols), axis=0)


def gelu_pair(upper):
    phi = 0.5 + 0.5 * lax.erf(upper * 0.7071067811865476)
    bell = jnp.exp(upper * upper * -0.5) * 0.3989422804014327
    return upper * phi, phi + upper * bell


def compute_kernel(
    dims,
    x_hbm,
    dy_hbm,
    wqkv_shard,
    wproj_shard,
    w1_shard,
    w2_shard,
    query_bias_ref,
    value_bias_ref,
    proj_bias_ref,
    hidden_bias_ref,
    output_bias_ref,
    gain1_ref,
    shift1_ref,
    gain2_ref,
    shift2_ref,
    table_ref,
    index_ref,
    y_hbm,
    dx_hbm,
    mixed_hbm,
    act_w_hbm,
    normal_w_hbm,
    work0_ref,
    work1_ref,
    work2_ref,
    work3_ref,
    work4_ref,
    work5_ref,
    total_ref,
    in_ref,
    y_ref,
    dx_ref,
    dwqkv_ref,
    dwproj_ref,
    dw1_ref,
    dw2t_ref,
    small_ref,
    dbias_ref,
    bias_ref,
    perm_ref,
    back_ref,
    act_w_ref,
    column_ref,
    qkv_ref,
    mixed_w_ref,
    mixed_ref,
    lse_ref,
    wide_ref,
    sa_ref,
    sat_ref,
    dyt_ref,
    u_ref,
    da_ref,
    plane_ref,
    names_ref,
    rows_ref,
    act_ref,
    dup_ref,
    wqkv_ref,
    wproj_ref,
    w1_ref,
    w2_ref,
    out0_ref,
    in0_ref,
    in1_ref,
    in2_ref,
    in3_ref,
    in4_ref,
    in5_ref,
    far0_ref,
    far1_ref,
    far2_ref,
    far3_ref,
    far4_ref,
    far5_ref,
    half0_ref,
    half1_ref,
    half2_ref,
    half3_ref,
    half4_ref,
    half5_ref,
    total_in_ref,
    own_sem,
    pair_send,
    pair_recv,
    chip_send,
    chip_recv,
    load_sem,
    y_sem,
    mixed_sem,
    act_w_sem,
    normal_w_sem,
    dx_sem,
    core_send,
    core_recv,
    far_send,
    far_recv,
    half_send,
    half_recv,
    join_send,
    join_recv,
    total_send,
    total_recv,
):
    tokens, windows, width, heads, hidden, shards, reps = dims
    me = lax.axis_index("shard")
    chips = shards // 2
    core = lax.rem(me, 2)
    chip = me // 2
    pair = chip * 2 + 1 - core

    def peer(k):
        return lax.rem(chip + k, chips) * 2 + core

    def owner(k, side):
        return lax.rem(chip + chips - k, chips) * 2 + side

    gathers = (
        (wqkv_shard, wqkv_ref, slice(0, wqkv_ref.shape[1] // 2)),
        (wqkv_shard, wqkv_ref, slice(wqkv_ref.shape[1] // 2, wqkv_ref.shape[1])),
        (wproj_shard, wproj_ref, slice(0, wproj_ref.shape[1])),
        (w1_shard, w1_ref, slice(0, w1_ref.shape[1])),
        (w2_shard, w2_ref, slice(0, w2_ref.shape[1])),
    )

    def block(ref, index, cols):
        size = ref.shape[0] // shards
        return ref.at[pl.ds(pl.multiple_of(index * size, size), size), cols]

    def own_copy(i):
        shard, full, cols = gathers[i]
        return pltpu.make_async_copy(shard.at[:, cols], block(full, me, cols), own_sem.at[i])

    def chip_copy(i, k):
        shard, full, cols = gathers[i]
        return pltpu.make_async_remote_copy(
            src_ref=shard.at[:, cols],
            dst_ref=block(full, me, cols),
            send_sem=chip_send.at[i, k - 1],
            recv_sem=chip_recv.at[i, k - 1],
            device_id={"shard": peer(k)},
            device_id_type=pl.DeviceIdType.MESH,
        )

    def pair_copy(i, k):
        shard, full, cols = gathers[i]
        return pltpu.make_async_remote_copy(
            src_ref=shard.at[:, cols] if k == 0 else block(full, owner(k, core), cols),
            dst_ref=block(full, owner(k, core), cols),
            send_sem=pair_send.at[i, k],
            recv_sem=pair_recv.at[i, k],
            device_id={"shard": pair},
            device_id_type=pl.DeviceIdType.MESH,
        )

    def gather_start(i):
        own_copy(i).start()
        for k in range(1, chips):
            chip_copy(i, k).start()
        pair_copy(i, 0).start()

    def gather_relay(i):
        for k in range(1, chips):
            chip_copy(i, k).wait_recv()
            pair_copy(i, k).start()

    def gather_finish(i):
        own_copy(i).wait()
        for k in range(chips):
            pair_copy(i, k).wait_recv()

    def gather_drain(i):
        for k in range(1, chips):
            chip_copy(i, k).wait_send()
        for k in range(chips):
            pair_copy(i, k).wait_send()

    rep = lax.axis_index("rep")
    bits = reps.bit_length() - 1

    near = min(bits, 3)
    near_size = 1 << near
    far_bits = list(range(near, bits))

    def flipped(index, distance, span):
        for b in range(span):
            if distance >> b & 1:
                index = index + (1 - 2 * lax.rem(index // (1 << b), 2)) * (1 << b)
        return index

    shard_span = shards.bit_length() - 1
    barrier = pltpu.get_barrier_semaphore()
    greeted = [{"shard": flipped(me, d, shard_span)} for d in range(1, shards)]
    greeted += [{"rep": flipped(rep, d, near)} for d in range(1, near_size)]
    greeted += [{"rep": flipped(rep, 1 << b, bits)} for b in far_bits]
    for target in greeted:
        pl.semaphore_signal(
            barrier, inc=1, device_id=target, device_id_type=pl.DeviceIdType.MESH
        )
    pl.semaphore_wait(barrier, len(greeted))
    gather_start(0)
    gather_start(1)

    head_size = width // heads
    scale = head_size ** (-0.5)
    pad = 64
    key_rows = 56
    sub = 8
    group = 2 * sub
    groups = windows // group
    quad = 128 // head_size
    quads = heads // quad
    rows8 = tokens * sub
    rows = tokens * group
    rows_w = sub * pad
    chunk = width
    step = 7
    lane_head = lax.broadcasted_iota(jnp.int32, (pad, 128), 1) // head_size
    head_masks = [lane_head == h for h in range(quad)]
    head_masks_half = [m.astype(f32).astype(bf16) for m in head_masks]

    base = {}
    at = 0
    for name, size in (
        ("qb", width),
        ("vb", width),
        ("pb", width),
        ("hb", hidden),
        ("ob", width),
        ("g1", width),
        ("s1", width),
        ("g2", width),
        ("s2", width),
    ):
        base[name] = (at, size)
        at += size

    def add_small(name, value, offset=0):
        start = base[name][0] + offset
        cols = pl.ds(start, value.shape[1])
        small_ref[:, cols] = small_ref[:, cols] + value

    def load(source, g, slot):
        return pltpu.make_async_copy(
            source.at[:, pl.ds(pl.multiple_of(g * group, group), group), :],
            in_ref.at[slot],
            load_sem.at[slot],
        )

    def store(source, target, g, sem):
        return pltpu.make_async_copy(
            source, target.at[:, pl.ds(pl.multiple_of(g * group, group), group), :], sem
        )

    def mixed_load(g):
        return pltpu.make_async_copy(
            mixed_hbm.at[:, pl.ds(pl.multiple_of(g * group, group), group), :], mixed_ref, mixed_sem
        )

    def act_w_store(g2, slot):
        return pltpu.make_async_copy(act_w_ref.at[slot], act_w_hbm.at[g2], act_w_sem.at[slot])

    def act_w_load(g2, slot):
        return pltpu.make_async_copy(act_w_hbm.at[g2], act_w_ref.at[slot], act_w_sem.at[slot])

    def normal_stage(slot):
        return mixed_w_ref if slot == 0 else out0_ref.at[0]

    def normal_w_store(g2, slot):
        return pltpu.make_async_copy(
            normal_stage(slot), normal_w_hbm.at[g2], normal_w_sem.at[slot]
        )

    def normal_w_load(g2, slot):
        return pltpu.make_async_copy(
            normal_w_hbm.at[g2], act_w_ref.at[slot], normal_w_sem.at[slot]
        )

    load(x_hbm, 0, 0).start()

    owned = width // shards
    works = (work0_ref, work1_ref, work2_ref, work3_ref, work4_ref, work5_ref)
    ins = (in0_ref, in1_ref, in2_ref, in3_ref, in4_ref, in5_ref)
    fars = (far0_ref, far1_ref, far2_ref, far3_ref, far4_ref, far5_ref)
    halves = (half0_ref, half1_ref, half2_ref, half3_ref, half4_ref, half5_ref)

    def unit_pieces(u, s):
        own = pl.ds(pl.multiple_of(s * owned, owned), owned)
        if u == 0:
            for i in range(hidden // width):
                cols = slice(width * i, width * (i + 1))
                yield owned * i, owned, (lambda cols=cols: dw1_ref[own, cols])
        elif u == 1:
            size = hidden // shards
            for i in range(size // 256):
                lanes = pl.ds(pl.multiple_of(s * size + i * 256, 256), 256)
                yield i * 256, 256, (lambda lanes=lanes: dw2t_ref[:, lanes].T)
        elif u == 2:
            yield 0, owned, (lambda: dwproj_ref[own, :])
        else:
            cols = slice(width * (u - 3), width * (u - 2))
            name = ("qb", "s1", "vb")[u - 3]
            sums = small_ref[0:1, base[name][0] : base[name][0] + width]
            yield 0, owned, (
                lambda: dwqkv_ref[own, cols] * column_ref[0, own, 0:1]
                + column_ref[1, own, 0:1] * sums
            )

    def unit_out(u, j):
        rows_u = works[u].shape[0]
        if u == 0:
            return mixed_w_ref.at[0:rows_u] if j == 0 else out0_ref.at[j - 1]
        if u == 1:
            return act_ref.at[0:rows_u, j * width : (j + 1) * width]
        first = (u - 2) * owned
        return act_ref.at[
            first : first + owned, (chips + j) * width : (chips + j + 1) * width
        ]

    def core_copy(u, j):
        return pltpu.make_async_remote_copy(
            src_ref=unit_out(u, j),
            dst_ref=ins[u].at[j],
            send_sem=core_send.at[u, j],
            recv_sem=core_recv.at[u, j],
            device_id={"shard": pair},
            device_id_type=pl.DeviceIdType.MESH,
        )

    def levels(u):
        if u < 2 and near == 3:
            return [(0, 1), (1, 2)]
        return [(0, near)]

    def level_index(u, at_level):
        low, count = levels(u)[at_level]
        return lax.rem(rep // (1 << low), 1 << count)

    def held(u, at_level):
        size = works[u].shape[0]
        start = 0
        for k in range(at_level):
            size >>= levels(u)[k][1]
            start = start + level_index(u, k) * size
        return start, size

    def lines_of(start, size):
        return pl.ds(start if isinstance(start, int) else pl.multiple_of(start, 16), size)

    def own_piece(u):
        return lines_of(*held(u, len(levels(u))))

    def peers_of(u, at_level):
        slot = 0
        row = 0
        for k in range(at_level):
            others = (1 << levels(u)[k][1]) - 1
            slot += others
            row += others * held(u, k + 1)[1]
        low, count = levels(u)[at_level]
        size = held(u, at_level + 1)[1]
        return [
            (d, slot + d - 1, row + (d - 1) * size, {"rep": flipped(rep, d << low, bits)})
            for d in range(1, 1 << count)
        ]

    def far_copy(u, k):
        return pltpu.make_async_remote_copy(
            src_ref=ins[u].at[lax.rem(chip + k, chips)],
            dst_ref=fars[u].at[k - 1],
            send_sem=far_send.at[u, k - 1],
            recv_sem=far_recv.at[u, k - 1],
            device_id={"shard": peer(k)},
            device_id_type=pl.DeviceIdType.MESH,
        )

    def spread_copy(u, at_level, link):
        d, slot, row, partner = link
        start, _ = held(u, at_level)
        size = held(u, at_level + 1)[1]
        index = flipped(level_index(u, at_level), d, levels(u)[at_level][1])
        return pltpu.make_async_remote_copy(
            src_ref=ins[u].at[chip, lines_of(start + index * size, size), :],
            dst_ref=halves[u].at[pl.ds(row, size), :],
            send_sem=half_send.at[u, slot],
            recv_sem=half_recv.at[u, slot],
            device_id=partner,
            device_id_type=pl.DeviceIdType.MESH,
        )

    def double_copy(u, b):
        slot = near_size - 1 + b - near
        size = works[u].shape[0] // near_size
        return pltpu.make_async_remote_copy(
            src_ref=ins[u].at[chip, own_piece(u), :],
            dst_ref=halves[u].at[pl.ds(slot * size, size), :],
            send_sem=half_send.at[u, slot],
            recv_sem=half_recv.at[u, slot],
            device_id={"rep": flipped(rep, 1 << b, bits)},
            device_id_type=pl.DeviceIdType.MESH,
        )

    def join_copy(u, at_level, link):
        d, slot, row, partner = link
        lines = lines_of(*held(u, at_level + 1))
        return pltpu.make_async_remote_copy(
            src_ref=works[u].at[lines, :],
            dst_ref=works[u].at[lines, :],
            send_sem=join_send.at[u, slot],
            recv_sem=join_recv.at[u, slot],
            device_id=partner,
            device_id_type=pl.DeviceIdType.MESH,
        )

    def level_start(u, at_level):
        for link in peers_of(u, at_level):
            spread_copy(u, at_level, link).start()

    def join_start(u, at_level):
        for link in peers_of(u, at_level):
            join_copy(u, at_level, link).start()

    def unit_stage(u, stage):
        if stage == 0:
            for j in range(chips):
                target = unit_out(u, j)
                for r0, nr, value in unit_pieces(u, 2 * j + 1 - core):
                    target[r0 : r0 + nr, :] = value().astype(bf16)
                core_copy(u, j).start()
            return
        if stage == 1:
            for j in range(chips):
                core_copy(u, j).wait()
            for k in range(1, chips + 1):
                j = lax.rem(chip + k, chips)
                for r0, nr, value in unit_pieces(u, 2 * j + core):
                    got = ins[u][j, r0 : r0 + nr, :].astype(f32)
                    ins[u][j, r0 : r0 + nr, :] = (value() + got).astype(bf16)
                if k == chips - 1:
                    for n in range(1, chips):
                        far_copy(u, n).start()
            return
        if stage == 2:
            for k in range(1, chips):
                far_copy(u, k).wait()
            total = ins[u][chip].astype(f32)
            for k in range(1, chips):
                total = total + fars[u][k - 1].astype(f32)
            ins[u][chip] = total.astype(bf16)
            level_start(u, 0)
            return
        count = len(levels(u))
        at_level = stage - 3
        if at_level < count:
            lines = lines_of(*held(u, at_level + 1))
            size = held(u, at_level + 1)[1]
            total = ins[u][chip, lines, :].astype(f32)
            for link in peers_of(u, at_level):
                spread_copy(u, at_level, link).wait()
                total = total + halves[u][link[2] : link[2] + size, :].astype(f32)
            if at_level + 1 < count:
                ins[u][chip, lines, :] = total.astype(bf16)
                level_start(u, at_level + 1)
            elif far_bits:
                ins[u][chip, lines, :] = total.astype(bf16)
                double_copy(u, far_bits[0]).start()
            else:
                works[u][lines, :] = total.astype(bf16)
                join_start(u, count - 1)
            return
        at_double = at_level - count
        if at_double < len(far_bits):
            b = far_bits[at_double]
            double_copy(u, b).wait()
            size = works[u].shape[0] // near_size
            row = (near_size - 1 + b - near) * size
            total = ins[u][chip, own_piece(u), :].astype(f32) + halves[u][
                row : row + size, :
            ].astype(f32)
            if b != far_bits[-1]:
                ins[u][chip, own_piece(u), :] = total.astype(bf16)
                double_copy(u, b + 1).start()
            else:
                works[u][own_piece(u), :] = total.astype(bf16)
                join_start(u, count - 1)
            return
        at_join = count - 1 - (at_double - len(far_bits))
        if at_join >= 0:
            for link in peers_of(u, at_join):
                join_copy(u, at_join, link).wait()
            if at_join > 0:
                join_start(u, at_join - 1)

    stages = 7 + len(far_bits)

    total_steps = 3 + len(far_bits)
    share = total_ref.shape[0] // shards

    def total_share(index):
        return total_ref.at[pl.ds(pl.multiple_of(index * share, share), share), :]

    def total_copies(step):
        if step == 0 or step == total_steps - 1:
            first = 0 if step == 0 else shards - 2 + near_size + len(far_bits)
            links = [
                (first + d - 1, flipped(me, d, shard_span), {"shard": flipped(me, d, shard_span)})
                for d in range(1, shards)
            ]
        elif step == 1:
            links = [
                (shards + d - 2, me, {"rep": flipped(rep, d, near)}) for d in range(1, near_size)
            ]
        else:
            b = far_bits[step - 2]
            links = [(shards + near_size + step - 4, me, {"rep": flipped(rep, 1 << b, bits)})]
        return [
            (
                at_slot,
                other,
                pltpu.make_async_remote_copy(
                    src_ref=total_share(other if step == 0 else me),
                    dst_ref=total_in_ref.at[at_slot],
                    send_sem=total_send.at[at_slot],
                    recv_sem=total_recv.at[at_slot],
                    device_id=target,
                    device_id_type=pl.DeviceIdType.MESH,
                ),
            )
            for at_slot, other, target in links
        ]

    def total_start(step):
        for _, _, copy in total_copies(step):
            copy.start()

    def total_finish(step):
        if step == total_steps - 1:
            for at_slot, other, copy in total_copies(step):
                copy.wait()
                total_share(other)[...] = total_in_ref[at_slot]
            return
        values = [total_share(me)[...]]
        for at_slot, _, copy in total_copies(step):
            copy.wait()
            values.append(total_in_ref[at_slot])
        while len(values) > 1:
            values = [values[i] + values[i + 1] for i in range(0, len(values), 2)]
        total_share(me)[...] = values[0]
        total_start(step + 1)

    small_ref[...] = jnp.zeros(small_ref.shape, f32)
    dbias_ref[...] = jnp.zeros(dbias_ref.shape, f32)
    for i, ref in enumerate((gain1_ref, shift1_ref)):
        column_ref[i] = jnp.broadcast_to(ref[...], (128, width)).T
    sat_ref[width:, :] = (
        lax.broadcasted_iota(jnp.int32, (16, rows), 0) == 0
    ).astype(f32).astype(bf16)

    @pl.loop(0, width // 32)
    def _(n):
        lines = pl.ds(pl.multiple_of(n * 32, 32), 32)
        dwqkv_ref[lines, :] = jnp.zeros((32, 3 * width), f32)
        dwproj_ref[lines, :] = jnp.zeros((32, width), f32)
        dw1_ref[lines, :] = jnp.zeros((32, hidden), f32)
        dw2t_ref[lines, :] = jnp.zeros((32, hidden), f32)

    @pl.loop(0, rows_w // 64)
    def _(n):
        start = pl.multiple_of(n * 64, 64)
        to = lax.broadcasted_iota(jnp.int32, (64, rows8), 0) + start
        source = lax.broadcasted_iota(jnp.int32, (64, rows8), 1)
        hit = (to // pad == source % sub) & (to % pad == source // sub)
        perm_ref[pl.ds(start, 64), :] = hit.astype(f32).astype(bf16)

    @pl.loop(0, rows8 // 56)
    def _(n):
        start = pl.multiple_of(n * 56, 8)
        to = lax.broadcasted_iota(jnp.int32, (56, rows_w), 0) + start
        source = lax.broadcasted_iota(jnp.int32, (56, rows_w), 1)
        hit = (source // pad == to % sub) & (source % pad == to // sub)
        back_ref[pl.ds(start, 56), :] = hit.astype(f32).astype(bf16)

    table_tall = heads // 2
    table_rows = table_ref.shape[1]
    table_lanes = -(-table_rows // 128) * 128
    row_iota = lax.broadcasted_iota(jnp.int32, (table_lanes, 128), 0).astype(f32)
    low_lanes = lax.broadcasted_iota(jnp.int32, (key_rows, 128), 1) < pad
    rows_ref[...] = jnp.zeros(rows_ref.shape, f32)
    rows_ref[:, 0:table_rows] = table_ref[...]
    names_ref[...] = jnp.full(names_ref.shape, -1.0, f32)
    names_ref[0:tokens, 0:tokens] = index_ref[...].astype(f32)
    names_ref[...] = names_ref[...].T

    def named(j):
        return (row_iota == names_ref[pl.ds(j, 1), :]).astype(f32).astype(bf16)

    table = rows_ref[...]
    high = table.astype(bf16)
    middle = (table - high.astype(f32)).astype(bf16)
    low = (table - high.astype(f32) - middle.astype(f32)).astype(bf16)
    plane_ref[...] = jnp.full(plane_ref.shape, -1e30, f32)

    def plane(h):
        return plane_ref.at[h * key_rows : (h + 1) * key_rows, :]

    @pl.loop(0, tokens)
    def _(j):
        hit = named(j)
        line = (dot_nn(high, hit) + dot_nn(middle, hit)) + dot_nn(low, hit)
        plane_ref[pl.ds(j, heads, stride=key_rows), :] = line

    for t in range(quads):
        for h in range(quad // 2):
            left = plane(t * quad + 2 * h)[...]
            right = plane(t * quad + 2 * h + 1)[...]
            bias_ref[t, :, 128 * h : 128 * (h + 1)] = jnp.where(
                low_lanes, left, pltpu.roll(right, pad, 1)
            )

    def stacked(tile):
        return jnp.concatenate([tile * m for m in head_masks_half], axis=0)

    def diagonal(tall):
        total = tall[0:pad]
        for h in range(1, quad):
            total = jnp.where(head_masks[h], tall[h * pad : (h + 1) * pad], total)
        return total

    def grow(values):
        return jnp.concatenate([values, jnp.zeros((pad - key_rows, values.shape[1]), f32)], axis=0)

    @pl.loop(0, groups)
    def _(g):
        slot = lax.rem(g, 2)
        load(x_hbm, g, slot).wait()
        load(x_hbm, lax.rem(g + 1, groups), 1 - slot).start()

        @pl.when(g == groups - 1)
        def _():
            gather_relay(0)

        @pl.loop(0, tokens // step)
        def _(n):
            part = in_ref[slot, pl.ds(n * step, step)].astype(f32)
            flat = part.reshape(step * group, width)
            normal, _ = norm_parts(flat)
            wide_ref[pl.ds(n * step, step)] = (normal * gain1_ref[...] + shift1_ref[...]).reshape(
                step, group, width
            )
            lines = pl.ds(pl.multiple_of(n * step * group, step * group), step * group)
            u_ref[lines, :] = normal

        for s in range(2):
            act8 = wide_ref[:, sub * s : sub * (s + 1), :].reshape(rows8, width).astype(bf16)

            @pl.when(g != 0)
            def _():
                act_w_store(2 * g - 2 + s, s).wait()
                normal_w_store(2 * g - 2 + s, s).wait()

            act_w_ref[s] = dot_nn(perm_ref[...], act8).astype(bf16)
            act_w_store(2 * g + s, s).start()
            normal8 = u_ref[...].reshape(tokens, group, width)[:, sub * s : sub * (s + 1), :]
            normal_stage(s)[...] = dot_nn(
                perm_ref[...], normal8.reshape(rows8, width).astype(bf16)
            ).astype(bf16)
            normal_w_store(2 * g + s, s).start()

    for s in range(2):
        act_w_store(2 * groups - 2 + s, s).wait()
        normal_w_store(2 * groups - 2 + s, s).wait()
    act_w_load(0, 0).start()
    gather_relay(1)
    for i in range(2, 5):
        gather_start(i)
    for i in range(2):
        gather_finish(i)

    @pl.loop(0, groups)
    def _(g):
        win0 = pl.multiple_of(g * group, group)
        slot = lax.rem(groups + g, 2)
        load(x_hbm, g, slot).wait()

        @pl.when(g < groups - 1)
        def _():
            load(x_hbm, g + 1, 1 - slot).start()

        @pl.when(g == groups - 1)
        def _():
            load(dy_hbm, 0, 1 - slot).start()
            gather_relay(3)

        @pl.loop(0, 2)
        def _(s):
            g2 = g * 2 + s
            act_w_load(g2, s).wait()

            @pl.when(g2 < 2 * groups - 1)
            def _():
                act_w_load(g2 + 1, 1 - s).start()

            for n in range(3):
                cols = slice(n * width, (n + 1) * width)
                out = dot_nn(act_w_ref[s], wqkv_ref[:, cols])
                if n == 0:
                    out = (out + query_bias_ref[...]) * scale
                if n == 2:
                    out = out + value_bias_ref[...]
                qkv_ref[g2, :, cols] = out.astype(bf16)

            @pl.loop(0, sub // 4)
            def _(wi):
                items = []
                for e in range(4):
                    w = wi * 4 + e
                    line = pl.ds(pl.multiple_of(w * pad, pad), pad)
                    items += [(w, line, t) for t in range(quads)]
                for first in range(0, len(items), 8):
                    batch = items[first : first + 8]
                    scores = [
                        dot_nt(
                            qkv_ref[g2, line, width + 128 * t : width + 128 * (t + 1)],
                            stacked(qkv_ref[g2, line, 128 * t : 128 * (t + 1)]),
                        )[0:key_rows]
                        + bias_ref[t]
                        for w, line, t in batch
                    ]
                    tops = [jnp.max(x, axis=0, keepdims=True) for x in scores]
                    weights = [jnp.exp(x - top) for x, top in zip(scores, tops)]
                    totals = [jnp.sum(x, axis=0, keepdims=True) for x in weights]
                    for (w, line, t), top, total in zip(batch, tops, totals):
                        lse_ref[g2, w, t : t + 1, :] = top + jnp.log(total)
                    probs = [
                        grow(x * (1.0 / total)).astype(bf16) for x, total in zip(weights, totals)
                    ]
                    mixes = [
                        dot_tn(
                            x, qkv_ref[g2, line, 2 * width + 128 * t : 2 * width + 128 * (t + 1)]
                        )
                        for x, (w, line, t) in zip(probs, batch)
                    ]
                    for x, (w, line, t) in zip(mixes, batch):
                        mixed_w_ref[line, 128 * t : 128 * (t + 1)] = diagonal(x).astype(bf16)

            wide_ref[:, pl.ds(pl.multiple_of(sub * s, sub), sub), :] = dot_nn(
                back_ref[...], mixed_w_ref[...]
            ).reshape(tokens, sub, width)

        @pl.when(g != 0)
        def _():
            store(mixed_ref, mixed_hbm, g - 1, mixed_sem).wait()

        @pl.when(g == 0)
        def _():
            gather_relay(2)
            gather_finish(2)

        @pl.when(g == groups - 1)
        def _():
            gather_relay(4)

        mixed_ref[...] = wide_ref[...].astype(bf16)
        store(mixed_ref, mixed_hbm, g, mixed_sem).start()
        out = dot_nn(mixed_ref[...].reshape(rows, width), wproj_ref[...]) + proj_bias_ref[...]
        dx_ref[:, pl.ds(win0, group), :] = in_ref[slot].astype(f32) + out.reshape(
            tokens, group, width
        )

    gather_finish(3)
    gather_finish(4)
    for i in range(5):
        gather_drain(i)
    store(mixed_ref, mixed_hbm, groups - 1, mixed_sem).wait()

    @pl.loop(0, groups)
    def _(g):
        win0 = pl.multiple_of(g * group, group)
        slot = lax.rem(2 * groups + g, 2)
        load(dy_hbm, g, slot).wait()

        @pl.when(g < groups - 1)
        def _():
            load(dy_hbm, g + 1, 1 - slot).start()

        @pl.when(g == groups - 1)
        def _():
            load(x_hbm, 0, 1 - slot).start()

        @pl.when(g != 0)
        def _():
            store(y_ref, y_hbm, g - 1, y_sem).wait()

        mixed_load(g).start()

        @pl.loop(0, tokens // step)
        def _(n):
            part = dx_ref[pl.ds(n * step, step), pl.ds(win0, group), :].reshape(step * group, width)
            normal, _ = norm_parts(part)
            lines = pl.ds(pl.multiple_of(n * step * group, step * group), step * group)
            sa_ref[lines, :] = (normal * gain2_ref[...] + shift2_ref[...]).astype(bf16)

        sat_ref[0:width, :] = sa_ref[...].T
        dyt_ref[...] = in_ref[slot].reshape(rows, width).T

        count = hidden // chunk
        columns = [slice(i * chunk, (i + 1) * chunk) for i in range(count)]

        def rise(i):
            u_ref[...] = dot_nn(sa_ref[...], w1_ref[:, columns[i]])
            da_ref[...] = dot_nt(in_ref[slot].reshape(rows, width), w2_ref[columns[i], :])

        def bend(i):
            for m in range(tokens // step):
                lines = slice(m * step * group, (m + 1) * step * group)
                value, slope = gelu_pair(u_ref[lines, :] + hidden_bias_ref[:, columns[i]])
                act_ref[lines, columns[i]] = value.astype(bf16)
                dup_ref[lines, columns[i]] = (da_ref[lines, :] * slope).astype(bf16)

        def gather_grads(i):
            cols = columns[i]
            part1 = dot_nn(sat_ref[...], dup_ref[:, cols])
            dw1_ref[:, cols] += part1[0:width]
            add_small("hb", part1[width : width + 8], cols.start)
            dw2t_ref[:, cols] += dot_nn(dyt_ref[...], act_ref[:, cols])

        rise(0)
        for i in range(count):
            bend(i)
            if i > 0:
                gather_grads(i - 1)
            if i + 1 < count:
                rise(i + 1)
        gather_grads(count - 1)

        @pl.when(g == groups - 1)
        def _():
            unit_stage(0, 0)

        out = dot_nn(act_ref[...], w2_ref[...]) + output_bias_ref[...]
        y_ref[...] = (
            dx_ref[:, pl.ds(win0, group), :] + out.reshape(tokens, group, width)
        ).astype(bf16)
        wide_ref[...] = dot_nt(dup_ref[...], w1_ref[...]).reshape(tokens, group, width)

        @pl.when(g == groups - 1)
        def _():
            unit_stage(1, 0)

        store(y_ref, y_hbm, g, y_sem).start()

        @pl.loop(0, tokens // step)
        def _(n):
            lines = pl.ds(pl.multiple_of(n * step * group, step * group), step * group)
            normal, inverse = norm_parts(
                dx_ref[pl.ds(n * step, step), pl.ds(win0, group), :].reshape(step * group, width)
            )
            grad = wide_ref[pl.ds(n * step, step)].reshape(step * group, width)
            scaled = grad * gain2_ref[...]
            back = inverse * (
                scaled
                - jnp.mean(scaled, axis=-1, keepdims=True)
                - normal * jnp.mean(scaled * normal, axis=-1, keepdims=True)
            )
            cot = in_ref[slot, pl.ds(n * step, step)].astype(f32).reshape(step * group, width)
            total = cot + back
            dx_ref[pl.ds(n * step, step), pl.ds(win0, group), :] = total.reshape(step, group, width)
            sa_ref[lines, :] = total.astype(bf16)
            tip = lax.broadcasted_iota(jnp.int32, (16, step * group), 0) == 0
            tip = tip.astype(f32).astype(bf16)
            for name, value in (("ob", cot), ("pb", total), ("g2", grad * normal), ("s2", grad)):
                add_small(name, dot_nn(tip, value.astype(bf16))[0:8])

        @pl.when(g == groups - 1)
        def _():
            unit_stage(0, 1)

        mixed_load(g).wait()
        dwproj_ref[...] += dot_tn(mixed_ref[...].reshape(rows, width), sa_ref[...])

    store(y_ref, y_hbm, groups - 1, y_sem).wait()
    unit_stage(1, 1)
    unit_stage(2, 0)
    normal_w_load(0, 0).start()

    plan = {0: ((2, 1),), 5: ((0, 2),), 6: ((1, 2),), 7: ((2, 2),), 8: ((0, 3),), 9: ((1, 3),), 10: ((2, 3),), 11: ((0, 4),)}

    def progress(g2, half):
        for point, calls in plan.items():
            if point % 2 == half:

                @pl.when(g2 == point // 2)
                def _():
                    for u, stage in calls:
                        unit_stage(u, stage)

    subs = 2 * groups

    @pl.loop(0, subs)
    def _(g2):
        s = lax.rem(g2, 2)
        half8 = dx_ref[:, pl.ds(pl.multiple_of(g2 * sub, sub), sub), :]
        half_w = dot_nn(perm_ref[...], half8.reshape(rows8, width).astype(bf16)).astype(bf16)
        mixed_w_ref[...] = dot_nt(half_w, wproj_ref[...]).astype(bf16)
        progress(g2, 0)

        @pl.loop(0, sub // 2)
        def _(wi):
            items = []
            for e in range(2):
                w = wi * 2 + e
                line = pl.ds(pl.multiple_of(w * pad, pad), pad)
                for t in range(quads):
                    cols = [
                        slice(i * width + 128 * t, i * width + 128 * (t + 1)) for i in range(3)
                    ]
                    items.append((w, line, t, cols))
            for first in range(0, len(items), 8):
                batch = items[first : first + 8]
                queries = [stacked(qkv_ref[g2, line, c[0]]) for w, line, t, c in batch]
                scores = [
                    dot_nt(qkv_ref[g2, line, c[1]], x)[0:key_rows] + bias_ref[t]
                    for x, (w, line, t, c) in zip(queries, batch)
                ]
                grads = [stacked(mixed_w_ref[line, c[0]]) for w, line, t, c in batch]
                prob_grads = [
                    dot_nt(qkv_ref[g2, line, c[2]], x)[0:key_rows]
                    for x, (w, line, t, c) in zip(grads, batch)
                ]
                probs = [
                    jnp.exp(x - lse_ref[g2, w, t : t + 1, :])
                    for x, (w, line, t, c) in zip(scores, batch)
                ]
                prob_halves = [grow(x).astype(bf16) for x in probs]
                value_grads = [dot_nn(x, y) for x, y in zip(prob_halves, grads)]
                deltas = [
                    jnp.sum(x * y, axis=0, keepdims=True) for x, y in zip(probs, prob_grads)
                ]
                score_grads = [
                    x * (y - delta) for x, y, delta in zip(probs, prob_grads, deltas)
                ]
                for x, (w, line, t, c) in zip(score_grads, batch):
                    dbias_ref[t] += x
                halves_ = [grow(x).astype(bf16) for x in score_grads]
                key_grads = [dot_nn(x, y) for x, y in zip(halves_, queries)]
                query_grads = [
                    dot_tn(x, qkv_ref[g2, line, c[1]])
                    for x, (w, line, t, c) in zip(halves_, batch)
                ]
                for k, (w, line, t, c) in enumerate(batch):
                    qkv_ref[g2, line, c[0]] = (diagonal(query_grads[k]) * scale).astype(bf16)
                    qkv_ref[g2, line, c[1]] = key_grads[k].astype(bf16)
                    qkv_ref[g2, line, c[2]] = value_grads[k].astype(bf16)

        progress(g2, 1)
        normal_w_load(g2, s).wait()

        @pl.when(g2 < subs - 1)
        def _():
            normal_w_load(g2 + 1, 1 - s).start()

        sat_ref[0:width, 0:rows_w] = act_w_ref[s].T
        for n in range(3):
            cols = slice(n * width, (n + 1) * width)
            part = dot_nn(sat_ref[:, 0:rows_w], qkv_ref[g2, :, cols])
            dwqkv_ref[:, cols] += part[0:width]
            add_small(("qb", "s1", "vb")[n], part[width : width + 8])

            @pl.when(g2 == subs - 1)
            def _():
                unit_stage(3 + n, 0)
                if n == 2:
                    unit_stage(3, 1)

    for t in range(quads):
        for h in range(quad // 2):
            both = dbias_ref[t, :, 128 * h : 128 * (h + 1)]
            plane(t * quad + 2 * h)[...] = jnp.where(low_lanes, both, 0.0)
            plane(t * quad + 2 * h + 1)[...] = jnp.where(
                low_lanes, pltpu.roll(both, pad, 1), 0.0
            )
    total_ref[...] = jnp.zeros(total_ref.shape, f32)

    @pl.loop(0, tokens)
    def _(j):
        hit = named(j)
        line = plane_ref[pl.ds(j, heads, stride=key_rows), :]
        upper_half = line.astype(bf16)
        lower_half = (line - upper_half.astype(f32)).astype(bf16)
        found = dot_nt(upper_half, hit) + dot_nt(lower_half, hit)
        for side in range(2):
            lanes = slice(side * table_lanes, (side + 1) * table_lanes)
            total_ref[0:table_tall, lanes] = (
                total_ref[0:table_tall, lanes] + found[side * table_tall : (side + 1) * table_tall]
            )

    for u in range(4, 6):
        unit_stage(u, 1)
    weighted = jnp.zeros((width, 128), f32)
    for n in range(3 * width // 128):
        lanes = slice(n * 128, (n + 1) * 128)
        weighted = weighted + dwqkv_ref[:, lanes] * wqkv_ref[:, lanes].astype(f32)
    add_small("g1", fold_rows(weighted.T))
    merged_sums = jnp.concatenate(
        [small_ref[:, base[n][0] : base[n][0] + width] for n in ("qb", "s1", "vb")], axis=1
    )
    sums_high = merged_sums.astype(bf16)
    sums_low = (merged_sums - sums_high.astype(f32)).astype(bf16)
    small_ref[:, base["s1"][0] : base["s1"][0] + width] = dot_nt(
        sums_high, wqkv_ref[...]
    ) + dot_nt(sums_low, wqkv_ref[...])

    def put_sums(first, last):
        for i in range(first, last):
            total_ref[table_tall + i : table_tall + i + 1, :] = jnp.sum(
                small_ref[:, i * width : (i + 1) * width], axis=0, keepdims=True
            )

    put_sums(0, small_ref.shape[1] // width)
    total_start(0)
    plan2 = {0: ((1, 4),), 1: ((3, 2), (2, 4), (-1, 0)), 2: ((0, 5), (4, 2)), 3: ((5, 2),), 4: ((1, 5), (-1, 1)), 5: ((3, 3),)}

    @pl.loop(0, groups)
    def _(g):
        win0 = pl.multiple_of(g * group, group)
        slot = lax.rem(3 * groups + g, 2)
        load(x_hbm, g, slot).wait()

        @pl.when(g < groups - 1)
        def _():
            load(x_hbm, g + 1, 1 - slot).start()

        for s in range(2):
            g2 = g * 2 + s
            mixed_w_ref[...] = dot_nt(qkv_ref[g2], wqkv_ref[...]).astype(bf16)
            wide_ref[:, sub * s : sub * (s + 1), :] = dot_nn(back_ref[...], mixed_w_ref[...]).reshape(
                tokens, sub, width
            )
            for point, calls in plan2.items():
                if point % 2 == s:

                    @pl.when(g == point // 2)
                    def _():
                        for u, stage in calls:
                            if u < 0:
                                total_finish(stage)
                            else:
                                unit_stage(u, stage)

        @pl.loop(0, tokens // step)
        def _(n):
            part = in_ref[slot, pl.ds(n * step, step)].astype(f32)
            normal, inverse = norm_parts(part.reshape(step * group, width))
            grad = wide_ref[pl.ds(n * step, step)].reshape(step * group, width)
            scaled = grad * gain1_ref[...]
            back = inverse * (
                scaled
                - jnp.mean(scaled, axis=-1, keepdims=True)
                - normal * jnp.mean(scaled * normal, axis=-1, keepdims=True)
            )
            dx_ref[pl.ds(n * step, step), pl.ds(win0, group), :] += back.reshape(step, group, width)

        @pl.when(g != 0)
        def _():
            store(y_ref, dx_hbm, g - 1, dx_sem).wait()

        y_ref[...] = dx_ref[:, pl.ds(win0, group), :].astype(bf16)
        store(y_ref, dx_hbm, g, dx_sem).start()

    done = {0: 5, 1: 5, 2: 4, 3: 3, 4: 2, 5: 2}
    for stage in range(2, stages):
        for u in (3, 4, 5, 2, 0, 1):
            if stage > done[u]:
                unit_stage(u, stage)
    for step_at in range(2, total_steps):
        total_finish(step_at)
    store(y_ref, dx_hbm, groups - 1, dx_sem).wait()


def local_pass(x, dy, wqkv, wproj, w1, w2, vectors, table, index, shards, reps):
    tokens, windows, width = x.shape
    hidden = w1.shape[1]
    heads = table.shape[0]
    dims = (tokens, windows, width, heads, hidden, shards, reps)
    chips = shards // 2
    bits = reps.bit_length() - 1
    sub = 8
    group = 2 * sub
    pad = 64
    rows = tokens * group
    small_size = 8 * width + hidden
    subs = windows // sub
    owned = width // shards
    unit_rows = (hidden // shards, hidden // shards, owned, owned, owned, owned)
    near_size = 1 << min(bits, 3)
    slots = near_size - 1 + bits - min(bits, 3)
    total_rows = -(-(heads // 2 + small_size // width) // (8 * shards)) * 8 * shards
    shapes = (
        [
            jax.ShapeDtypeStruct(x.shape, bf16),
            jax.ShapeDtypeStruct(x.shape, bf16),
            jax.ShapeDtypeStruct(x.shape, bf16),
            jax.ShapeDtypeStruct((subs, sub * pad, width), bf16),
            jax.ShapeDtypeStruct((subs, sub * pad, width), bf16),
        ]
        + [jax.ShapeDtypeStruct((r, width), bf16) for r in unit_rows]
        + [jax.ShapeDtypeStruct((total_rows, width), f32)]
    )
    vmem = pl.BlockSpec(memory_space=pltpu.VMEM)
    hbm = pl.BlockSpec(memory_space=pl.ANY)

    return pl.pallas_call(
        functools.partial(compute_kernel, dims),
        out_shape=shapes,
        in_specs=[hbm] * 6 + [vmem] * 11,
        out_specs=[hbm] * 5 + [vmem] * 7,
        scratch_shapes=[
            pltpu.VMEM((2, tokens, group, width), bf16),
            pltpu.VMEM((tokens, group, width), bf16),
            pltpu.VMEM(x.shape, f32),
            pltpu.VMEM((width, 3 * width), f32),
            pltpu.VMEM((width, width), f32),
            pltpu.VMEM((width, hidden), f32),
            pltpu.VMEM((width, hidden), f32),
            pltpu.VMEM((8, small_size), f32),
            pltpu.VMEM((heads // 4, 56, 256), f32),
            pltpu.VMEM((heads // 4, 56, 256), f32),
            pltpu.VMEM((sub * pad, tokens * sub), bf16),
            pltpu.VMEM((tokens * sub, sub * pad), bf16),
            pltpu.VMEM((2, sub * pad, width), bf16),
            pltpu.VMEM((2, width, 128), f32),
            pltpu.VMEM((subs, sub * pad, 3 * width), bf16),
            pltpu.VMEM((sub * pad, width), bf16),
            pltpu.VMEM((tokens, group, width), bf16),
            pltpu.VMEM((subs, sub, heads // 4, 256), f32),
            pltpu.VMEM((tokens, group, width), f32),
            pltpu.VMEM((rows, width), bf16),
            pltpu.VMEM((width + 16, rows), bf16),
            pltpu.VMEM((width, rows), bf16),
            pltpu.VMEM((rows, width), f32),
            pltpu.VMEM((rows, width), f32),
            pltpu.VMEM((heads * 56, 128), f32),
            pltpu.VMEM((128, 128), f32),
            pltpu.VMEM((heads, -(-table.shape[1] // 128) * 128), f32),
            pltpu.VMEM((rows, hidden), bf16),
            pltpu.VMEM((rows, hidden), bf16),
            pltpu.VMEM((width, 3 * width), bf16),
            pltpu.VMEM((width, width), bf16),
            pltpu.VMEM((width, hidden), bf16),
            pltpu.VMEM((hidden, width), bf16),
            pltpu.VMEM((chips - 1, unit_rows[0], width), bf16),
            *[pltpu.VMEM((chips, r, width), bf16) for r in unit_rows],
            *[pltpu.VMEM((chips - 1, r, width), bf16) for r in unit_rows],
            *[pltpu.VMEM((slots * r // near_size, width), bf16) for r in unit_rows],
            pltpu.VMEM((2 * shards - 2 + slots, total_rows // shards, width), f32),
            pltpu.SemaphoreType.DMA((5,)),
            pltpu.SemaphoreType.DMA((5, chips)),
            pltpu.SemaphoreType.DMA((5, chips)),
            pltpu.SemaphoreType.DMA((5, chips - 1)),
            pltpu.SemaphoreType.DMA((5, chips - 1)),
            pltpu.SemaphoreType.DMA((2,)),
            pltpu.SemaphoreType.DMA,
            pltpu.SemaphoreType.DMA,
            pltpu.SemaphoreType.DMA((2,)),
            pltpu.SemaphoreType.DMA((2,)),
            pltpu.SemaphoreType.DMA,
            pltpu.SemaphoreType.DMA((6, chips)),
            pltpu.SemaphoreType.DMA((6, chips)),
            pltpu.SemaphoreType.DMA((6, chips - 1)),
            pltpu.SemaphoreType.DMA((6, chips - 1)),
            pltpu.SemaphoreType.DMA((6, slots)),
            pltpu.SemaphoreType.DMA((6, slots)),
            pltpu.SemaphoreType.DMA((6, slots)),
            pltpu.SemaphoreType.DMA((6, slots)),
            pltpu.SemaphoreType.DMA((2 * shards - 2 + slots,)),
            pltpu.SemaphoreType.DMA((2 * shards - 2 + slots,)),
        ],
        compiler_params=pltpu.CompilerParams(
            vmem_limit_bytes=67043328, collective_id=0, has_side_effects=True
        ),
    )(x, dy, wqkv, wproj, w1, w2, *vectors, table, index)


def spread_kernel(heads, sizes, *refs):
    works = refs[:6]
    total_ref, y_in, dx_in = refs[6:9]
    dwqkv_ref, dwproj_ref, dw1_ref, dw2_ref, table_ref = refs[9:14]
    sums = refs[14:-2]
    y_ref, dx_ref = refs[-2:]
    width = dwproj_ref.shape[1]
    owned = dwproj_ref.shape[0]
    y_ref[...] = y_in[...]
    dx_ref[...] = dx_in[...].astype(f32)

    @pl.when(pl.program_id(0) == 0)
    def _():
        for i in range(dw1_ref.shape[1] // width):
            dw1_ref[:, i * width : (i + 1) * width] = works[0][
                i * owned : (i + 1) * owned, :
            ].astype(f32)
        dw2_ref[...] = works[1][...].astype(f32)
        dwproj_ref[...] = works[2][...].astype(f32)
        for i in range(3):
            dwqkv_ref[:, i * width : (i + 1) * width] = works[3 + i][...].astype(f32)
        tall = heads // 2
        rows_t = table_ref.shape[1]
        lanes = total_ref.shape[1] // 2
        table_ref[0:tall, :] = total_ref[0:tall, 0:rows_t]
        table_ref[tall:heads, :] = total_ref[0:tall, lanes : lanes + rows_t]
        row = tall
        for ref, size in zip(sums, sizes):
            for i in range(size // width):
                ref[:, i * width : (i + 1) * width] = total_ref[row : row + 1, :]
                row += 1


def spread(works, total, y, dx, hidden, heads, table_rows):
    tokens, windows, width = y.shape
    owned = works[2].shape[0]
    sizes = (width, width, width, hidden, width, width, width, width, width)
    shapes = [
        (owned, 3 * width),
        (owned, width),
        (owned, hidden),
        works[1].shape,
        (heads, table_rows),
    ] + [(1, size) for size in sizes]
    step = tokens
    slab = pl.BlockSpec((step, windows, width), lambda i: (i, 0, 0))
    whole = lambda shape: pl.BlockSpec(shape, lambda i: (0, 0))
    return pl.pallas_call(
        functools.partial(spread_kernel, heads, sizes),
        grid=(tokens // step,),
        out_shape=[jax.ShapeDtypeStruct(shape, f32) for shape in shapes]
        + [jax.ShapeDtypeStruct(y.shape, bf16), jax.ShapeDtypeStruct(y.shape, f32)],
        in_specs=[whole(w.shape) for w in works] + [whole(total.shape), slab, slab],
        out_specs=[whole(shape) for shape in shapes] + [slab, slab],
    )(*works, total, y, dx)


def on_device(
    shards,
    reps,
    block_input,
    out_grad,
    qkv_weight,
    query_bias,
    value_bias,
    proj_weight,
    proj_bias,
    hidden_weight,
    hidden_bias,
    output_weight,
    output_bias,
    first_gain,
    first_shift,
    second_gain,
    second_shift,
    bias_table,
    table_index,
):
    windows, tokens, width = block_input.shape
    table_rows, heads = bias_table.shape
    hidden = hidden_bias.shape[0]
    vectors = [
        v.reshape(1, -1)
        for v in (
            query_bias,
            value_bias,
            proj_bias,
            hidden_bias,
            output_bias,
            first_gain,
            first_shift,
            second_gain,
            second_shift,
        )
    ]
    y, dx, _, _, _, *works, total = local_pass(
        jnp.transpose(block_input, (1, 0, 2)),
        jnp.transpose(out_grad, (1, 0, 2)),
        qkv_weight,
        proj_weight,
        hidden_weight,
        output_weight,
        vectors,
        bias_table.T,
        table_index,
        shards,
        reps,
    )
    (dwqkv, dwproj, dw1, dw2, table_grad, qb, vb, pb, hb, ob, g1, s1, g2, s2, y, dx) = spread(
        works, total, y, dx, hidden, heads, table_rows
    )
    return (
        jnp.transpose(y, (1, 0, 2)),
        jnp.transpose(dx, (1, 0, 2)),
        dwqkv,
        qb.reshape(-1),
        vb.reshape(-1),
        dwproj,
        pb.reshape(-1),
        dw1,
        hb.reshape(-1),
        dw2,
        ob.reshape(-1),
        g1.reshape(-1),
        s1.reshape(-1),
        g2.reshape(-1),
        s2.reshape(-1),
        table_grad.T,
    )


def solution(mesh):
    rows = P(("shard", "rep"), None, None)
    cut = P("shard", None)
    full = P()
    return jax.shard_map(
        functools.partial(on_device, mesh.shape["shard"], mesh.shape["rep"]),
        mesh=mesh,
        in_specs=(
            rows,
            rows,
            cut,
            full,
            full,
            cut,
            full,
            cut,
            full,
            cut,
            full,
            full,
            full,
            full,
            full,
            full,
            full,
        ),
        out_specs=(
            rows,
            rows,
            cut,
            full,
            full,
            cut,
            full,
            cut,
            full,
            cut,
            full,
            full,
            full,
            full,
            full,
            full,
        ),
        check_vma=False,
    )
```
